32 devices in a mesh: px: 4 (over y, x), py: 8 (over z, core).
Axes of the slice: x: 2, y: 2, z: 4, core: 2. Of those that a mesh axis runs over, the one named last changes fastest.
Arguments:
- white_noise: float32 [2, 64, 256, 256], P(None, 'px', 'py'), may hold values from -6 to 6
- spectrum: float32 [64, 256, 256], P('px', 'py'), may hold values from 0.1 to 2, as said below
- group_table: int32 [3, 8], replicated, may hold values from 0 to 7, each once within a row
Outputs:
- modulus: float32 [2, 64, 256, 256], P(None, 'px', 'py')
- level_one: float32 [2, 32, 128, 128], P(None, 'px', 'py')
- level_two: float32 [2, 16, 64, 64], P(None, 'px', 'py')
- level_three: float32 [2, 8, 32, 32], P(None, 'px', 'py')
The draws below stay inside these ranges and needn't reach their ends.
Inputs may be any that keep to these rules, and one draw needn't show every extreme that they name: spectrum[j, m, k] equals spectrum[(64 - j) % 64, (256 - m) % 256, (256 - k) % 256]. `group_table`: each row is a permutation of 0 to 7.
All inputs are finite; a program needn't handle non-finite values.
Results may differ from the reference program's by a relative error of at most 0.000088.
Values sent between devices are 32-bit elements; how exact they have to be, the bound alone decides.
A program may use at most 192 MiB of HBM per device.

```python
import math
import jax
import jax.numpy as jnp

FIELDS = 2
LEVELS = 3
NZ = 256
NX = 64
NY = 256
N_PY = 8


def draw_spectrum(key, part):
    log_low = math.log(0.1)
    log_high = math.log(2.0)
    rough_part = jnp.exp(jax.random.uniform(key, (NX, NY, NZ), jnp.float32, log_low, log_high))
    mirror = jnp.roll(jnp.flip(rough_part, (0, 1, 2)), 1, (0, 1, 2))
    values = 0.5 * (rough_part + mirror)
    return values


def level_of(stream_key, extent, shards, low, top_value):
    def one(axis_at, blocks):
        draws = jax.random.uniform(jax.random.fold_in(jax.random.fold_in(stream_key, 6), axis_at), (blocks,), jnp.float32, low / len(shards), top_value / len(shards))
        return jnp.repeat(jnp.exp(draws), extent[axis_at] // blocks).reshape((-1,) + (1,) * (len(extent) - axis_at - 1))

    level = one(*shards[0])
    for cut in shards[1:]:
        level = level * one(*cut)
    return level


def normal_values(own_key, shape, deviation, most, split=(), dtype=jnp.bfloat16):
    array = jax.random.normal(own_key, shape, jnp.float32) * deviation
    if len(split) > 0:
        array = level_of(own_key, shape, split, -0.22, 0.18) * array
    return jnp.clip(array, min=-most, max=most).astype(dtype)


def setup_inputs(seed: int = 0) -> dict:
    arg_keys = jax.random.split(jax.random.key(seed), 4)
    white_noise = normal_values(arg_keys[0], (FIELDS, NX, NY, NZ), 1.0, 6.0, ((1, 4), (2, 8)), jnp.float32)
    spectrum = draw_spectrum(jax.random.fold_in(arg_keys[3], 71), 0)
    group_table = jax.vmap(lambda own: jax.random.permutation(own, N_PY))(jax.random.split(arg_keys[2], LEVELS)).reshape((LEVELS, N_PY)).astype(jnp.int32)
    return dict(white_noise=white_noise, spectrum=spectrum, group_table=group_table)


def coarsen(values):
    members, size_x, size_y, size_z = values.shape
    blocks = values.reshape(members, size_x // 2, 2, size_y // 2, 2, size_z // 2, 2)
    return blocks.mean(axis=(2, 4, 6))


def route_blocks(coarse, group_order):
    members, size_x, size_y, size_z = coarse.shape
    blocks = coarse.reshape(members, size_x, N_PY, size_y // N_PY, size_z)
    picked = jnp.take(blocks, group_order, axis=2)
    return picked.reshape(members, size_x, size_y, size_z)


def reference(white_noise, spectrum, group_table):
    spectra = jnp.fft.fftn(white_noise, axes=(1, 2, 3))
    scaled = spectra * spectrum[None]
    fields_real = jnp.real(jnp.fft.ifftn(scaled, axes=(1, 2, 3)))
    modulus = jnp.exp(0.5 * fields_real)
    coarse_one = coarsen(modulus)
    coarse_two = coarsen(coarse_one)
    coarse_three = coarsen(coarse_two)
    level_one = route_blocks(coarse_one, group_table[0])
    level_two = route_blocks(coarse_two, group_table[1])
    level_three = route_blocks(coarse_three, group_table[2])
    return modulus, level_one, level_two, level_three
```

```python
import numpy as np

import jax
import jax.numpy as jnp
from jax import lax
from jax.experimental import pallas as pl
from jax.experimental.pallas import tpu as pltpu
from jax.sharding import PartitionSpec as P


def angles_of(length):
    positions = np.arange(length, dtype=np.int64)
    return (positions[:, None] * positions[None, :] % length) * (2.0 * np.pi / length)


def complex_array(length, direction):
    angles = angles_of(length)
    cos, sin = np.cos(angles), direction * np.sin(angles)
    return np.stack([np.stack([cos, sin], 1), np.stack([-sin, cos], 1)], 0)


def complex_table(length, direction):
    return jnp.asarray(complex_array(length, direction), jnp.float32)


def half_tables(length):
    angles = angles_of(length)[:, : length // 2]
    ahead = np.stack([np.cos(angles), -np.sin(angles)], 1)
    back = 2.0 * ahead
    nyquist = np.where(np.arange(length) % 2 == 0, 1.0, -1.0)
    ahead[:, 1, 0] = nyquist
    back[:, 0, 0] = 1.0
    back[:, 1, 0] = nyquist
    return jnp.asarray(ahead, jnp.float32), jnp.asarray(back, jnp.float32)


def einsum(pattern, left, right):
    return jnp.einsum(pattern, left, right, precision=lax.Precision.HIGH)


def swap_first(values):
    first = values[:, :, :1]
    turned = jnp.swapaxes(first, 0, 1)
    return jnp.concatenate([turned, values[:, :, 1:]], 2)


def coarsen(values):
    members, size_x, size_y, size_z = values.shape
    blocks = values.reshape(members, size_x // 2, 2, size_y // 2, 2, size_z // 2, 2)
    return blocks.mean(axis=(2, 4, 6))


def general_path(white_noise, spectrum, group_table):
    members, cells_x, cells_y, length_z = white_noise.shape
    size_px, size_py = lax.axis_size("px"), lax.axis_size("py")
    length_x, length_y = cells_x * size_px, cells_y * size_py
    half_z = length_z // 2
    block_py, block = half_z // size_py, half_z // size_py // size_px
    z_ahead, z_back = half_tables(length_z)
    scale = 1.0 / (length_x * length_y * length_z)

    table = jnp.transpose(spectrum, (2, 0, 1))
    last = jnp.broadcast_to(table[half_z : half_z + 1], (size_py, 1, cells_x, cells_y))
    table = jnp.concatenate([table[:half_z].reshape(size_py, block_py, cells_x, cells_y), last], 1)
    table = lax.all_to_all(table, "py", split_axis=0, concat_axis=3, tiled=True)[0]
    last = jnp.broadcast_to(table[block_py:], (size_px, 1, cells_x, length_y))
    table = jnp.concatenate([table[:block_py].reshape(size_px, block, cells_x, length_y), last], 1)
    table = lax.all_to_all(table, "px", split_axis=0, concat_axis=2, tiled=True)[0] * scale
    is_first = (lax.axis_index("px") == 0) & (lax.axis_index("py") == 0)
    other = jnp.where(is_first, table[block:], table[:1])
    tables = jnp.stack([table[:block], jnp.concatenate([other, table[1:block]], 0)], 0)

    values = einsum("fxyz,zck->fckxy", white_noise, z_ahead)
    values = swap_first(values)
    values = lax.all_to_all(values, "py", split_axis=2, concat_axis=4, tiled=True)
    values = einsum("fckxy,cydm->fdkxm", values, complex_table(length_y, -1.0))
    values = lax.all_to_all(values, "px", split_axis=2, concat_axis=3, tiled=True)
    values = einsum("fckxm,cxdj->fdkjm", values, complex_table(length_x, -1.0))
    values = values * tables[:, None]
    values = einsum("fckjm,cjdx->fdkxm", values, complex_table(length_x, 1.0))
    values = lax.all_to_all(values, "px", split_axis=3, concat_axis=2, tiled=True)
    values = einsum("fckxm,cmdy->fdkxy", values, complex_table(length_y, 1.0))
    values = lax.all_to_all(values, "py", split_axis=4, concat_axis=2, tiled=True)
    values = swap_first(values)
    fields = einsum("fckxy,zck->fxyz", values, z_back)
    modulus = jnp.exp(0.5 * fields)

    levels = []
    level = modulus
    for _ in range(3):
        level = coarsen(level)
        levels.append(level)
    pieces = [jnp.reshape(level, (size_py, -1)) for level in levels]
    widths = [piece.shape[1] for piece in pieces]
    joined = jnp.concatenate(pieces, 1)
    spread = lax.all_to_all(joined, "py", split_axis=0, concat_axis=0, tiled=True)
    picked, start = [], 0
    for index, width in enumerate(widths):
        part = spread[:, start : start + width]
        picked.append(jnp.take(part, group_table[index], axis=0))
        start += width
    joined = lax.all_to_all(
        jnp.concatenate(picked, 1), "py", split_axis=0, concat_axis=0, tiled=True
    )
    routed, start = [], 0
    for level, width in zip(levels, widths):
        routed.append(joined[:, start : start + width].reshape(level.shape))
        start += width
    return (modulus, routed[0], routed[1], routed[2])


LANES = 128
MESH = pl.DeviceIdType.MESH
BF16 = jnp.bfloat16
F32 = jnp.float32


def halves(values):
    high = values.astype(BF16)
    low = (values - high.astype(F32)).astype(BF16)
    return high, low


def host_halves(values):
    values = np.asarray(values, np.float64)
    high = values.astype(np.float32).astype(BF16)
    low = (values - high.astype(np.float64)).astype(np.float32).astype(BF16)
    return jnp.asarray(high), jnp.asarray(low)


def mm(left, right):
    return jnp.dot(left, right, preferred_element_type=F32)


def lane_of(shape):
    return lax.broadcasted_iota(jnp.int32, shape, len(shape) - 1)


def exchange(arrays, width):
    arrays = list(arrays)
    lane = lane_of(arrays[0].shape)
    distance = 1
    while distance < len(arrays):
        step = distance * width
        low = (lane // step) % 2 == 0
        for index in range(len(arrays)):
            if (index // distance) % 2 == 0:
                first, second = arrays[index], arrays[index + distance]
                arrays[index] = jnp.where(low, first, pltpu.roll(second, step, 1))
                arrays[index + distance] = jnp.where(
                    low, pltpu.roll(first, LANES - step, 1), second
                )
        distance *= 2
    return arrays


def turned(values, slots, ahead):
    real = (lane_of(values.shape) // slots) % 2 == 0
    from_imag = pltpu.roll(values, LANES - slots, 1)
    from_real = pltpu.roll(values, slots, 1)
    if ahead:
        return jnp.where(real, from_imag, -from_real)
    return jnp.where(real, -from_imag, from_real)


def swap_slot(first, second, slots):
    place = lane_of(first.shape) % (2 * slots)
    return (
        jnp.where(place == slots, pltpu.roll(second, slots, 1), first),
        jnp.where(place == 0, pltpu.roll(first, LANES - slots, 1), second),
    )


class Route:
    def __init__(self, axis, count, away, source, target, send, recv):
        self.axis, self.count, self.away = axis, count, away
        self.source, self.target = source, target
        self.send, self.recv = send, recv
        self.me = lax.axis_index(axis)

    def copy(self, source, target, peer, part):
        return pltpu.make_async_remote_copy(
            src_ref=source,
            dst_ref=target,
            send_sem=self.send,
            recv_sem=self.recv.at[part] if part is not None else self.recv,
            device_id={self.axis: peer},
            device_id_type=MESH,
        )

    def at(self, ref, where, index):
        return ref.at[where + (index,)]

    def start(self, where, part):
        for peer in self.away:
            source = self.at(self.source, where, peer)
            target = self.at(self.target, where, self.me)
            self.copy(source, target, peer, part).start()

    def arrive(self, where, part):
        spot = self.at(self.target, where, pl.ds(0, self.count - 1))
        self.copy(spot, spot, self.away[0], part).wait_recv()
        self.target[where + (self.me,)] = self.source[where + (self.me,)]

    def drain(self, where):
        spot = self.source.at[where + (pl.ds(0, self.count - 1),)]
        self.copy(spot, spot, self.away[0], 0 if len(self.recv.shape) else None).wait_send()


def whole_kernel(sizes, loads, *refs):
    cells_x, cells_y, length_z, slots, ranks_y = sizes
    members = 2
    width = 2 * slots
    per_tile = cells_x // ranks_y
    tiles = length_z // LANES
    chunks = tiles * per_tile
    length_y = cells_y * ranks_y
    blocks = slots // members
    rows_m = length_y // blocks
    (group_table, *sources) = refs[: 1 + loads]
    modulus_out, level_one, level_two, level_three = refs[1 + loads : 5 + loads]
    held_in = refs[5 + loads : 5 + 2 * loads]
    (
        z_send, z_recv, x_send, x_recv, w_send, w_recv, b_send, b_recv,
        s_send, s_recv, t_send, t_recv, n_send, n_recv, m_recv,
        tables, other, held, modulus, c_send, c_recv_0, c_recv_1, d_send, d_recv,
        load_sem, store_sem, send_sem, z_sem, x_sem, w_sem, b_sem, c_sem, d_sem, s_sem,
    ) = refs[5 + 2 * loads :]
    (
        spectrum, noise, ahead_hi, ahead_lo, y_hi, y_lo, x_ahead, x_back,
        back_hi, back_lo, pool_rows, pool_columns,
    ) = held_in

    me_x, me_y = lax.axis_index("px"), lax.axis_index("py")
    copies = [
        pltpu.make_async_copy(source, target, load_sem.at[index])
        for index, (source, target) in enumerate(zip(sources, held_in))
    ]
    for copy in copies:
        copy.start()

    place, core = me_y // 2, me_y % 2
    chips = ranks_y // 2
    near = chips - 1 - (chips - 2) * (place % 2)
    steps = [chips // 2, near, chips - near]
    away_y = []
    for step in steps:
        for side in (0, 1):
            away_y.append((place + step) % chips * 2 + (core + side) % 2)
    away_y.append(place * 2 + 1 - core)
    away_x = [slots - 1 - me_x, (me_x + 2) % slots, me_x + 1 - 2 * (me_x % 2)]

    barrier = pltpu.get_barrier_semaphore()
    for peer in away_y:
        pl.semaphore_signal(barrier, inc=1, device_id={"py": peer}, device_id_type=MESH)
    for peer in away_x:
        pl.semaphore_signal(barrier, inc=1, device_id={"px": peer}, device_id_type=MESH)

    def route(axis, source, target, send, recv):
        away, count = (away_y, ranks_y) if axis == "py" else (away_x, slots)
        return Route(axis, count, away, source, target, send_sem.at[send], recv)

    z_route = route("py", z_send, z_recv, 0, z_sem)
    x_route = route("px", x_send, x_recv, 1, x_sem)
    w_route = route("px", w_send, w_recv, 2, w_sem)
    b_route = route("py", b_send, b_recv, 3, b_sem)
    s_route = route("py", s_send, s_recv, 4, s_sem.at[0])
    t_route = route("px", t_send, t_recv, 5, s_sem.at[1])
    c_recv = (c_recv_0, c_recv_1)
    c_routes = [route("py", c_send.at[f], c_recv[f], 6, c_sem.at[f]) for f in range(members)]
    d_route = route("py", d_send, d_recv, 7, d_sem)

    copies[0].wait()
    for row in range(0, cells_y, 8):
        rows = pl.ds(row, 8)
        moved = exchange([spectrum[x, rows, pl.ds(0, LANES)] for x in range(cells_x)], width)
        for group in range(cells_x):
            s_send[group % ranks_y, group // ranks_y, rows] = moved[group]
    lane = lane_of((8, LANES))
    strip = jnp.zeros((8, LANES), F32)
    quarter = (lane // 2) % slots
    for x in range(cells_x):
        for part in range(cells_y // 8):
            value = spectrum[x, pl.ds(part * 8, 8), pl.ds(LANES, 1)]
            strip = jnp.where((lane // width == x) & (quarter == part), value, strip)
    n_send[...] = strip

    pl.semaphore_wait(barrier, ranks_y + slots - 2)
    s_route.start((), None)

    def strip_copy():
        return pltpu.make_async_remote_copy(
            src_ref=n_send, dst_ref=n_recv.at[me_y], send_sem=send_sem.at[8],
            recv_sem=s_sem.at[2], device_id={"py": 0}, device_id_type=MESH,
        )

    pl.when(me_y != 0)(lambda: strip_copy().start())

    copies[1].wait()
    copies[2].wait()
    copies[3].wait()
    cells = cells_x * cells_y
    for f in range(members):
        high, low = halves(noise[f].reshape(cells, length_z))
        held[f] = mm(high, ahead_hi[...]) + mm(high, ahead_lo[...]) + mm(low, ahead_hi[...])
    for tile in range(tiles):
        lanes = pl.ds(tile * LANES, LANES)
        for row in range(0, cells_y, 8):
            rows = pl.ds(row, 8)
            both = []
            for f in range(members):
                both.append(
                    exchange(
                        [held[f, pl.ds(x * cells_y + row, 8), lanes] for x in range(cells_x)],
                        width,
                    )
                )
            if tile == 0:
                both[0][0], both[1][0] = swap_slot(both[0][0], both[1][0], slots)
            for f in range(members):
                for group in range(cells_x):
                    chunk = tile * per_tile + group // ranks_y
                    z_send[chunk, group % ranks_y, f, rows] = both[f][group]
        for part in range(per_tile):
            chunk = tile * per_tile + part
            z_route.start((chunk,), chunk)

    s_route.arrive((), None)
    for row in range(0, rows_m, 8):
        arrays = []
        for tile in range(tiles):
            for block in range(blocks):
                at = block * rows_m + row
                arrays.append(s_recv[at // cells_y, tile, pl.ds(at % cells_y, 8)])
        moved = exchange(arrays, 2)
        for rank in range(slots):
            t_send[rank, pl.ds(row, 8)] = moved[rank]
    t_route.start((), None)

    def strips_copy(source):
        return pltpu.make_async_remote_copy(
            src_ref=n_recv, dst_ref=m_recv.at[source], send_sem=send_sem.at[9],
            recv_sem=s_sem.at[3], device_id={"px": 0}, device_id_type=MESH,
        )

    @pl.when(me_y == 0)
    def _():
        spot = n_recv.at[pl.ds(0, ranks_y - 1)]
        pltpu.make_async_remote_copy(
            src_ref=spot, dst_ref=spot, send_sem=send_sem.at[8], recv_sem=s_sem.at[2],
            device_id={"py": 1}, device_id_type=MESH,
        ).wait_recv()
        n_recv[0] = n_send[...]
        pl.when(me_x != 0)(lambda: strips_copy(me_x).start())

    def along_y(route, part, columns, ahead):
        high, low = halves(columns)
        product = mm(y_hi[...], high) + mm(y_hi[...], low) + mm(y_lo[...], high)
        return product

    def combined(product, f, start, rows, ahead):
        lanes = slice(f * LANES, (f + 1) * LANES)
        by_cos = product[start : start + rows, lanes]
        by_sin = product[length_y + start : length_y + start + rows, lanes]
        return by_cos + turned(by_sin, slots, ahead)

    def y_ahead(chunk):
        z_route.arrive((chunk,), chunk)
        columns = [z_recv[chunk, :, f].reshape(length_y, LANES) for f in range(members)]
        product = along_y(z_route, chunk, jnp.concatenate(columns, 1), True)
        for row in range(0, rows_m, 16):
            arrays = []
            for f in range(members):
                for block in range(blocks):
                    arrays.append(combined(product, f, block * rows_m + row, 16, True))
            moved = exchange(arrays, 1)
            for rank in range(slots):
                x_send[chunk, rank, pl.ds(row, 16)] = moved[rank]
        x_route.start((chunk,), chunk)

    def gathered(ref, chunk):
        pieces = [[] for _ in range(slots)]
        for row in range(0, rows_m, 16):
            moved = exchange([ref[chunk, s, pl.ds(row, 16)] for s in range(slots)], 1)
            for index in range(slots):
                pieces[index].append(moved[index])
        return [jnp.concatenate(piece, 0) for piece in pieces]

    def along_x(values, table):
        product = mm(jnp.concatenate(halves(values), 1), table[...])
        return product[:, :LANES] + product[:, LANES:]

    def x_both(chunk):
        x_route.arrive((chunk,), chunk)
        values = along_x(jnp.concatenate(gathered(x_recv, chunk), 0), x_ahead)
        scaled = []
        for f in range(members):
            for block in range(blocks):
                at = (f * blocks + block) * rows_m
                table = other[block] if f == 1 and chunk == 0 else tables[chunk, block]
                scaled.append(values[at : at + rows_m] * table)
        values = along_x(jnp.concatenate(scaled, 0), x_back)
        for row in range(0, rows_m, 16):
            arrays = [values[a * rows_m + row : a * rows_m + row + 16] for a in range(slots)]
            moved = exchange(arrays, 1)
            for s in range(slots):
                w_send[chunk, s, pl.ds(row, 16)] = moved[s]
        w_route.start((chunk,), chunk)

    def y_back(chunk):
        w_route.arrive((chunk,), chunk)
        arrays = gathered(w_recv, chunk)
        columns = [
            jnp.concatenate(arrays[f * blocks : (f + 1) * blocks], 0) for f in range(members)
        ]
        product = along_y(w_route, chunk, jnp.concatenate(columns, 1), False)
        for f in range(members):
            for p in range(ranks_y):
                b_send[chunk, f, p] = combined(product, f, p * cells_y, cells_y, False)
            b_route.start((chunk, f), chunk * members + f)

    def spectrum_tables():
        t_route.arrive((), None)
        for row in range(0, rows_m, 8):
            rows = pl.ds(row, 8)
            moved = exchange([t_recv[s, rows] for s in range(slots)], 2)
            even = lane % 2 == 0
            for tile in range(tiles):
                for block in range(blocks):
                    part = moved[tile * blocks + block]
                    first = jnp.where(even, part, pltpu.roll(part, 1, 1))
                    second = jnp.where(even, pltpu.roll(part, LANES - 1, 1), part)
                    tables[tile * per_tile, block, rows] = first
                    tables[tile * per_tile + 1, block, rows] = second
                    if tile == 0:
                        other[block, rows] = first

        @pl.when((me_y == 0) & (me_x == 0))
        def _():
            spot = m_recv.at[pl.ds(1, slots - 1)]
            pltpu.make_async_remote_copy(
                src_ref=spot, dst_ref=spot, send_sem=send_sem.at[9], recv_sem=s_sem.at[3],
                device_id={"px": 1}, device_id_type=MESH,
            ).wait_recv()
            for p in range(ranks_y):
                strips = [n_recv[p] if s == 0 else m_recv[s, p] for s in range(slots)]
                for part in range(cells_y // 8):
                    value = strips[part]
                    for s in range(slots):
                        shift = (s - part) * 2 % LANES
                        moved = pltpu.roll(strips[s], shift, 1) if shift else strips[s]
                        value = jnp.where(quarter == s, moved, value)
                    at = p * cells_y + part * 8
                    other[at // rows_m, pl.ds(at % rows_m, 8)] = value

    for copy in copies[4:]:
        copy.wait()
    y_ahead(0)
    spectrum_tables()
    for step in range(1, chunks + 2):
        if step < chunks:
            y_ahead(step)
        if 0 <= step - 1 < chunks:
            x_both(step - 1)
        if 0 <= step - 2 < chunks:
            y_back(step - 2)

    low_rows = lax.broadcasted_iota(jnp.int32, (8, LANES), 0)
    tall = cells // 4 // ranks_y
    stores = []

    def z_back(f):
        arriving = [(chunk, f) for chunk in range(1, chunks)]
        for chunk, g in arriving + ([(0, g) for g in range(members)] if f == 0 else []):
            b_route.arrive((chunk, g), chunk * members + g)
        for tile in range(tiles):
            for row in range(0, cells_y, 8):
                rows = pl.ds(row, 8)
                arrays = []
                for group in range(cells_x):
                    chunk = tile * per_tile + group // ranks_y
                    arrays.append(b_recv[chunk, f, group % ranks_y, rows])
                if tile == 0:
                    pair = [b_recv[0, 0, 0, rows], b_recv[0, 1, 0, rows]]
                    arrays[0] = swap_slot(*pair, slots)[f]
                moved = exchange(arrays, width)
                for x in range(cells_x):
                    at = pl.ds(x * cells_y + row, 8)
                    held[f, at, pl.ds(tile * LANES, LANES)] = moved[x]
        high, low = halves(held[f])
        fields = mm(high, back_hi[...]) + mm(high, back_lo[...]) + mm(low, back_hi[...])
        values = jnp.exp(0.5 * fields)
        modulus[f] = values.reshape(cells_x, cells_y, length_z)
        store = pltpu.make_async_copy(modulus.at[f], modulus_out.at[f], store_sem.at[f])
        store.start()
        stores.append(store)
        high, low = halves(values)
        pooled = mm(pool_rows[...], high) + mm(pool_rows[...], low)
        high, low = halves(pooled)
        coarse = mm(high, pool_columns[...]) + mm(low, pool_columns[...])
        for d in range(ranks_y):
            at = ranks_y * tall + d * 8
            c_send[f, d, pl.ds(0, tall)] = coarse[d * tall : (d + 1) * tall, :LANES]
            c_send[f, d, pl.ds(tall, 8)] = coarse[at : at + 8, LANES:]
        c_routes[f].start((), None)

    def pick(f):
        c_routes[f].arrive((), None)
        for g in range(ranks_y):
            d_send[f, g, pl.ds(0, tall)] = c_recv[f][group_table[0, g], pl.ds(0, tall)]
            second = c_recv[f][group_table[1, g], pl.ds(tall, 8)]
            third = c_recv[f][group_table[2, g], pl.ds(tall, 8)]
            d_send[f, g, pl.ds(tall, 8)] = jnp.where(low_rows < 4, second, third)
        d_route.start((f,), f)

    def place_levels(f):
        d_route.arrive((f,), f)
        for d in range(ranks_y):
            level_one[f, d] = d_recv[f, d, pl.ds(0, tall)]
        lows = [d_recv[f, d, pl.ds(tall, 8)] for d in range(ranks_y)]
        half_y = cells_y // 4
        for x in range(ranks_y // 2):
            value = jnp.where(low_rows < 4, lows[2 * x], pltpu.roll(lows[2 * x + 1], 4, 0))
            level_two[f, x] = value[:half_y, : length_z // 4]
        for x in range(ranks_y // 4):
            value = lows[4 * x]
            for y in range(4):
                value = jnp.where(low_rows == y, pltpu.roll(lows[4 * x + y], (y + 4) % 8, 0), value)
            value = pltpu.roll(value, LANES // 2, 1)
            level_three[f, x] = value[: half_y // 2, : length_z // 8]

    z_back(0)
    z_back(1)
    pick(0)
    pick(1)
    place_levels(0)
    place_levels(1)

    every = pl.ds(0, chunks)
    z_route.drain((every,))
    x_route.drain((every,))
    w_route.drain((every,))
    b_route.drain((every, pl.ds(0, members)))
    s_route.drain(())
    t_route.drain(())
    spot = c_send.at[:, pl.ds(0, ranks_y - 1)]
    c_routes[0].copy(spot, spot, away_y[0], None).wait_send()
    d_route.drain((pl.ds(0, members),))
    pl.when(me_y != 0)(lambda: strip_copy().wait_send())
    pl.when((me_y == 0) & (me_x != 0))(lambda: strips_copy(me_x).wait_send())
    for store in stores:
        store.wait()


def lanes_path(white_noise, spectrum, group_table):
    members, cells_x, cells_y, length_z = white_noise.shape
    size_px, size_py = lax.axis_size("px"), lax.axis_size("py")
    length_x, length_y = cells_x * size_px, cells_y * size_py
    slots, width = size_px, 2 * size_px
    tiles = length_z // LANES
    per_tile = cells_x // size_py
    chunks = tiles * per_tile
    blocks = slots // members
    rows_m = length_y // blocks

    column = np.arange(length_z)
    tile, lane = column // LANES, column % LANES
    part = (lane // slots) % 2
    group = lane // width
    rank_q, rank_p, inner = lane % slots, group % size_py, group // size_py
    k = ((tile * size_py + rank_p) * slots + rank_q) * per_tile + inner
    angles = angles_of(length_z)
    sign = np.where(np.arange(length_z) % 2 == 0, 1.0, -1.0)
    z_ahead = np.where(part == 0, np.cos(angles[:, k]), -np.sin(angles[:, k]))
    z_back = 2.0 * z_ahead
    first = (k == 0) & (part == 0)
    second = (k == 0) & (part == 1)
    z_ahead[:, second] = sign[:, None]
    z_back[:, first] = 1.0
    z_back[:, second] = sign[:, None]
    z_back = z_back.T / (length_x * length_y * length_z)

    angles = angles_of(length_y)
    y_table = np.concatenate([np.cos(angles), np.sin(angles)], 0)

    lane = np.arange(LANES)
    cell = (lane // slots % 2, lane % slots * cells_x + lane // width)
    mode = (lane % 2, lane // 2 % slots * cells_x + lane // width)

    def x_table(direction, rows, columns):
        table = complex_array(length_x, direction)[rows][:, columns[0], columns[1]]
        high, low = host_halves(table)
        return jnp.concatenate(
            [
                jnp.concatenate([high, low], 1),
                jnp.concatenate([high, jnp.zeros_like(low)], 1),
            ],
            0,
        )

    def pool(extent_x, extent_y, factor):
        short_x, short_y = extent_x // factor, extent_y // factor
        row, cell = np.arange(short_x * short_y), np.arange(extent_x * extent_y)
        same_x = cell[None] // extent_y // factor == row[:, None] // short_y
        same_y = cell[None] % extent_y // factor == row[:, None] % short_y
        return np.where(same_x & same_y, 1.0 / factor**3, 0.0)

    second, third = pool(cells_x, cells_y, 4), pool(cells_x, cells_y, 8)
    lower = np.zeros((size_py, 8, cells_x * cells_y))
    lower[:, :4] = second.reshape(size_py, 4, -1)
    lower[:, 4:5] = third.reshape(size_py, 1, -1)
    pool_rows = np.concatenate([pool(cells_x, cells_y, 2), lower.reshape(8 * size_py, -1)], 0)
    pool_columns = np.zeros((length_z, 2 * LANES))
    z = np.arange(length_z)
    pool_columns[z, z // 2] = 1.0
    pool_columns[z, LANES + z // 4] = 1.0
    pool_columns[z, LANES + length_z // 4 + z // 8] = 1.0

    held_in = [
        spectrum,
        white_noise,
        *host_halves(z_ahead),
        *host_halves(y_table),
        x_table(-1.0, cell, mode),
        x_table(1.0, mode, cell),
        *host_halves(z_back),
        jnp.asarray(pool_rows, BF16),
        jnp.asarray(pool_columns, BF16),
    ]
    sizes = (cells_x, cells_y, length_z, slots, size_py)

    def body(*refs):
        whole_kernel(sizes, len(held_in), *refs)

    def vmem(*shape):
        return pltpu.VMEM(shape, F32)

    z_shape = (chunks, size_py, members, cells_y, LANES)
    x_shape = (chunks, slots, rows_m, LANES)
    b_shape = (chunks, members, size_py, cells_y, LANES)
    s_shape = (size_py, tiles, cells_y, LANES)
    t_shape = (slots, rows_m, LANES)
    height = cells_x * cells_y // 4 // size_py + 8
    c_shape = (members, size_py, height, LANES)
    sem = pltpu.SemaphoreType.DMA
    scratch = [pltpu.VMEM(value.shape, value.dtype) for value in held_in]
    for shape in (z_shape, x_shape, x_shape, b_shape, s_shape, t_shape):
        scratch += [vmem(*shape), vmem(*shape)]
    scratch += [vmem(8, LANES), vmem(size_py, 8, LANES), vmem(slots, size_py, 8, LANES)]
    scratch += [
        vmem(chunks, blocks, rows_m, LANES),
        vmem(blocks, rows_m, LANES),
        vmem(members, cells_x * cells_y, length_z),
        vmem(*white_noise.shape),
        vmem(*c_shape),
        vmem(*c_shape[1:]),
        vmem(*c_shape[1:]),
        vmem(*c_shape),
        vmem(*c_shape),
    ]
    scratch += [
        sem((len(held_in),)), sem((members,)), sem((10,)), sem((chunks,)), sem((chunks,)),
        sem((chunks,)), sem((chunks * members,)), sem((members,)), sem((members,)), sem((4,)),
    ]
    outs = [white_noise.shape]
    for level in range(1, 4):
        outs.append((members,) + tuple(extent >> level for extent in white_noise.shape[1:]))
    hbm = pl.BlockSpec(memory_space=pl.ANY)
    local = pl.BlockSpec(memory_space=pltpu.VMEM)
    return tuple(
        pl.pallas_call(
            body,
            out_shape=[jax.ShapeDtypeStruct(shape, F32) for shape in outs],
            in_specs=[pl.BlockSpec(memory_space=pltpu.SMEM)] + [hbm] * len(held_in),
            out_specs=[hbm, local, local, local],
            scratch_shapes=scratch,
            compiler_params=pltpu.CompilerParams(
                collective_id=0, has_side_effects=True, vmem_limit_bytes=56 * 1024 * 1024
            ),
        )(group_table, *held_in)
    )


def on_device(white_noise, spectrum, group_table):
    members, cells_x, cells_y, length_z = white_noise.shape
    size_px, size_py = lax.axis_size("px"), lax.axis_size("py")
    fits = members == 2 and length_z == 2 * LANES and size_px == 4 and size_py == 8
    fits = fits and 2 * cells_x * size_px == LANES and cells_x == 2 * size_py
    fits = fits and cells_y == 2 * cells_x
    chosen = lanes_path if fits else general_path
    return chosen(white_noise, spectrum, group_table)


def solution(mesh):
    in_specs = (P(None, "px", "py", None), P("px", "py", None), P())
    out_specs = (P(None, "px", "py", None),) * 4
    return jax.shard_map(
        on_device, mesh=mesh, in_specs=in_specs, out_specs=out_specs, check_vma=False
    )
```

```python
import numpy as np

import jax
import jax.numpy as jnp
from jax import lax
from jax.experimental import pallas as pl
from jax.experimental.pallas import tpu as pltpu
from jax.sharding import PartitionSpec as P


def angles_of(length):
    positions = np.arange(length, dtype=np.int64)
    return (positions[:, None] * positions[None, :] % length) * (2.0 * np.pi / length)


def complex_array(length, direction):
    angles = angles_of(length)
    cos, sin = np.cos(angles), direction * np.sin(angles)
    return np.stack([np.stack([cos, sin], 1), np.stack([-sin, cos], 1)], 0)


def complex_table(length, direction):
    return jnp.asarray(complex_array(length, direction), jnp.float32)


def half_tables(length):
    angles = angles_of(length)[:, : length // 2]
    ahead = np.stack([np.cos(angles), -np.sin(angles)], 1)
    back = 2.0 * ahead
    nyquist = np.where(np.arange(length) % 2 == 0, 1.0, -1.0)
    ahead[:, 1, 0] = nyquist
    back[:, 0, 0] = 1.0
    back[:, 1, 0] = nyquist
    return jnp.asarray(ahead, jnp.float32), jnp.asarray(back, jnp.float32)


def einsum(pattern, left, right):
    return jnp.einsum(pattern, left, right, precision=lax.Precision.HIGH)


def swap_first(values):
    first = values[:, :, :1]
    turned = jnp.swapaxes(first, 0, 1)
    return jnp.concatenate([turned, values[:, :, 1:]], 2)


def coarsen(values):
    members, size_x, size_y, size_z = values.shape
    blocks = values.reshape(members, size_x // 2, 2, size_y // 2, 2, size_z // 2, 2)
    return blocks.mean(axis=(2, 4, 6))


def general_path(white_noise, spectrum, group_table):
    members, cells_x, cells_y, length_z = white_noise.shape
    size_px, size_py = lax.axis_size("px"), lax.axis_size("py")
    length_x, length_y = cells_x * size_px, cells_y * size_py
    half_z = length_z // 2
    block_py, block = half_z // size_py, half_z // size_py // size_px
    z_ahead, z_back = half_tables(length_z)
    scale = 1.0 / (length_x * length_y * length_z)

    table = jnp.transpose(spectrum, (2, 0, 1))
    last = jnp.broadcast_to(table[half_z : half_z + 1], (size_py, 1, cells_x, cells_y))
    table = jnp.concatenate([table[:half_z].reshape(size_py, block_py, cells_x, cells_y), last], 1)
    table = lax.all_to_all(table, "py", split_axis=0, concat_axis=3, tiled=True)[0]
    last = jnp.broadcast_to(table[block_py:], (size_px, 1, cells_x, length_y))
    table = jnp.concatenate([table[:block_py].reshape(size_px, block, cells_x, length_y), last], 1)
    table = lax.all_to_all(table, "px", split_axis=0, concat_axis=2, tiled=True)[0] * scale
    is_first = (lax.axis_index("px") == 0) & (lax.axis_index("py") == 0)
    other = jnp.where(is_first, table[block:], table[:1])
    tables = jnp.stack([table[:block], jnp.concatenate([other, table[1:block]], 0)], 0)

    values = einsum("fxyz,zck->fckxy", white_noise, z_ahead)
    values = swap_first(values)
    values = lax.all_to_all(values, "py", split_axis=2, concat_axis=4, tiled=True)
    values = einsum("fckxy,cydm->fdkxm", values, complex_table(length_y, -1.0))
    values = lax.all_to_all(values, "px", split_axis=2, concat_axis=3, tiled=True)
    values = einsum("fckxm,cxdj->fdkjm", values, complex_table(length_x, -1.0))
    values = values * tables[:, None]
    values = einsum("fckjm,cjdx->fdkxm", values, complex_table(length_x, 1.0))
    values = lax.all_to_all(values, "px", split_axis=3, concat_axis=2, tiled=True)
    values = einsum("fckxm,cmdy->fdkxy", values, complex_table(length_y, 1.0))
    values = lax.all_to_all(values, "py", split_axis=4, concat_axis=2, tiled=True)
    values = swap_first(values)
    fields = einsum("fckxy,zck->fxyz", values, z_back)
    modulus = jnp.exp(0.5 * fields)

    levels = []
    level = modulus
    for _ in range(3):
        level = coarsen(level)
        levels.append(level)
    pieces = [jnp.reshape(level, (size_py, -1)) for level in levels]
    widths = [piece.shape[1] for piece in pieces]
    joined = jnp.concatenate(pieces, 1)
    spread = lax.all_to_all(joined, "py", split_axis=0, concat_axis=0, tiled=True)
    picked, start = [], 0
    for index, width in enumerate(widths):
        part = spread[:, start : start + width]
        picked.append(jnp.take(part, group_table[index], axis=0))
        start += width
    joined = lax.all_to_all(
        jnp.concatenate(picked, 1), "py", split_axis=0, concat_axis=0, tiled=True
    )
    routed, start = [], 0
    for level, width in zip(levels, widths):
        routed.append(joined[:, start : start + width].reshape(level.shape))
        start += width
    return (modulus, routed[0], routed[1], routed[2])


LANES = 128
PARTS = 2
MESH = pl.DeviceIdType.MESH
BF16 = jnp.bfloat16
F32 = jnp.float32


def halves(values):
    high = values.astype(BF16)
    low = (values - high.astype(F32)).astype(BF16)
    return high, low


def host_halves(values):
    values = np.asarray(values, np.float64)
    high = values.astype(np.float32).astype(BF16)
    low = (values - high.astype(np.float64)).astype(np.float32).astype(BF16)
    return jnp.asarray(high), jnp.asarray(low)


def mm(left, right):
    return jnp.dot(left, right, preferred_element_type=F32)


def lane_of(shape):
    return lax.broadcasted_iota(jnp.int32, shape, len(shape) - 1)


def exchange(arrays, width):
    arrays = list(arrays)
    lane = lane_of(arrays[0].shape)
    distance = 1
    while distance < len(arrays):
        step = distance * width
        low = (lane // step) % 2 == 0
        for index in range(len(arrays)):
            if (index // distance) % 2 == 0:
                first, second = arrays[index], arrays[index + distance]
                arrays[index] = jnp.where(low, first, pltpu.roll(second, step, 1))
                arrays[index + distance] = jnp.where(
                    low, pltpu.roll(first, LANES - step, 1), second
                )
        distance *= 2
    return arrays


def turned(values, slots, ahead):
    real = (lane_of(values.shape) // slots) % 2 == 0
    from_imag = pltpu.roll(values, LANES - slots, 1)
    from_real = pltpu.roll(values, slots, 1)
    if ahead:
        return jnp.where(real, from_imag, -from_real)
    return jnp.where(real, -from_imag, from_real)


def swap_slot(first, second, slots):
    place = lane_of(first.shape) % (2 * slots)
    return (
        jnp.where(place == slots, pltpu.roll(second, slots, 1), first),
        jnp.where(place == 0, pltpu.roll(first, LANES - slots, 1), second),
    )


class Route:
    def __init__(self, axis, count, away, source, target, send, recv):
        self.axis, self.count, self.away = axis, count, away
        self.source, self.target = source, target
        self.send, self.recv = send, recv
        self.me = lax.axis_index(axis)

    def copy(self, source, target, peer, part):
        return pltpu.make_async_remote_copy(
            src_ref=source,
            dst_ref=target,
            send_sem=self.send,
            recv_sem=self.recv.at[part] if part is not None else self.recv,
            device_id={self.axis: peer},
            device_id_type=MESH,
        )

    def at(self, ref, where, index):
        return ref.at[where + (index,)]

    def start(self, where, part):
        for peer in self.away:
            source = self.at(self.source, where, peer)
            target = self.at(self.target, where, self.me)
            self.copy(source, target, peer, part).start()

    def arrive(self, where, part):
        spot = self.at(self.target, where, pl.ds(0, self.count - 1))
        self.copy(spot, spot, self.away[0], part).wait_recv()
        self.target[where + (self.me,)] = self.source[where + (self.me,)]

    def drain(self, where):
        spot = self.source.at[where + (pl.ds(0, self.count - 1),)]
        self.copy(spot, spot, self.away[0], 0 if len(self.recv.shape) else None).wait_send()


def whole_kernel(sizes, loads, *refs):
    cells_x, cells_y, length_z, slots, ranks_y = sizes
    members = 2
    width = 2 * slots
    per_tile = cells_x // ranks_y
    tiles = length_z // LANES
    chunks = tiles * per_tile
    length_y = cells_y * ranks_y
    blocks = slots // members
    rows_m = length_y // blocks
    parts = PARTS
    rows_part = rows_m // parts
    sources, held_in = refs[:loads], refs[2 + loads : 2 + 2 * loads]
    modulus, d_recv = refs[loads : 2 + loads]
    (
        z_send, z_recv, x_send, x_recv, w_send, w_recv, b_send, b_recv,
        s_send, s_recv, e_recv, t_send, t_recv, n_send, n_recv, m_recv,
        tables, other, held, h_recv, c_send, c_recv_0, c_recv_1, d_send,
        load_sem, send_sem, z_sem, x_sem, w_sem, b_sem, c_sem, d_sem, s_sem, h_sem,
    ) = refs[2 + 2 * loads :]
    (
        spectrum, mirror_z, noise, ahead_hi, ahead_lo, mirror_x, mirror_y, y_hi, y_lo, x_ahead, x_back,
        back_hi, back_lo, pool_rows, pool_columns, group_table,
    ) = held_in

    me_x, me_y = lax.axis_index("px"), lax.axis_index("py")
    copies = [
        pltpu.make_async_copy(source, target, load_sem.at[index])
        for index, (source, target) in enumerate(zip(sources, held_in))
    ]
    for copy in copies:
        copy.start()

    place, core = me_y // 2, me_y % 2
    chips = ranks_y // 2
    near = chips - 1 - (chips - 2) * (place % 2)
    steps = [chips // 2, near, chips - near]
    away_y = []
    for step in steps:
        for side in (0, 1):
            away_y.append((place + step) % chips * 2 + (core + side) % 2)
    away_y.append(place * 2 + 1 - core)
    away_x = [slots - 1 - me_x, (me_x + 2) % slots, me_x + 1 - 2 * (me_x % 2)]

    barrier = pltpu.get_barrier_semaphore()
    for peer in away_y:
        pl.semaphore_signal(barrier, inc=1, device_id={"py": peer}, device_id_type=MESH)
    for peer in away_x:
        pl.semaphore_signal(barrier, inc=1, device_id={"px": peer}, device_id_type=MESH)

    def route(axis, source, target, send, recv):
        away, count = (away_y, ranks_y) if axis == "py" else (away_x, slots)
        return Route(axis, count, away, source, target, send_sem.at[send], recv)

    z_route = route("py", z_send, z_recv, 0, z_sem)
    x_route = route("px", x_send, x_recv, 1, x_sem)
    w_route = route("px", w_send, w_recv, 2, w_sem)
    b_route = route("py", b_send, b_recv, 3, b_sem)
    t_route = route("px", t_send, t_recv, 5, s_sem.at[1])
    c_recv = (c_recv_0, c_recv_1)
    c_routes = [route("py", c_send.at[f], c_recv[f], 6, c_sem.at[f]) for f in range(members)]
    d_route = route("py", d_send, d_recv, 7, d_sem)

    lane = lane_of((8, LANES))
    half_y = ranks_y // 2
    my_half, my_place = me_y // half_y, me_y % half_y
    copies[0].wait()
    copies[1].wait()
    mirrored = jnp.concatenate(
        halves(spectrum[:, :, LANES : 2 * LANES].reshape(cells_x * cells_y, LANES)), 1
    )
    held[0, :, pl.ds(0, LANES)] = mm(mirrored, mirror_z[...])
    for row in range(0, cells_y, 8):
        rows = pl.ds(row, 8)
        plain = [spectrum[x, rows, pl.ds(0, LANES)] for x in range(cells_x)]
        turned_z = []
        for x in range(cells_x):
            value = held[0, pl.ds(x * cells_y + row, 8), pl.ds(0, LANES)]
            turned_z.append(jnp.where(lane == 0, plain[x], value))
        for kind, arrays in enumerate((plain, turned_z)):
            moved = exchange(arrays, width)
            for group in range(cells_x):
                s_send[group % ranks_y, kind, group // ranks_y, rows] = moved[group]
    strip = jnp.zeros((8, LANES), F32)
    quarter = (lane // 2) % slots
    for x in range(cells_x):
        for part in range(cells_y // 8):
            value = spectrum[x, pl.ds(part * 8, 8), pl.ds(LANES, 1)]
            strip = jnp.where((lane // width == x) & (quarter == part), value, strip)
    n_send[...] = strip

    def strip_copy():
        return pltpu.make_async_remote_copy(
            src_ref=n_send, dst_ref=n_recv.at[me_y], send_sem=send_sem.at[8],
            recv_sem=s_sem.at[2], device_id={"py": 0}, device_id_type=MESH,
        )

    def half_copy(peer):
        return pltpu.make_async_remote_copy(
            src_ref=s_send.at[peer], dst_ref=s_recv.at[my_place], send_sem=send_sem.at[4],
            recv_sem=s_sem.at[0], device_id={"py": peer}, device_id_type=MESH,
        )

    def edge_copy(peer):
        return pltpu.make_async_remote_copy(
            src_ref=s_send.at[peer, 1, :, pl.ds(0, 8)], dst_ref=e_recv, send_sem=send_sem.at[10],
            recv_sem=s_sem.at[4], device_id={"py": peer}, device_id_type=MESH,
        )

    others = [my_half * half_y + (my_place + step) % half_y for step in range(1, half_y)]
    across = [(1 - my_half) * half_y + step for step in range(half_y)]

    def send_spectrum():
        pl.when(me_y != 0)(lambda: strip_copy().start())
        for peer in others[1:] + others[:1]:
            half_copy(peer).start()

        @pl.when(my_place == 0)
        def _():
            for peer in across:
                edge_copy(peer).start()

    middle = (place == chips // 2) | (place == chips // 2 - 1)
    giver, taker = middle & (core == 0), middle & (core == 1)

    def hand_copy(chunk):
        return pltpu.make_async_remote_copy(
            src_ref=z_send.at[chunk, pl.ds((1 - my_half) * half_y, half_y)],
            dst_ref=h_recv.at[chunk], send_sem=send_sem.at[0], recv_sem=h_sem.at[chunk],
            device_id={"py": place * 2 + 1 - core}, device_id_type=MESH,
        )

    def z_copy(source, chunk, slot, peer, send):
        return pltpu.make_async_remote_copy(
            src_ref=source, dst_ref=z_recv.at[chunk, slot], send_sem=send_sem.at[send],
            recv_sem=z_sem.at[chunk], device_id={"py": peer}, device_id_type=MESH,
        )

    def z_start(chunk):
        @pl.when(giver)
        def _():
            hand_copy(chunk).start()
            for peer in others:
                z_copy(z_send.at[chunk, peer], chunk, me_y, peer, 0).start()

        @pl.when(jnp.logical_not(giver))
        def _():
            z_route.start((chunk,), chunk)

        @pl.when(taker)
        def _():
            hand_copy(chunk).wait_recv()
            for step, peer in enumerate(across):
                z_copy(h_recv.at[chunk, step], chunk, me_y - 1, peer, 11).start()

    for copy in copies[2:6]:
        copy.wait()
    cells = cells_x * cells_y
    for f in range(members):
        high, low = halves(noise[f].reshape(cells, length_z))
        held[f] = mm(high, ahead_hi[...]) + mm(high, ahead_lo[...]) + mm(low, ahead_hi[...])
    for tile in range(tiles):
        lanes = pl.ds(tile * LANES, LANES)
        for row in range(0, cells_y, 8):
            rows = pl.ds(row, 8)
            both = []
            for f in range(members):
                both.append(
                    exchange(
                        [held[f, pl.ds(x * cells_y + row, 8), lanes] for x in range(cells_x)],
                        width,
                    )
                )
            if tile == 0:
                both[0][0], both[1][0] = swap_slot(both[0][0], both[1][0], slots)
            for f in range(members):
                for group in range(cells_x):
                    chunk = tile * per_tile + group // ranks_y
                    z_send[chunk, group % ranks_y, f, rows] = both[f][group]
        if tile == 0:
            pl.semaphore_wait(barrier, ranks_y + slots - 2)
            send_spectrum()
        for part in range(per_tile):
            chunk = tile * per_tile + part
            z_start(chunk)

    spot = s_recv.at[pl.ds(0, half_y - 1)]
    pltpu.make_async_remote_copy(
        src_ref=spot, dst_ref=spot, send_sem=send_sem.at[4], recv_sem=s_sem.at[0],
        device_id={"py": others[0]}, device_id_type=MESH,
    ).wait_recv()
    edge_copy(others[0]).wait_recv()
    s_recv[my_place] = s_send[me_y]
    copies[6].wait()
    copies[7].wait()
    pair = [s_recv[:, 1, tile].reshape(rows_m, LANES) for tile in range(tiles)]
    pair = jnp.concatenate(halves(jnp.concatenate(pair, 1)), 0)
    held[1, pl.ds(0, rows_m)] = mm(mirror_y[...], pair)
    sublane = lax.broadcasted_iota(jnp.int32, (8, LANES), 0)
    for row in range(0, rows_m, 8):
        arrays = []
        for tile in range(tiles):
            arrays.append(s_recv[row // cells_y, 0, tile, pl.ds(row % cells_y, 8)])
            value = held[1, pl.ds(row, 8), pl.ds(tile * LANES, LANES)]
            if row == 0:
                value = jnp.where(sublane == 0, e_recv[tile], value)
            arrays.append(value)
        moved = exchange(arrays, 2)
        for rank in range(slots):
            t_send[rank, pl.ds(row, 8)] = moved[rank]
    t_route.start((), None)

    def strips_copy(source):
        return pltpu.make_async_remote_copy(
            src_ref=n_recv, dst_ref=m_recv.at[source], send_sem=send_sem.at[9],
            recv_sem=s_sem.at[3], device_id={"px": 0}, device_id_type=MESH,
        )

    def along_y(route, part, columns, ahead):
        high, low = halves(columns)
        product = mm(y_hi[...], high) + mm(y_hi[...], low) + mm(y_lo[...], high)
        return product

    def combined(product, f, start, rows, ahead):
        lanes = slice(f * LANES, (f + 1) * LANES)
        by_cos = product[start : start + rows, lanes]
        by_sin = product[length_y + start : length_y + start + rows, lanes]
        return by_cos + turned(by_sin, slots, ahead)

    def y_ahead(chunk):
        z_route.arrive((chunk,), chunk)
        columns = [z_recv[chunk, :, f].reshape(length_y, LANES) for f in range(members)]
        product = along_y(z_route, chunk, jnp.concatenate(columns, 1), True)
        for part in range(parts):
            for row in range(0, rows_part, 16):
                arrays = []
                for f in range(members):
                    for block in range(blocks):
                        at = block * rows_m + part * rows_part + row
                        arrays.append(combined(product, f, at, 16, True))
                moved = exchange(arrays, 1)
                for rank in range(slots):
                    x_send[chunk, part, rank, pl.ds(row, 16)] = moved[rank]
            x_route.start((chunk, part), chunk * parts + part)

    def gathered(ref, chunk, some):
        pieces = [[] for _ in range(slots)]
        for part in some:
            for row in range(0, rows_part, 16):
                moved = exchange([ref[chunk, part, s, pl.ds(row, 16)] for s in range(slots)], 1)
                for index in range(slots):
                    pieces[index].append(moved[index])
        return [jnp.concatenate(piece, 0) for piece in pieces]

    def along_x(values, table):
        product = mm(jnp.concatenate(halves(values), 1), table[...])
        return product[:, :LANES] + product[:, LANES:]

    def x_both(chunk):
        for part in range(parts):
            x_route.arrive((chunk, part), chunk * parts + part)
            values = along_x(jnp.concatenate(gathered(x_recv, chunk, [part]), 0), x_ahead)
            scaled = []
            rows = pl.ds(part * rows_part, rows_part)
            for f in range(members):
                for block in range(blocks):
                    at = (f * blocks + block) * rows_part
                    table = other if f == 1 and chunk == 0 else tables.at[chunk]
                    scaled.append(values[at : at + rows_part] * table[block, rows])
            values = along_x(jnp.concatenate(scaled, 0), x_back)
            for row in range(0, rows_part, 16):
                arrays = [
                    values[a * rows_part + row : a * rows_part + row + 16] for a in range(slots)
                ]
                moved = exchange(arrays, 1)
                for s in range(slots):
                    w_send[chunk, part, s, pl.ds(row, 16)] = moved[s]
            w_route.start((chunk, part), chunk * parts + part)

    def y_back(chunk):
        for part in range(parts):
            w_route.arrive((chunk, part), chunk * parts + part)
        arrays = gathered(w_recv, chunk, range(parts))
        columns = [
            jnp.concatenate(arrays[f * blocks : (f + 1) * blocks], 0) for f in range(members)
        ]
        product = along_y(w_route, chunk, jnp.concatenate(columns, 1), False)
        for f in range(members):
            for p in range(ranks_y):
                b_send[chunk, f, p] = combined(product, f, p * cells_y, cells_y, False)
            b_route.start((chunk, f), chunk * members + f)

    def table_rows(tile, block, rows, part):
        even = lane % 2 == 0
        first = jnp.where(even, part, pltpu.roll(part, 1, 1))
        second = jnp.where(even, pltpu.roll(part, LANES - 1, 1), part)
        tables[tile * per_tile, block, rows] = first
        tables[tile * per_tile + 1, block, rows] = second
        if tile == 0:
            other[block, rows] = first

    def spectrum_tables():
        t_route.arrive((), None)
        images = [[] for _ in range(tiles)]
        for row in range(0, rows_m, 8):
            rows = pl.ds(row, 8)
            moved = exchange([t_recv[s, rows] for s in range(slots)], 2)
            for tile in range(tiles):
                table_rows(tile, my_half, rows, moved[2 * tile])
                images[tile].append(moved[2 * tile + 1])
        images = jnp.concatenate([piece for pieces in images for piece in pieces], 0)
        images = mm(jnp.concatenate(halves(images), 1), mirror_x[...])
        for tile in range(tiles):
            for row in range(0, rows_m, 8):
                at = tile * rows_m + row
                table_rows(tile, 1 - my_half, pl.ds(row, 8), images[at : at + 8])

        @pl.when((me_y == 0) & (me_x == 0))
        def _():
            spot = m_recv.at[pl.ds(1, slots - 1)]
            pltpu.make_async_remote_copy(
                src_ref=spot, dst_ref=spot, send_sem=send_sem.at[9], recv_sem=s_sem.at[3],
                device_id={"px": 1}, device_id_type=MESH,
            ).wait_recv()
            for p in range(ranks_y):
                strips = [n_recv[p] if s == 0 else m_recv[s, p] for s in range(slots)]
                for part in range(cells_y // 8):
                    value = strips[part]
                    for s in range(slots):
                        shift = (s - part) * 2 % LANES
                        moved = pltpu.roll(strips[s], shift, 1) if shift else strips[s]
                        value = jnp.where(quarter == s, moved, value)
                    at = p * cells_y + part * 8
                    other[at // rows_m, pl.ds(at % rows_m, 8)] = value

    @pl.when(me_y == 0)
    def _():
        spot = n_recv.at[pl.ds(0, ranks_y - 1)]
        pltpu.make_async_remote_copy(
            src_ref=spot, dst_ref=spot, send_sem=send_sem.at[8], recv_sem=s_sem.at[2],
            device_id={"py": 1}, device_id_type=MESH,
        ).wait_recv()
        n_recv[0] = n_send[...]
        pl.when(me_x != 0)(lambda: strips_copy(me_x).start())

    for copy in copies[8:]:
        copy.wait()
    y_ahead(0)
    spectrum_tables()
    for chunk in range(chunks):
        x_both(chunk)
        if chunk + 1 < chunks:
            y_ahead(chunk + 1)
        y_back(chunk)

    low_rows = lax.broadcasted_iota(jnp.int32, (8, LANES), 0)
    tall = cells // 4 // ranks_y

    def z_back(f):
        arriving = [(chunk, f) for chunk in range(1, chunks)]
        for chunk, g in arriving + ([(0, g) for g in range(members)] if f == 0 else []):
            b_route.arrive((chunk, g), chunk * members + g)
        for tile in range(tiles):
            for row in range(0, cells_y, 8):
                rows = pl.ds(row, 8)
                arrays = []
                for group in range(cells_x):
                    chunk = tile * per_tile + group // ranks_y
                    arrays.append(b_recv[chunk, f, group % ranks_y, rows])
                if tile == 0:
                    pair = [b_recv[0, 0, 0, rows], b_recv[0, 1, 0, rows]]
                    arrays[0] = swap_slot(*pair, slots)[f]
                moved = exchange(arrays, width)
                for x in range(cells_x):
                    at = pl.ds(x * cells_y + row, 8)
                    held[f, at, pl.ds(tile * LANES, LANES)] = moved[x]
        high, low = halves(held[f])
        fields = mm(high, back_hi[...]) + mm(high, back_lo[...]) + mm(low, back_hi[...])
        values = jnp.exp(0.5 * fields)
        modulus[f] = values.reshape(cells_x, cells_y, length_z)
        high, low = halves(values)
        pooled = mm(pool_rows[...], high) + mm(pool_rows[...], low)
        high, low = halves(pooled)
        coarse = mm(high, pool_columns[...]) + mm(low, pool_columns[...])
        for d in range(ranks_y):
            at = ranks_y * tall + d * 8
            c_send[f, d, pl.ds(0, tall)] = coarse[d * tall : (d + 1) * tall, :LANES]
            c_send[f, d, pl.ds(tall, 8)] = coarse[at : at + 8, LANES:]
        c_routes[f].start((), None)

    def pick(f):
        c_routes[f].arrive((), None)
        for g in range(ranks_y):
            d_send[f, g, pl.ds(0, tall)] = c_recv[f][group_table[0, g], pl.ds(0, tall)]
            second = c_recv[f][group_table[1, g], pl.ds(tall, 8)]
            third = c_recv[f][group_table[2, g], pl.ds(tall, 8)]
            d_send[f, g, pl.ds(tall, 8)] = jnp.where(low_rows < 4, second, third)
        d_route.start((f,), f)

    z_back(0)
    z_back(1)
    pick(0)
    pick(1)
    d_route.arrive((0,), 0)
    d_route.arrive((1,), 1)

    every = pl.ds(0, chunks)
    z_route.drain((every,))

    @pl.when(taker)
    def _():
        pltpu.make_async_remote_copy(
            src_ref=h_recv, dst_ref=h_recv, send_sem=send_sem.at[11], recv_sem=h_sem.at[0],
            device_id={"py": others[0]}, device_id_type=MESH,
        ).wait_send()

    x_route.drain((every, pl.ds(0, parts)))
    w_route.drain((every, pl.ds(0, parts)))
    b_route.drain((every, pl.ds(0, members)))
    spot = s_send.at[pl.ds(0, half_y - 1)]
    pltpu.make_async_remote_copy(
        src_ref=spot, dst_ref=spot, send_sem=send_sem.at[4], recv_sem=s_sem.at[0],
        device_id={"py": others[0]}, device_id_type=MESH,
    ).wait_send()

    @pl.when(my_place == 0)
    def _():
        spot = s_send.at[pl.ds(0, half_y), 1, :, pl.ds(0, 8)]
        pltpu.make_async_remote_copy(
            src_ref=spot, dst_ref=spot, send_sem=send_sem.at[10], recv_sem=s_sem.at[4],
            device_id={"py": others[0]}, device_id_type=MESH,
        ).wait_send()

    t_route.drain(())
    spot = c_send.at[:, pl.ds(0, ranks_y - 1)]
    c_routes[0].copy(spot, spot, away_y[0], None).wait_send()
    d_route.drain((pl.ds(0, members),))
    pl.when(me_y != 0)(lambda: strip_copy().wait_send())
    pl.when((me_y == 0) & (me_x != 0))(lambda: strips_copy(me_x).wait_send())


def leaving_kernel(modulus, coarse, modulus_out, one_out, level_two, level_three, sems):
    members, cells_x, cells_y, length_z = modulus.shape
    ranks_y, tall = coarse.shape[1], coarse.shape[2] - 8
    copies = [
        pltpu.make_async_copy(modulus.at[f], modulus_out.at[f], sems.at[f]) for f in range(members)
    ]
    copies.append(
        pltpu.make_async_copy(coarse.at[:, :, pl.ds(0, tall)], one_out, sems.at[members])
    )
    for copy in copies:
        copy.start()
    low_rows = lax.broadcasted_iota(jnp.int32, (8, LANES), 0)
    short = cells_y // 4
    for f in range(members):
        lows = [coarse[f, d, pl.ds(tall, 8)] for d in range(ranks_y)]
        for x in range(ranks_y // 2):
            value = jnp.where(low_rows < 4, lows[2 * x], pltpu.roll(lows[2 * x + 1], 4, 0))
            level_two[f, x] = value[:short, : length_z // 4]
        for x in range(ranks_y // 4):
            value = lows[4 * x]
            for y in range(4):
                value = jnp.where(low_rows == y, pltpu.roll(lows[4 * x + y], (y + 4) % 8, 0), value)
            value = pltpu.roll(value, LANES // 2, 1)
            level_three[f, x] = value[: short // 2, : length_z // 8]
    for copy in copies:
        copy.wait()


def lanes_path(white_noise, spectrum, group_table):
    members, cells_x, cells_y, length_z = white_noise.shape
    size_px, size_py = lax.axis_size("px"), lax.axis_size("py")
    length_x, length_y = cells_x * size_px, cells_y * size_py
    slots, width = size_px, 2 * size_px
    tiles = length_z // LANES
    per_tile = cells_x // size_py
    chunks = tiles * per_tile
    blocks = slots // members
    rows_m = length_y // blocks

    column = np.arange(length_z)
    tile, lane = column // LANES, column % LANES
    part = (lane // slots) % 2
    group = lane // width
    rank_q, rank_p, inner = lane % slots, group % size_py, group // size_py
    k = ((tile * size_py + rank_p) * slots + rank_q) * per_tile + inner
    angles = angles_of(length_z)
    sign = np.where(np.arange(length_z) % 2 == 0, 1.0, -1.0)
    z_ahead = np.where(part == 0, np.cos(angles[:, k]), -np.sin(angles[:, k]))
    z_back = 2.0 * z_ahead
    first = (k == 0) & (part == 0)
    second = (k == 0) & (part == 1)
    z_ahead[:, second] = sign[:, None]
    z_back[:, first] = 1.0
    z_back[:, second] = sign[:, None]
    z_back = z_back.T / (length_x * length_y * length_z)

    angles = angles_of(length_y)
    y_table = np.concatenate([np.cos(angles), np.sin(angles)], 0)

    lane = np.arange(LANES)
    cell = (lane // slots % 2, lane % slots * cells_x + lane // width)
    mode = (lane % 2, lane // 2 % slots * cells_x + lane // width)

    def x_table(direction, rows, columns):
        table = complex_array(length_x, direction)[rows][:, columns[0], columns[1]]
        high, low = host_halves(table)
        return jnp.concatenate(
            [
                jnp.concatenate([high, low], 1),
                jnp.concatenate([high, jnp.zeros_like(low)], 1),
            ],
            0,
        )

    at = np.arange(1, LANES)
    mirror_z = np.zeros((LANES, LANES))
    mirror_z[LANES - at, at] = 1.0
    at = np.arange(1, rows_m)
    mirror_y = np.zeros((rows_m, rows_m))
    mirror_y[at, rows_m - at] = 1.0
    same = (mode[1][:, None] + mode[1][None]) % length_x == 0
    mirror_x = np.where(same & (mode[0][:, None] == mode[0][None]), 1.0, 0.0)

    def pool(extent_x, extent_y, factor):
        short_x, short_y = extent_x // factor, extent_y // factor
        row, cell = np.arange(short_x * short_y), np.arange(extent_x * extent_y)
        same_x = cell[None] // extent_y // factor == row[:, None] // short_y
        same_y = cell[None] % extent_y // factor == row[:, None] % short_y
        return np.where(same_x & same_y, 1.0 / factor**3, 0.0)

    second, third = pool(cells_x, cells_y, 4), pool(cells_x, cells_y, 8)
    lower = np.zeros((size_py, 8, cells_x * cells_y))
    lower[:, :4] = second.reshape(size_py, 4, -1)
    lower[:, 4:5] = third.reshape(size_py, 1, -1)
    pool_rows = np.concatenate([pool(cells_x, cells_y, 2), lower.reshape(8 * size_py, -1)], 0)
    pool_columns = np.zeros((length_z, 2 * LANES))
    z = np.arange(length_z)
    pool_columns[z, z // 2] = 1.0
    pool_columns[z, LANES + z // 4] = 1.0
    pool_columns[z, LANES + length_z // 4 + z // 8] = 1.0

    held_in = [
        spectrum,
        jnp.asarray(np.tile(mirror_z, (2, 1)), BF16),
        white_noise,
        *host_halves(z_ahead),
        jnp.asarray(np.tile(mirror_x, (2, 1)), BF16),
        jnp.asarray(np.tile(mirror_y, (1, 2)), BF16),
        *host_halves(y_table),
        x_table(-1.0, cell, mode),
        x_table(1.0, mode, cell),
        *host_halves(z_back),
        jnp.asarray(pool_rows, BF16),
        jnp.asarray(pool_columns, BF16),
        group_table,
    ]
    sizes = (cells_x, cells_y, length_z, slots, size_py)

    def body(*refs):
        whole_kernel(sizes, len(held_in), *refs)

    def vmem(*shape):
        return pltpu.VMEM(shape, F32)

    z_shape = (chunks, size_py, members, cells_y, LANES)
    x_shape = (chunks, PARTS, slots, rows_m // PARTS, LANES)
    b_shape = (chunks, members, size_py, cells_y, LANES)
    s_shape = (2, tiles, cells_y, LANES)
    t_shape = (slots, rows_m, LANES)
    height = cells_x * cells_y // 4 // size_py + 8
    c_shape = (members, size_py, height, LANES)
    sem = pltpu.SemaphoreType.DMA
    scratch = [pltpu.VMEM(value.shape, value.dtype) for value in held_in[:-1]]
    scratch.append(pltpu.SMEM(group_table.shape, group_table.dtype))
    for shape in (z_shape, x_shape, x_shape, b_shape):
        scratch += [vmem(*shape), vmem(*shape)]
    scratch += [vmem(size_py, *s_shape), vmem(size_py // 2, *s_shape), vmem(tiles, 8, LANES)]
    scratch += [vmem(*t_shape), vmem(*t_shape)]
    scratch += [vmem(8, LANES), vmem(size_py, 8, LANES), vmem(slots, size_py, 8, LANES)]
    scratch += [
        vmem(chunks, blocks, rows_m, LANES),
        vmem(blocks, rows_m, LANES),
        vmem(members, cells_x * cells_y, length_z),
        vmem(chunks, size_py // 2, members, cells_y, LANES),
        vmem(*c_shape),
        vmem(*c_shape[1:]),
        vmem(*c_shape[1:]),
        vmem(*c_shape),
    ]
    scratch += [
        sem((len(held_in),)), sem((12,)), sem((chunks,)), sem((chunks * PARTS,)),
        sem((chunks * PARTS,)), sem((chunks * members,)), sem((members,)), sem((members,)), sem((5,)), sem((chunks,)),
    ]
    hbm = pl.BlockSpec(memory_space=pltpu.HBM)
    local = pl.BlockSpec(memory_space=pltpu.VMEM)
    modulus, coarse = pl.pallas_call(
        body,
        out_shape=[jax.ShapeDtypeStruct(shape, F32) for shape in (white_noise.shape, c_shape)],
        in_specs=[hbm] * len(held_in),
        out_specs=[local, local],
        scratch_shapes=scratch,
        compiler_params=pltpu.CompilerParams(
            collective_id=0, has_side_effects=True, vmem_limit_bytes=40 * 1024 * 1024
        ),
    )(*[pltpu.with_memory_space_constraint(v, pltpu.HBM) for v in held_in])
    outs = [white_noise.shape]
    for level in range(1, 4):
        outs.append((members,) + tuple(extent >> level for extent in white_noise.shape[1:]))
    return tuple(
        pl.pallas_call(
            leaving_kernel,
            out_shape=[jax.ShapeDtypeStruct(shape, F32) for shape in outs],
            in_specs=[local, local],
            out_specs=[hbm, hbm, local, local],
            scratch_shapes=[sem((members + 1,))],
            compiler_params=pltpu.CompilerParams(vmem_limit_bytes=4 * 1024 * 1024),
        )(modulus, coarse)
    )


def on_device(white_noise, spectrum, group_table):
    members, cells_x, cells_y, length_z = white_noise.shape
    size_px, size_py = lax.axis_size("px"), lax.axis_size("py")
    fits = members == 2 and length_z == 2 * LANES and size_px == 4 and size_py == 8
    fits = fits and 2 * cells_x * size_px == LANES and cells_x == 2 * size_py
    fits = fits and cells_y == 2 * cells_x
    chosen = lanes_path if fits else general_path
    return chosen(white_noise, spectrum, group_table)


def solution(mesh):
    in_specs = (P(None, "px", "py", None), P("px", "py", None), P())
    out_specs = (P(None, "px", "py", None),) * 4
    return jax.shard_map(
        on_device, mesh=mesh, in_specs=in_specs, out_specs=out_specs, check_vma=False
    )
```

```python
import numpy as np

import jax
import jax.numpy as jnp
from jax import lax
from jax.experimental import pallas as pl
from jax.experimental.pallas import tpu as pltpu
from jax.sharding import PartitionSpec as P


def angles_of(length):
    positions = np.arange(length, dtype=np.int64)
    return (positions[:, None] * positions[None, :] % length) * (2.0 * np.pi / length)


def complex_array(length, direction):
    angles = angles_of(length)
    cos, sin = np.cos(angles), direction * np.sin(angles)
    return np.stack([np.stack([cos, sin], 1), np.stack([-sin, cos], 1)], 0)


def complex_table(length, direction):
    return jnp.asarray(complex_array(length, direction), jnp.float32)


def half_tables(length):
    angles = angles_of(length)[:, : length // 2]
    ahead = np.stack([np.cos(angles), -np.sin(angles)], 1)
    back = 2.0 * ahead
    nyquist = np.where(np.arange(length) % 2 == 0, 1.0, -1.0)
    ahead[:, 1, 0] = nyquist
    back[:, 0, 0] = 1.0
    back[:, 1, 0] = nyquist
    return jnp.asarray(ahead, jnp.float32), jnp.asarray(back, jnp.float32)


def einsum(pattern, left, right):
    return jnp.einsum(pattern, left, right, precision=lax.Precision.HIGH)


def swap_first(values):
    first = values[:, :, :1]
    turned = jnp.swapaxes(first, 0, 1)
    return jnp.concatenate([turned, values[:, :, 1:]], 2)


def coarsen(values):
    members, size_x, size_y, size_z = values.shape
    blocks = values.reshape(members, size_x // 2, 2, size_y // 2, 2, size_z // 2, 2)
    return blocks.mean(axis=(2, 4, 6))


def general_path(white_noise, spectrum, group_table):
    members, cells_x, cells_y, length_z = white_noise.shape
    size_px, size_py = lax.axis_size("px"), lax.axis_size("py")
    length_x, length_y = cells_x * size_px, cells_y * size_py
    half_z = length_z // 2
    block_py, block = half_z // size_py, half_z // size_py // size_px
    z_ahead, z_back = half_tables(length_z)
    scale = 1.0 / (length_x * length_y * length_z)

    table = jnp.transpose(spectrum, (2, 0, 1))
    last = jnp.broadcast_to(table[half_z : half_z + 1], (size_py, 1, cells_x, cells_y))
    table = jnp.concatenate([table[:half_z].reshape(size_py, block_py, cells_x, cells_y), last], 1)
    table = lax.all_to_all(table, "py", split_axis=0, concat_axis=3, tiled=True)[0]
    last = jnp.broadcast_to(table[block_py:], (size_px, 1, cells_x, length_y))
    table = jnp.concatenate([table[:block_py].reshape(size_px, block, cells_x, length_y), last], 1)
    table = lax.all_to_all(table, "px", split_axis=0, concat_axis=2, tiled=True)[0] * scale
    is_first = (lax.axis_index("px") == 0) & (lax.axis_index("py") == 0)
    other = jnp.where(is_first, table[block:], table[:1])
    tables = jnp.stack([table[:block], jnp.concatenate([other, table[1:block]], 0)], 0)

    values = einsum("fxyz,zck->fckxy", white_noise, z_ahead)
    values = swap_first(values)
    values = lax.all_to_all(values, "py", split_axis=2, concat_axis=4, tiled=True)
    values = einsum("fckxy,cydm->fdkxm", values, complex_table(length_y, -1.0))
    values = lax.all_to_all(values, "px", split_axis=2, concat_axis=3, tiled=True)
    values = einsum("fckxm,cxdj->fdkjm", values, complex_table(length_x, -1.0))
    values = values * tables[:, None]
    values = einsum("fckjm,cjdx->fdkxm", values, complex_table(length_x, 1.0))
    values = lax.all_to_all(values, "px", split_axis=3, concat_axis=2, tiled=True)
    values = einsum("fckxm,cmdy->fdkxy", values, complex_table(length_y, 1.0))
    values = lax.all_to_all(values, "py", split_axis=4, concat_axis=2, tiled=True)
    values = swap_first(values)
    fields = einsum("fckxy,zck->fxyz", values, z_back)
    modulus = jnp.exp(0.5 * fields)

    levels = []
    level = modulus
    for _ in range(3):
        level = coarsen(level)
        levels.append(level)
    pieces = [jnp.reshape(level, (size_py, -1)) for level in levels]
    widths = [piece.shape[1] for piece in pieces]
    joined = jnp.concatenate(pieces, 1)
    spread = lax.all_to_all(joined, "py", split_axis=0, concat_axis=0, tiled=True)
    picked, start = [], 0
    for index, width in enumerate(widths):
        part = spread[:, start : start + width]
        picked.append(jnp.take(part, group_table[index], axis=0))
        start += width
    joined = lax.all_to_all(
        jnp.concatenate(picked, 1), "py", split_axis=0, concat_axis=0, tiled=True
    )
    routed, start = [], 0
    for level, width in zip(levels, widths):
        routed.append(joined[:, start : start + width].reshape(level.shape))
        start += width
    return (modulus, routed[0], routed[1], routed[2])


LANES = 128
PARTS = 2
MESH = pl.DeviceIdType.MESH
BF16 = jnp.bfloat16
F32 = jnp.float32


def halves(values):
    high = values.astype(BF16)
    low = (values - high.astype(F32)).astype(BF16)
    return high, low


def host_halves(values):
    values = np.asarray(values, np.float64)
    high = values.astype(np.float32).astype(BF16)
    low = (values - high.astype(np.float64)).astype(np.float32).astype(BF16)
    return jnp.asarray(high), jnp.asarray(low)


def mm(left, right):
    return jnp.dot(left, right, preferred_element_type=F32)


def lane_of(shape):
    return lax.broadcasted_iota(jnp.int32, shape, len(shape) - 1)


def exchange(arrays, width):
    count = len(arrays)
    field = (lane_of(arrays[0].shape) // width) % count
    skewed = [pltpu.roll(a, i * width, 1) if i else a for i, a in enumerate(arrays)]
    moved = [skewed[-index % count] for index in range(count)]
    distance = 1
    while distance < count:
        take = (field // distance) % 2 == 1
        moved = [
            jnp.where(take, moved[(index - distance) % count], moved[index])
            for index in range(count)
        ]
        distance *= 2
    return [pltpu.roll(m, LANES - i * width, 1) if i else m for i, m in enumerate(moved)]


def turned(values, slots, ahead):
    real = (lane_of(values.shape) // slots) % 2 == 0
    from_imag = pltpu.roll(values, LANES - slots, 1)
    from_real = pltpu.roll(values, slots, 1)
    if ahead:
        return jnp.where(real, from_imag, -from_real)
    return jnp.where(real, -from_imag, from_real)


def swap_slot(first, second, slots):
    place = lane_of(first.shape) % (2 * slots)
    return (
        jnp.where(place == slots, pltpu.roll(second, slots, 1), first),
        jnp.where(place == 0, pltpu.roll(first, LANES - slots, 1), second),
    )


class Route:
    def __init__(self, axis, count, away, source, target, send, recv):
        self.axis, self.count, self.away = axis, count, away
        self.source, self.target = source, target
        self.send, self.recv = send, recv
        self.me = lax.axis_index(axis)

    def copy(self, source, target, peer, part):
        return pltpu.make_async_remote_copy(
            src_ref=source,
            dst_ref=target,
            send_sem=self.send,
            recv_sem=self.recv.at[part] if part is not None else self.recv,
            device_id={self.axis: peer},
            device_id_type=MESH,
        )

    def at(self, ref, where, index):
        return ref.at[where + (index,)]

    def start(self, where, part):
        for peer in self.away:
            source = self.at(self.source, where, peer)
            target = self.at(self.target, where, self.me)
            self.copy(source, target, peer, part).start()

    def arrive(self, where, part):
        spot = self.at(self.target, where, pl.ds(0, self.count - 1))
        self.copy(spot, spot, self.away[0], part).wait_recv()
        self.target[where + (self.me,)] = self.source[where + (self.me,)]

    def drain(self, where):
        spot = self.source.at[where + (pl.ds(0, self.count - 1),)]
        self.copy(spot, spot, self.away[0], 0 if len(self.recv.shape) else None).wait_send()


def whole_kernel(sizes, loads, *refs):
    cells_x, cells_y, length_z, slots, ranks_y = sizes
    members = 2
    width = 2 * slots
    per_tile = cells_x // ranks_y
    tiles = length_z // LANES
    chunks = tiles * per_tile
    length_y = cells_y * ranks_y
    blocks = slots // members
    rows_m = length_y // blocks
    parts = PARTS
    rows_part = rows_m // parts
    sources, held_in = refs[:loads], refs[3 + loads : 3 + 2 * loads]
    modulus, d_recv_0, d_recv_1 = refs[loads : 3 + loads]
    (
        z_send, z_recv, x_send, x_recv, w_send, w_recv, b_send, b_recv,
        s_send, s_recv, e_recv, t_send, t_recv, n_send, n_recv, m_recv,
        tables, other, held, partial, back_hi, back_lo, lower, h_recv, c_send_0, c_send_1, c_recv_0, c_recv_1,
        d_send_0, d_send_1,
        load_sem, send_sem, z_sem, x_sem, w_sem, b_sem, c_sem, d_sem, s_sem, h_sem,
    ) = refs[3 + 2 * loads :]
    (
        spectrum, mirror_z, noise, ahead_hi, ahead_lo, mirror_x, mirror_y, y_hi, y_lo, x_ahead, x_back,
        side_hi, side_lo, pool_rows, pool_columns, group_table,
    ) = held_in

    me_x, me_y = lax.axis_index("px"), lax.axis_index("py")
    copies = [
        pltpu.make_async_copy(source, target, load_sem.at[index])
        for index, (source, target) in enumerate(zip(sources, held_in))
    ]
    place, core = me_y // 2, me_y % 2
    chips = ranks_y // 2
    near = chips - 1 - (chips - 2) * (place % 2)
    steps = [chips // 2, near, chips - near]
    away_y = []
    for step in steps:
        for side in (0, 1):
            away_y.append((place + step) % chips * 2 + (core + side) % 2)
    away_y.append(place * 2 + 1 - core)
    away_x = [slots - 1 - me_x, (me_x + 2) % slots, me_x + 1 - 2 * (me_x % 2)]

    barrier = pltpu.get_barrier_semaphore()
    for peer in away_y:
        pl.semaphore_signal(barrier, inc=1, device_id={"py": peer}, device_id_type=MESH)
    for peer in away_x:
        pl.semaphore_signal(barrier, inc=1, device_id={"px": peer}, device_id_type=MESH)

    early = 6
    for copy in copies[:early]:
        copy.start()

    def route(axis, source, target, send, recv):
        away, count = (away_y, ranks_y) if axis == "py" else (away_x, slots)
        return Route(axis, count, away, source, target, send_sem.at[send], recv)

    z_route = route("py", z_send, z_recv, 0, z_sem)
    x_route = route("px", x_send, x_recv, 1, x_sem)
    w_route = route("px", w_send, w_recv, 2, w_sem)
    b_route = route("py", b_send, b_recv, 3, b_sem)
    t_route = route("px", t_send, t_recv, 5, s_sem.at[1])
    c_send, c_recv = (c_send_0, c_send_1), (c_recv_0, c_recv_1)
    d_send, d_recv = (d_send_0, d_send_1), (d_recv_0, d_recv_1)
    c_routes = [route("py", c_send[f], c_recv[f], 12 + f, c_sem.at[f]) for f in range(members)]
    d_routes = [route("py", d_send[f], d_recv[f], 14 + f, d_sem.at[f]) for f in range(members)]

    lane = lane_of((8, LANES))
    half_y = ranks_y // 2
    my_half, my_place = me_y // half_y, me_y % half_y
    copies[0].wait()
    copies[1].wait()
    mirrored = jnp.concatenate(
        halves(spectrum[:, :, LANES : 2 * LANES].reshape(cells_x * cells_y, LANES)), 1
    )
    held[0, :, pl.ds(0, LANES)] = mm(mirrored, mirror_z[...])
    for row in range(0, cells_y, 8):
        rows = pl.ds(row, 8)
        plain = [spectrum[x, rows, pl.ds(0, LANES)] for x in range(cells_x)]
        turned_z = []
        for x in range(cells_x):
            value = held[0, pl.ds(x * cells_y + row, 8), pl.ds(0, LANES)]
            turned_z.append(jnp.where(lane == 0, plain[x], value))
        for kind, arrays in enumerate((plain, turned_z)):
            moved = exchange(arrays, width)
            for group in range(cells_x):
                s_send[group % ranks_y, kind, group // ranks_y, rows] = moved[group]
    strip = jnp.zeros((8, LANES), F32)
    quarter = (lane // 2) % slots
    for x in range(cells_x):
        for part in range(cells_y // 8):
            value = spectrum[x, pl.ds(part * 8, 8), pl.ds(LANES, 1)]
            strip = jnp.where((lane // width == x) & (quarter == part), value, strip)
    n_send[...] = strip

    def strip_copy():
        return pltpu.make_async_remote_copy(
            src_ref=n_send, dst_ref=n_recv.at[me_y], send_sem=send_sem.at[8],
            recv_sem=s_sem.at[2], device_id={"py": 0}, device_id_type=MESH,
        )

    def half_copy(peer):
        return pltpu.make_async_remote_copy(
            src_ref=s_send.at[peer], dst_ref=s_recv.at[my_place], send_sem=send_sem.at[4],
            recv_sem=s_sem.at[0], device_id={"py": peer}, device_id_type=MESH,
        )

    def edge_copy(peer):
        return pltpu.make_async_remote_copy(
            src_ref=s_send.at[peer, 1, :, pl.ds(0, 8)], dst_ref=e_recv, send_sem=send_sem.at[10],
            recv_sem=s_sem.at[4], device_id={"py": peer}, device_id_type=MESH,
        )

    others = [my_half * half_y + (my_place + step) % half_y for step in range(1, half_y)]
    across = [(1 - my_half) * half_y + step for step in range(half_y)]

    def send_spectrum():
        pl.when(me_y != 0)(lambda: strip_copy().start())
        for peer in others[1:] + others[:1]:
            half_copy(peer).start()

        @pl.when(my_place == 0)
        def _():
            for peer in across:
                edge_copy(peer).start()

    middle = (place == chips // 2) | (place == chips // 2 - 1)
    giver, taker = middle & (core == 0), middle & (core == 1)

    def hand_copy(chunk):
        return pltpu.make_async_remote_copy(
            src_ref=z_send.at[chunk, pl.ds((1 - my_half) * half_y, half_y)],
            dst_ref=h_recv.at[chunk], send_sem=send_sem.at[0], recv_sem=h_sem.at[chunk],
            device_id={"py": place * 2 + 1 - core}, device_id_type=MESH,
        )

    def z_copy(source, chunk, slot, peer, send):
        return pltpu.make_async_remote_copy(
            src_ref=source, dst_ref=z_recv.at[chunk, slot], send_sem=send_sem.at[send],
            recv_sem=z_sem.at[chunk], device_id={"py": peer}, device_id_type=MESH,
        )

    def z_start(chunk):
        @pl.when(giver)
        def _():
            hand_copy(chunk).start()
            for peer in others:
                z_copy(z_send.at[chunk, peer], chunk, me_y, peer, 0).start()

        @pl.when(jnp.logical_not(giver))
        def _():
            z_route.start((chunk,), chunk)

        @pl.when(taker)
        def _():
            hand_copy(chunk).wait_recv()
            for step, peer in enumerate(across):
                z_copy(h_recv.at[chunk, step], chunk, me_y - 1, peer, 11).start()

    for copy in copies[2:early]:
        copy.wait()
    for copy in copies[early:]:
        copy.start()
    cells = cells_x * cells_y
    for f in range(members):
        high, low = halves(noise[f].reshape(cells, length_z))
        held[f] = mm(high, ahead_hi[...]) + mm(high, ahead_lo[...]) + mm(low, ahead_hi[...])
    for tile in range(tiles):
        lanes = pl.ds(tile * LANES, LANES)
        for row in range(0, cells_y, 8):
            rows = pl.ds(row, 8)
            both = []
            for f in range(members):
                both.append(
                    exchange(
                        [held[f, pl.ds(x * cells_y + row, 8), lanes] for x in range(cells_x)],
                        width,
                    )
                )
            if tile == 0:
                both[0][0], both[1][0] = swap_slot(both[0][0], both[1][0], slots)
            for f in range(members):
                for group in range(cells_x):
                    chunk = tile * per_tile + group // ranks_y
                    z_send[chunk, group % ranks_y, f, rows] = both[f][group]
        if tile == 0:
            pl.semaphore_wait(barrier, ranks_y + slots - 2)
            send_spectrum()
        for part in range(per_tile):
            chunk = tile * per_tile + part
            z_start(chunk)

    for copy in copies[early:]:
        copy.wait()
    sides = cells_x // ranks_y
    rows_side = LANES // sides
    for target, source, count in ((back_hi, side_hi, 2), (back_lo, side_lo, 1)):
        blank = jnp.zeros((rows_side, length_z), BF16)
        for chunk in range(chunks):
            for block in range(count * sides):
                rows = pl.ds(block * rows_side, rows_side)
                for side in range(sides):
                    value = source[chunk] if block % sides == side else blank
                    target[chunk, rows, pl.ds(side * length_z, length_z)] = value

    spot = s_recv.at[pl.ds(0, half_y - 1)]
    pltpu.make_async_remote_copy(
        src_ref=spot, dst_ref=spot, send_sem=send_sem.at[4], recv_sem=s_sem.at[0],
        device_id={"py": others[0]}, device_id_type=MESH,
    ).wait_recv()
    edge_copy(others[0]).wait_recv()
    s_recv[my_place] = s_send[me_y]
    pair = [s_recv[:, 1, tile].reshape(rows_m, LANES) for tile in range(tiles)]
    pair = jnp.concatenate(halves(jnp.concatenate(pair, 1)), 0)
    held[1, pl.ds(0, rows_m)] = mm(mirror_y[...], pair)
    sublane = lax.broadcasted_iota(jnp.int32, (8, LANES), 0)
    for row in range(0, rows_m, 8):
        arrays = []
        for tile in range(tiles):
            arrays.append(s_recv[row // cells_y, 0, tile, pl.ds(row % cells_y, 8)])
            value = held[1, pl.ds(row, 8), pl.ds(tile * LANES, LANES)]
            if row == 0:
                value = jnp.where(sublane == 0, e_recv[tile], value)
            arrays.append(value)
        moved = exchange(arrays, 2)
        for rank in range(slots):
            t_send[rank, pl.ds(row, 8)] = moved[rank]
    t_route.start((), None)

    def strips_copy(source):
        return pltpu.make_async_remote_copy(
            src_ref=n_recv, dst_ref=m_recv.at[source], send_sem=send_sem.at[9],
            recv_sem=s_sem.at[3], device_id={"px": 0}, device_id_type=MESH,
        )

    def along_y(route, part, columns, ahead):
        high, low = halves(columns)
        product = mm(y_hi[...], high) + mm(y_hi[...], low) + mm(y_lo[...], high)
        return product

    def combined(product, f, start, rows, ahead):
        lanes = slice(f * LANES, (f + 1) * LANES)
        by_cos = product[start : start + rows, lanes]
        by_sin = product[length_y + start : length_y + start + rows, lanes]
        return by_cos + turned(by_sin, slots, ahead)

    def y_ahead(chunk):
        z_route.arrive((chunk,), chunk)
        columns = [z_recv[chunk, :, f].reshape(length_y, LANES) for f in range(members)]
        product = along_y(z_route, chunk, jnp.concatenate(columns, 1), True)
        for part in range(parts):
            for row in range(0, rows_part, 16):
                arrays = []
                for f in range(members):
                    for block in range(blocks):
                        at = block * rows_m + part * rows_part + row
                        arrays.append(combined(product, f, at, 16, True))
                moved = exchange(arrays, 1)
                for rank in range(slots):
                    x_send[chunk, part, rank, pl.ds(row, 16)] = moved[rank]
            x_route.start((chunk, part), chunk * parts + part)

    def gathered(ref, chunk, some):
        pieces = [[] for _ in range(slots)]
        for part in some:
            for row in range(0, rows_part, 16):
                moved = exchange([ref[chunk, part, s, pl.ds(row, 16)] for s in range(slots)], 1)
                for index in range(slots):
                    pieces[index].append(moved[index])
        return [jnp.concatenate(piece, 0) for piece in pieces]

    def along_x(values, table):
        product = mm(jnp.concatenate(halves(values), 1), table[...])
        return product[:, :LANES] + product[:, LANES:]

    def x_both(chunk):
        for part in range(parts):
            x_route.arrive((chunk, part), chunk * parts + part)
            values = along_x(jnp.concatenate(gathered(x_recv, chunk, [part]), 0), x_ahead)
            scaled = []
            rows = pl.ds(part * rows_part, rows_part)
            for f in range(members):
                for block in range(blocks):
                    at = (f * blocks + block) * rows_part
                    table = other if f == 1 and chunk == 0 else tables.at[chunk]
                    scaled.append(values[at : at + rows_part] * table[block, rows])
            values = along_x(jnp.concatenate(scaled, 0), x_back)
            for row in range(0, rows_part, 16):
                arrays = [
                    values[a * rows_part + row : a * rows_part + row + 16] for a in range(slots)
                ]
                moved = exchange(arrays, 1)
                for s in range(slots):
                    w_send[chunk, part, s, pl.ds(row, 16)] = moved[s]
            w_route.start((chunk, part), chunk * parts + part)

    def y_back(chunk):
        for part in range(parts):
            w_route.arrive((chunk, part), chunk * parts + part)
        arrays = gathered(w_recv, chunk, range(parts))
        columns = [
            jnp.concatenate(arrays[f * blocks : (f + 1) * blocks], 0) for f in range(members)
        ]
        product = along_y(w_route, chunk, jnp.concatenate(columns, 1), False)
        for f in range(members):
            for p in range(ranks_y):
                b_send[chunk, f, p] = combined(product, f, p * cells_y, cells_y, False)
            b_route.start((chunk, f), chunk * members + f)

    def table_rows(tile, block, rows, part):
        even = lane % 2 == 0
        first = jnp.where(even, part, pltpu.roll(part, 1, 1))
        second = jnp.where(even, pltpu.roll(part, LANES - 1, 1), part)
        tables[tile * per_tile, block, rows] = first
        tables[tile * per_tile + 1, block, rows] = second
        if tile == 0:
            other[block, rows] = first

    def spectrum_tables():
        t_route.arrive((), None)
        images = [[] for _ in range(tiles)]
        for row in range(0, rows_m, 8):
            rows = pl.ds(row, 8)
            moved = exchange([t_recv[s, rows] for s in range(slots)], 2)
            for tile in range(tiles):
                table_rows(tile, my_half, rows, moved[2 * tile])
                images[tile].append(moved[2 * tile + 1])
        images = jnp.concatenate([piece for pieces in images for piece in pieces], 0)
        images = mm(jnp.concatenate(halves(images), 1), mirror_x[...])
        for tile in range(tiles):
            for row in range(0, rows_m, 8):
                at = tile * rows_m + row
                table_rows(tile, 1 - my_half, pl.ds(row, 8), images[at : at + 8])

        @pl.when((me_y == 0) & (me_x == 0))
        def _():
            spot = m_recv.at[pl.ds(1, slots - 1)]
            pltpu.make_async_remote_copy(
                src_ref=spot, dst_ref=spot, send_sem=send_sem.at[9], recv_sem=s_sem.at[3],
                device_id={"px": 1}, device_id_type=MESH,
            ).wait_recv()
            for p in range(ranks_y):
                strips = [n_recv[p] if s == 0 else m_recv[s, p] for s in range(slots)]
                for part in range(cells_y // 8):
                    value = strips[part]
                    for s in range(slots):
                        shift = (s - part) * 2 % LANES
                        moved = pltpu.roll(strips[s], shift, 1) if shift else strips[s]
                        value = jnp.where(quarter == s, moved, value)
                    at = p * cells_y + part * 8
                    other[at // rows_m, pl.ds(at % rows_m, 8)] = value

    @pl.when(me_y == 0)
    def _():
        spot = n_recv.at[pl.ds(0, ranks_y - 1)]
        pltpu.make_async_remote_copy(
            src_ref=spot, dst_ref=spot, send_sem=send_sem.at[8], recv_sem=s_sem.at[2],
            device_id={"py": 1}, device_id_type=MESH,
        ).wait_recv()
        n_recv[0] = n_send[...]
        pl.when(me_x != 0)(lambda: strips_copy(me_x).start())

    y_ahead(0)
    spectrum_tables()
    for chunk in range(chunks):
        x_both(chunk)
        if chunk + 1 < chunks:
            y_ahead(chunk + 1)
        y_back(chunk)

    tall = cells // 4 // ranks_y
    def z_back(chunk, f):
        pieces = [[] for _ in range(ranks_y)]
        for row in range(0, cells_y, 8):
            rows = pl.ds(row, 8)
            arrays = [b_recv[chunk, f, group, rows] for group in range(ranks_y)]
            if chunk == 0:
                pair = [b_recv[0, 0, 0, rows], b_recv[0, 1, 0, rows]]
                arrays[0] = swap_slot(*pair, slots)[f]
            moved = exchange(arrays, width)
            for x in range(ranks_y):
                pieces[x].append(moved[x])
        high, low = halves(jnp.concatenate([piece for some in pieces for piece in some], 0))
        fields = mm(jnp.concatenate([high, low], 1), back_hi[chunk]) + mm(high, back_lo[chunk])
        if chunk > 0:
            fields = fields + partial[f]
        if chunk + 1 < chunks:
            partial[f] = fields
            return
        values = jnp.exp(0.5 * fields)
        for side in range(sides):
            lanes = slice(side * length_z, (side + 1) * length_z)
            cut = values[:, lanes].reshape(ranks_y, cells_y, length_z)
            modulus[f, pl.ds(side * ranks_y, ranks_y)] = cut
        high, low = halves(values)
        pooled = mm(pool_rows[...], high) + mm(pool_rows[...], low)
        pooled = [pooled[:, side * length_z : (side + 1) * length_z] for side in range(sides)]
        high, low = halves(jnp.concatenate(pooled, 0))
        coarse = mm(high, pool_columns[...]) + mm(low, pool_columns[...])
        per_side = ranks_y // sides
        height = coarse.shape[0] // sides
        for d in range(ranks_y):
            base = d // per_side * height
            at = base + d % per_side * tall
            c_send[f][d, pl.ds(0, tall)] = coarse[at : at + tall, :LANES]
            at = base + per_side * tall + d % per_side * 8
            value = coarse[at : at + 8, LANES:]
            value = jnp.where(lane < LANES // 2, value, pltpu.roll(value, 4, 0))
            if f == 0:
                lower[d] = value
            else:
                c_send[f][d, pl.ds(tall, 8)] = jnp.where(
                    sublane < 4, lower[d], pltpu.roll(value, 4, 0)
                )
        c_routes[f].start((), None)

    def pick(f):
        c_routes[f].arrive((), None)
        for g in range(ranks_y):
            d_send[f][g, pl.ds(0, tall)] = c_recv[f][group_table[0, g], pl.ds(0, tall)]
            if f == 1:
                second = c_recv[f][group_table[1, g], pl.ds(tall, 8)]
                third = c_recv[f][group_table[2, g], pl.ds(tall, 8)]
                d_send[f][g, pl.ds(tall, 8)] = jnp.where(lane < LANES // 2, second, third)
        d_routes[f].start((), None)

    for chunk in range(chunks):
        for f in range(members):
            b_route.arrive((chunk, f), chunk * members + f)
            if chunk > 0:
                z_back(chunk, f)
        if chunk == 0:
            for f in range(members):
                z_back(chunk, f)
    for f in range(members):
        pick(f)
    for f in range(members):
        d_routes[f].arrive((), None)

    every = pl.ds(0, chunks)
    z_route.drain((every,))

    @pl.when(taker)
    def _():
        pltpu.make_async_remote_copy(
            src_ref=h_recv, dst_ref=h_recv, send_sem=send_sem.at[11], recv_sem=h_sem.at[0],
            device_id={"py": others[0]}, device_id_type=MESH,
        ).wait_send()

    x_route.drain((every, pl.ds(0, parts)))
    w_route.drain((every, pl.ds(0, parts)))
    b_route.drain((every, pl.ds(0, members)))
    spot = s_send.at[pl.ds(0, half_y - 1)]
    pltpu.make_async_remote_copy(
        src_ref=spot, dst_ref=spot, send_sem=send_sem.at[4], recv_sem=s_sem.at[0],
        device_id={"py": others[0]}, device_id_type=MESH,
    ).wait_send()

    @pl.when(my_place == 0)
    def _():
        spot = s_send.at[pl.ds(0, half_y), 1, :, pl.ds(0, 8)]
        pltpu.make_async_remote_copy(
            src_ref=spot, dst_ref=spot, send_sem=send_sem.at[10], recv_sem=s_sem.at[4],
            device_id={"py": others[0]}, device_id_type=MESH,
        ).wait_send()

    t_route.drain(())
    for some in c_routes + d_routes:
        some.drain(())
    pl.when(me_y != 0)(lambda: strip_copy().wait_send())
    pl.when((me_y == 0) & (me_x != 0))(lambda: strips_copy(me_x).wait_send())


def leaving_kernel(modulus, first, second, modulus_out, one_out, level_two, level_three, sems):
    members, cells_x, cells_y, length_z = modulus.shape
    ranks_y, tall = first.shape[:2]
    copies = []
    for f, coarse in enumerate((first, second)):
        copies.append(pltpu.make_async_copy(modulus.at[f], modulus_out.at[f], sems.at[f]))
        copies.append(
            pltpu.make_async_copy(
                coarse.at[:, pl.ds(0, tall)], one_out.at[f], sems.at[members + f]
            )
        )
    for copy in copies:
        copy.start()
    row = lax.broadcasted_iota(jnp.int32, (8, LANES), 0)
    short = cells_y // 4
    lows = [second[d, pl.ds(tall, 8)] for d in range(ranks_y)]
    for f in range(members):
        shifts = [4 * f, 4 - 4 * f]
        for x in range(ranks_y // 2):
            pair = [
                pltpu.roll(low, shift, 0) if shift else low
                for low, shift in zip(lows[2 * x : 2 * x + 2], shifts)
            ]
            value = jnp.where(row < 4, *pair)
            level_two[f, x] = value[:short, : length_z // 4]
        for x in range(ranks_y // 4):
            value = jnp.zeros((8, LANES), F32)
            for y in range(4):
                low = lows[4 * x + y]
                shift = (y - 4 * f) % 8
                low = pltpu.roll(low, shift, 0) if shift else low
                value = jnp.where(row == y, low, value)
            value = pltpu.roll(value, LANES // 2, 1)
            level_three[f, x] = value[: short // 2, : length_z // 8]
    for copy in copies:
        copy.wait()


def lanes_path(white_noise, spectrum, group_table):
    members, cells_x, cells_y, length_z = white_noise.shape
    size_px, size_py = lax.axis_size("px"), lax.axis_size("py")
    length_x, length_y = cells_x * size_px, cells_y * size_py
    slots, width = size_px, 2 * size_px
    tiles = length_z // LANES
    per_tile = cells_x // size_py
    chunks = tiles * per_tile
    blocks = slots // members
    rows_m = length_y // blocks

    column = np.arange(length_z)
    tile, lane = column // LANES, column % LANES
    part = (lane // slots) % 2
    group = lane // width
    rank_q, rank_p, inner = lane % slots, group % size_py, group // size_py
    k = ((tile * size_py + rank_p) * slots + rank_q) * per_tile + inner
    angles = angles_of(length_z)
    sign = np.where(np.arange(length_z) % 2 == 0, 1.0, -1.0)
    z_ahead = np.where(part == 0, np.cos(angles[:, k]), -np.sin(angles[:, k]))
    z_back = 2.0 * z_ahead
    first = (k == 0) & (part == 0)
    second = (k == 0) & (part == 1)
    z_ahead[:, second] = sign[:, None]
    z_back[:, first] = 1.0
    z_back[:, second] = sign[:, None]
    z_back = z_back.T / (length_x * length_y * length_z)

    sides = cells_x // size_py
    half_cells = cells_x * cells_y // sides
    back_hi, back_lo = host_halves(z_back.reshape(chunks, LANES // sides, length_z))

    angles = angles_of(length_y)
    y_table = np.concatenate([np.cos(angles), np.sin(angles)], 0)

    lane = np.arange(LANES)
    cell = (lane // slots % 2, lane % slots * cells_x + lane // width)
    mode = (lane % 2, lane // 2 % slots * cells_x + lane // width)

    def x_table(direction, rows, columns):
        table = complex_array(length_x, direction)[rows][:, columns[0], columns[1]]
        high, low = host_halves(table)
        return jnp.concatenate(
            [
                jnp.concatenate([high, low], 1),
                jnp.concatenate([high, jnp.zeros_like(low)], 1),
            ],
            0,
        )

    at = np.arange(1, LANES)
    mirror_z = np.zeros((LANES, LANES))
    mirror_z[LANES - at, at] = 1.0
    at = np.arange(1, rows_m)
    mirror_y = np.zeros((rows_m, rows_m))
    mirror_y[at, rows_m - at] = 1.0
    same = (mode[1][:, None] + mode[1][None]) % length_x == 0
    mirror_x = np.where(same & (mode[0][:, None] == mode[0][None]), 1.0, 0.0)

    def pool(extent_x, extent_y, factor):
        short_x, short_y = extent_x // factor, extent_y // factor
        row, cell = np.arange(short_x * short_y), np.arange(extent_x * extent_y)
        same_x = cell[None] // extent_y // factor == row[:, None] // short_y
        same_y = cell[None] % extent_y // factor == row[:, None] % short_y
        return np.where(same_x & same_y, 1.0 / factor**3, 0.0)

    per_side = size_py // sides
    some = size_py, cells_y
    lower = np.zeros((per_side, 8, half_cells))
    lower[:, :4] = pool(*some, 4).reshape(per_side, 4, -1)
    lower[:, 4:5] = pool(*some, 8).reshape(per_side, 1, -1)
    pool_rows = np.concatenate([pool(*some, 2), lower.reshape(8 * per_side, -1)], 0)
    pool_columns = np.zeros((length_z, 2 * LANES))
    z = np.arange(length_z)
    pool_columns[z, z // 2] = 1.0
    pool_columns[z, LANES + z // 4] = 1.0
    pool_columns[z, LANES + length_z // 4 + z // 8] = 1.0

    held_in = [
        spectrum,
        jnp.asarray(np.tile(mirror_z, (2, 1)), BF16),
        white_noise,
        *host_halves(z_ahead),
        jnp.asarray(np.tile(mirror_x, (2, 1)), BF16),
        jnp.asarray(np.tile(mirror_y, (1, 2)), BF16),
        *host_halves(y_table),
        x_table(-1.0, cell, mode),
        x_table(1.0, mode, cell),
        back_hi,
        back_lo,
        jnp.asarray(pool_rows, BF16),
        jnp.asarray(pool_columns, BF16),
        group_table,
    ]
    sizes = (cells_x, cells_y, length_z, slots, size_py)

    def body(*refs):
        whole_kernel(sizes, len(held_in), *refs)

    def vmem(*shape):
        return pltpu.VMEM(shape, F32)

    z_shape = (chunks, size_py, members, cells_y, LANES)
    x_shape = (chunks, PARTS, slots, rows_m // PARTS, LANES)
    b_shape = (chunks, members, size_py, cells_y, LANES)
    s_shape = (2, tiles, cells_y, LANES)
    t_shape = (slots, rows_m, LANES)
    tall = cells_x * cells_y // 4 // size_py
    c_shapes = [(size_py, tall, LANES), (size_py, tall + 8, LANES)]
    sem = pltpu.SemaphoreType.DMA
    scratch = [pltpu.VMEM(value.shape, value.dtype) for value in held_in[:-1]]
    scratch.append(pltpu.SMEM(group_table.shape, group_table.dtype))
    for shape in (z_shape, x_shape, x_shape, b_shape):
        scratch += [vmem(*shape), vmem(*shape)]
    scratch += [vmem(size_py, *s_shape), vmem(size_py // 2, *s_shape), vmem(tiles, 8, LANES)]
    scratch += [vmem(*t_shape), vmem(*t_shape)]
    scratch += [vmem(8, LANES), vmem(size_py, 8, LANES), vmem(slots, size_py, 8, LANES)]
    scratch += [
        vmem(chunks, blocks, rows_m, LANES),
        vmem(blocks, rows_m, LANES),
        vmem(members, cells_x * cells_y, length_z),
        vmem(members, half_cells, sides * length_z),
        pltpu.VMEM((chunks, 2 * LANES, sides * length_z), BF16),
        pltpu.VMEM((chunks, LANES, sides * length_z), BF16),
        vmem(size_py, 8, LANES),
        vmem(chunks, size_py // 2, members, cells_y, LANES),
        *[vmem(*shape) for shape in c_shapes * 3],
    ]
    scratch += [
        sem((len(held_in),)), sem((16,)), sem((chunks,)), sem((chunks * PARTS,)),
        sem((chunks * PARTS,)), sem((chunks * members,)), sem((members,)), sem((members,)), sem((5,)), sem((chunks,)),
    ]
    hbm = pl.BlockSpec(memory_space=pltpu.HBM)
    local = pl.BlockSpec(memory_space=pltpu.VMEM)
    leaving = pl.pallas_call(
        body,
        out_shape=[jax.ShapeDtypeStruct(shape, F32) for shape in [white_noise.shape] + c_shapes],
        in_specs=[hbm] * len(held_in),
        out_specs=[local] * 3,
        scratch_shapes=scratch,
        compiler_params=pltpu.CompilerParams(
            collective_id=0, has_side_effects=True, vmem_limit_bytes=40 * 1024 * 1024
        ),
    )(*[pltpu.with_memory_space_constraint(v, pltpu.HBM) for v in held_in])
    outs = [white_noise.shape]
    for level in range(1, 4):
        outs.append((members,) + tuple(extent >> level for extent in white_noise.shape[1:]))
    return tuple(
        pl.pallas_call(
            leaving_kernel,
            out_shape=[jax.ShapeDtypeStruct(shape, F32) for shape in outs],
            in_specs=[local] * 3,
            out_specs=[hbm, hbm, local, local],
            scratch_shapes=[sem((2 * members,))],
            compiler_params=pltpu.CompilerParams(vmem_limit_bytes=4 * 1024 * 1024),
        )(*leaving)
    )


def on_device(white_noise, spectrum, group_table):
    members, cells_x, cells_y, length_z = white_noise.shape
    size_px, size_py = lax.axis_size("px"), lax.axis_size("py")
    fits = members == 2 and length_z == 2 * LANES and size_px == 4 and size_py == 8
    fits = fits and 2 * cells_x * size_px == LANES and cells_x == 2 * size_py
    fits = fits and cells_y == 2 * cells_x
    chosen = lanes_path if fits else general_path
    return chosen(white_noise, spectrum, group_table)


def solution(mesh):
    in_specs = (P(None, "px", "py", None), P("px", "py", None), P())
    out_specs = (P(None, "px", "py", None),) * 4
    return jax.shard_map(
        on_device, mesh=mesh, in_specs=in_specs, out_specs=out_specs, check_vma=False
    )
```

```python
import numpy as np

import jax
import jax.numpy as jnp
from jax import lax
from jax.experimental import pallas as pl
from jax.experimental.pallas import tpu as pltpu
from jax.sharding import PartitionSpec as P


def angles_of(length):
    positions = np.arange(length, dtype=np.int64)
    return (positions[:, None] * positions[None, :] % length) * (2.0 * np.pi / length)


def complex_array(length, direction):
    angles = angles_of(length)
    cos, sin = np.cos(angles), direction * np.sin(angles)
    return np.stack([np.stack([cos, sin], 1), np.stack([-sin, cos], 1)], 0)


def complex_table(length, direction):
    return jnp.asarray(complex_array(length, direction), jnp.float32)


def half_tables(length):
    angles = angles_of(length)[:, : length // 2]
    ahead = np.stack([np.cos(angles), -np.sin(angles)], 1)
    back = 2.0 * ahead
    nyquist = np.where(np.arange(length) % 2 == 0, 1.0, -1.0)
    ahead[:, 1, 0] = nyquist
    back[:, 0, 0] = 1.0
    back[:, 1, 0] = nyquist
    return jnp.asarray(ahead, jnp.float32), jnp.asarray(back, jnp.float32)


def einsum(pattern, left, right):
    return jnp.einsum(pattern, left, right, precision=lax.Precision.HIGH)


def swap_first(values):
    first = values[:, :, :1]
    turned = jnp.swapaxes(first, 0, 1)
    return jnp.concatenate([turned, values[:, :, 1:]], 2)


def coarsen(values):
    members, size_x, size_y, size_z = values.shape
    blocks = values.reshape(members, size_x // 2, 2, size_y // 2, 2, size_z // 2, 2)
    return blocks.mean(axis=(2, 4, 6))


def general_path(white_noise, spectrum, group_table):
    members, cells_x, cells_y, length_z = white_noise.shape
    size_px, size_py = lax.axis_size("px"), lax.axis_size("py")
    length_x, length_y = cells_x * size_px, cells_y * size_py
    half_z = length_z // 2
    block_py, block = half_z // size_py, half_z // size_py // size_px
    z_ahead, z_back = half_tables(length_z)
    scale = 1.0 / (length_x * length_y * length_z)

    table = jnp.transpose(spectrum, (2, 0, 1))
    last = jnp.broadcast_to(table[half_z : half_z + 1], (size_py, 1, cells_x, cells_y))
    table = jnp.concatenate([table[:half_z].reshape(size_py, block_py, cells_x, cells_y), last], 1)
    table = lax.all_to_all(table, "py", split_axis=0, concat_axis=3, tiled=True)[0]
    last = jnp.broadcast_to(table[block_py:], (size_px, 1, cells_x, length_y))
    table = jnp.concatenate([table[:block_py].reshape(size_px, block, cells_x, length_y), last], 1)
    table = lax.all_to_all(table, "px", split_axis=0, concat_axis=2, tiled=True)[0] * scale
    is_first = (lax.axis_index("px") == 0) & (lax.axis_index("py") == 0)
    other = jnp.where(is_first, table[block:], table[:1])
    tables = jnp.stack([table[:block], jnp.concatenate([other, table[1:block]], 0)], 0)

    values = einsum("fxyz,zck->fckxy", white_noise, z_ahead)
    values = swap_first(values)
    values = lax.all_to_all(values, "py", split_axis=2, concat_axis=4, tiled=True)
    values = einsum("fckxy,cydm->fdkxm", values, complex_table(length_y, -1.0))
    values = lax.all_to_all(values, "px", split_axis=2, concat_axis=3, tiled=True)
    values = einsum("fckxm,cxdj->fdkjm", values, complex_table(length_x, -1.0))
    values = values * tables[:, None]
    values = einsum("fckjm,cjdx->fdkxm", values, complex_table(length_x, 1.0))
    values = lax.all_to_all(values, "px", split_axis=3, concat_axis=2, tiled=True)
    values = einsum("fckxm,cmdy->fdkxy", values, complex_table(length_y, 1.0))
    values = lax.all_to_all(values, "py", split_axis=4, concat_axis=2, tiled=True)
    values = swap_first(values)
    fields = einsum("fckxy,zck->fxyz", values, z_back)
    modulus = jnp.exp(0.5 * fields)

    levels = []
    level = modulus
    for _ in range(3):
        level = coarsen(level)
        levels.append(level)
    pieces = [jnp.reshape(level, (size_py, -1)) for level in levels]
    widths = [piece.shape[1] for piece in pieces]
    joined = jnp.concatenate(pieces, 1)
    spread = lax.all_to_all(joined, "py", split_axis=0, concat_axis=0, tiled=True)
    picked, start = [], 0
    for index, width in enumerate(widths):
        part = spread[:, start : start + width]
        picked.append(jnp.take(part, group_table[index], axis=0))
        start += width
    joined = lax.all_to_all(
        jnp.concatenate(picked, 1), "py", split_axis=0, concat_axis=0, tiled=True
    )
    routed, start = [], 0
    for level, width in zip(levels, widths):
        routed.append(joined[:, start : start + width].reshape(level.shape))
        start += width
    return (modulus, routed[0], routed[1], routed[2])


LANES = 128
ORDER = (
    "y0", "y1", "T", "y2", "x0", "y3", "x1", "y4", "x2", "b0", "x3", "y5", "b1",
    "y6", "x4", "b2", "y7", "b3", "x5", "x6", "b4", "x7", "b5", "b6", "b7",
)
MESH = pl.DeviceIdType.MESH
BF16 = jnp.bfloat16
F32 = jnp.float32


def halves(values):
    high = values.astype(BF16)
    low = (values - high.astype(F32)).astype(BF16)
    return high, low


def host_halves(values):
    values = np.asarray(values, np.float64)
    high = values.astype(np.float32).astype(BF16)
    low = (values - high.astype(np.float64)).astype(np.float32).astype(BF16)
    return jnp.asarray(high), jnp.asarray(low)


def mm(left, right):
    return jnp.dot(left, right, preferred_element_type=F32)


def lane_of(shape):
    return lax.broadcasted_iota(jnp.int32, shape, len(shape) - 1)


def exchange(arrays, width):
    count = len(arrays)
    field = (lane_of(arrays[0].shape) // width) % count
    skewed = [pltpu.roll(a, i * width, 1) if i else a for i, a in enumerate(arrays)]
    moved = [skewed[-index % count] for index in range(count)]
    distance = 1
    while distance < count:
        take = (field // distance) % 2 == 1
        moved = [
            jnp.where(take, moved[(index - distance) % count], moved[index])
            for index in range(count)
        ]
        distance *= 2
    return [pltpu.roll(m, LANES - i * width, 1) if i else m for i, m in enumerate(moved)]


def turned(values, slots, ahead):
    real = (lane_of(values.shape) // slots) % 2 == 0
    from_imag = pltpu.roll(values, LANES - slots, 1)
    from_real = pltpu.roll(values, slots, 1)
    if ahead:
        return jnp.where(real, from_imag, -from_real)
    return jnp.where(real, -from_imag, from_real)


def swap_slot(first, second, slots):
    place = lane_of(first.shape) % (2 * slots)
    return (
        jnp.where(place == slots, pltpu.roll(second, slots, 1), first),
        jnp.where(place == 0, pltpu.roll(first, LANES - slots, 1), second),
    )


class Route:
    def __init__(self, axis, count, away, source, target, send, recv):
        self.axis, self.count, self.away = axis, count, away
        self.source, self.target = source, target
        self.send, self.recv = send, recv
        self.me = lax.axis_index(axis)

    def copy(self, source, target, peer, part):
        return pltpu.make_async_remote_copy(
            src_ref=source,
            dst_ref=target,
            send_sem=self.send,
            recv_sem=self.recv.at[part] if part is not None else self.recv,
            device_id={self.axis: peer},
            device_id_type=MESH,
        )

    def at(self, ref, where, index):
        return ref.at[where + (index,)]

    def start(self, where, part):
        for peer in self.away:
            source = self.at(self.source, where, peer)
            target = self.at(self.target, where, self.me)
            self.copy(source, target, peer, part).start()

    def arrive(self, where, part):
        spot = self.at(self.target, where, pl.ds(0, self.count - 1))
        self.copy(spot, spot, self.away[0], part).wait_recv()
        self.target[where + (self.me,)] = self.source[where + (self.me,)]

    def drain(self, where):
        spot = self.source.at[where + (pl.ds(0, self.count - 1),)]
        self.copy(spot, spot, self.away[0], 0 if len(self.recv.shape) else None).wait_send()


def whole_kernel(sizes, loads, *refs):
    cells_x, cells_y, length_z, slots, ranks_y = sizes
    members = 2
    width = 2 * slots
    per_tile = cells_x // ranks_y
    tiles = length_z // LANES
    chunks = tiles * per_tile
    length_y = cells_y * ranks_y
    blocks = slots // members
    rows_m = length_y // blocks
    rows_part = length_y // slots
    sources, held_in = refs[:loads], refs[3 + loads : 3 + 2 * loads]
    modulus, d_recv_0, d_recv_1 = refs[loads : 3 + loads]
    (
        z_send, z_recv, x_send, x_recv, w_send, w_recv, b_send, b_recv,
        s_send, s_recv, e_recv, t_send, t_recv, n_send, n_recv, m_recv,
        tables, other, held, image, partial, back_hi, back_lo, lower, h_recv, c_send_0, c_send_1, c_recv_0, c_recv_1,
        d_send_0, d_send_1,
        load_sem, send_sem, z_sem, x_sem, w_sem, b_sem, c_sem, d_sem, s_sem, h_sem,
    ) = refs[3 + 2 * loads :]
    (
        noise, ahead, spectrum, mirror_z, mirror_x, mirror_y, y_hi, y_lo, x_ahead, x_back,
        side_hi, side_lo, pool_rows, pool_columns, group_table,
    ) = held_in

    me_x, me_y = lax.axis_index("px"), lax.axis_index("py")
    copies = [
        pltpu.make_async_copy(source, target, load_sem.at[index])
        for index, (source, target) in enumerate(zip(sources, held_in))
    ]
    place, core = me_y // 2, me_y % 2
    chips = ranks_y // 2
    near = chips - 1 - (chips - 2) * (place % 2)
    steps = [chips // 2, near, chips - near]
    away_y = []
    for step in steps:
        for side in (0, 1):
            away_y.append((place + step) % chips * 2 + (core + side) % 2)
    away_y.append(place * 2 + 1 - core)
    away_x = [slots - 1 - me_x, (me_x + 2) % slots, me_x + 1 - 2 * (me_x % 2)]

    barrier = pltpu.get_barrier_semaphore()
    for peer in away_y:
        pl.semaphore_signal(barrier, inc=1, device_id={"py": peer}, device_id_type=MESH)
    for peer in away_x:
        pl.semaphore_signal(barrier, inc=1, device_id={"px": peer}, device_id_type=MESH)

    early = 4
    for copy in copies[:early]:
        copy.start()

    def route(axis, source, target, send, recv):
        away, count = (away_y, ranks_y) if axis == "py" else (away_x, slots)
        return Route(axis, count, away, source, target, send_sem.at[send], recv)

    z_route = route("py", z_send, z_recv, 0, z_sem)
    x_route = route("px", x_send, x_recv, 1, x_sem)
    w_route = route("px", w_send, w_recv, 2, w_sem)
    b_route = route("py", b_send, b_recv, 3, b_sem)
    t_route = route("px", t_send, t_recv, 5, s_sem.at[1])
    c_send, c_recv = (c_send_0, c_send_1), (c_recv_0, c_recv_1)
    d_send, d_recv = (d_send_0, d_send_1), (d_recv_0, d_recv_1)
    c_routes = [route("py", c_send[f], c_recv[f], 12 + f, c_sem.at[f]) for f in range(members)]
    d_routes = [route("py", d_send[f], d_recv[f], 14 + f, d_sem.at[f]) for f in range(members)]

    lane = lane_of((8, LANES))
    quarter = (lane // 2) % slots
    half_y = ranks_y // 2
    my_half, my_place = me_y // half_y, me_y % half_y

    def strip_copy():
        return pltpu.make_async_remote_copy(
            src_ref=n_send, dst_ref=n_recv.at[me_y], send_sem=send_sem.at[8],
            recv_sem=s_sem.at[2], device_id={"py": 0}, device_id_type=MESH,
        )

    def half_copy(peer):
        return pltpu.make_async_remote_copy(
            src_ref=s_send.at[peer], dst_ref=s_recv.at[my_place], send_sem=send_sem.at[4],
            recv_sem=s_sem.at[0], device_id={"py": peer}, device_id_type=MESH,
        )

    def edge_copy(peer):
        return pltpu.make_async_remote_copy(
            src_ref=s_send.at[peer, 1, :, pl.ds(0, 8)], dst_ref=e_recv, send_sem=send_sem.at[10],
            recv_sem=s_sem.at[4], device_id={"py": peer}, device_id_type=MESH,
        )

    others = [my_half * half_y + (my_place + step) % half_y for step in range(1, half_y)]
    across = [(1 - my_half) * half_y + step for step in range(half_y)]

    def send_spectrum():
        pl.when(me_y != 0)(lambda: strip_copy().start())
        for peer in others[1:] + others[:1]:
            half_copy(peer).start()

        @pl.when(my_place == 0)
        def _():
            for peer in across:
                edge_copy(peer).start()

    middle = (place == chips // 2) | (place == chips // 2 - 1)
    giver, taker = middle & (core == 0), middle & (core == 1)

    def hand_copy(chunk, f):
        return pltpu.make_async_remote_copy(
            src_ref=z_send.at[chunk, f, pl.ds((1 - my_half) * half_y, half_y)],
            dst_ref=h_recv.at[chunk, f], send_sem=send_sem.at[0],
            recv_sem=h_sem.at[chunk * members + f],
            device_id={"py": place * 2 + 1 - core}, device_id_type=MESH,
        )

    def z_copy(source, chunk, f, slot, peer, send):
        return pltpu.make_async_remote_copy(
            src_ref=source, dst_ref=z_recv.at[chunk, f, slot], send_sem=send_sem.at[send],
            recv_sem=z_sem.at[chunk * members + f], device_id={"py": peer}, device_id_type=MESH,
        )

    def z_start(chunk, f):
        @pl.when(giver)
        def _():
            hand_copy(chunk, f).start()
            for peer in others:
                z_copy(z_send.at[chunk, f, peer], chunk, f, me_y, peer, 0).start()

        @pl.when(jnp.logical_not(giver))
        def _():
            z_route.start((chunk, f), chunk * members + f)

        @pl.when(taker)
        def _():
            hand_copy(chunk, f).wait_recv()
            for step, peer in enumerate(across):
                z_copy(h_recv.at[chunk, f, step], chunk, f, me_y - 1, peer, 11).start()

    def own_spectrum():
        mirrored = jnp.concatenate(
            halves(spectrum[:, :, LANES : 2 * LANES].reshape(cells_x * cells_y, LANES)), 1
        )
        image[...] = mm(mirrored, mirror_z[...])
        for row in range(0, cells_y, 8):
            rows = pl.ds(row, 8)
            plain = [spectrum[x, rows, pl.ds(0, LANES)] for x in range(cells_x)]
            turned_z = []
            for x in range(cells_x):
                value = image[pl.ds(x * cells_y + row, 8)]
                turned_z.append(jnp.where(lane == 0, plain[x], value))
            for kind, arrays in enumerate((plain, turned_z)):
                moved = exchange(arrays, width)
                for group in range(cells_x):
                    s_send[group % ranks_y, kind, group // ranks_y, rows] = moved[group]
        strip = jnp.zeros((8, LANES), F32)
        for x in range(cells_x):
            for part in range(cells_y // 8):
                value = spectrum[x, pl.ds(part * 8, 8), pl.ds(LANES, 1)]
                strip = jnp.where((lane // width == x) & (quarter == part), value, strip)
        n_send[...] = strip

    for copy in copies[:2]:
        copy.wait()
    cells = cells_x * cells_y
    lined = [halves(noise[f].reshape(cells, length_z)) for f in range(members)]
    for tile in range(tiles):
        for f, (high, low) in enumerate(lined):
            both = mm(high, ahead[tile])
            both = both[:, :LANES] + both[:, LANES:] + mm(low, ahead[tile, :, pl.ds(0, LANES)])
            held[f, :, pl.ds(tile * LANES, LANES)] = both
        lanes = pl.ds(tile * LANES, LANES)
        for row in range(0, cells_y, 8):
            rows = pl.ds(row, 8)
            both = []
            for f in range(members):
                both.append(
                    exchange(
                        [held[f, pl.ds(x * cells_y + row, 8), lanes] for x in range(cells_x)],
                        width,
                    )
                )
            if tile == 0:
                both[0][0], both[1][0] = swap_slot(both[0][0], both[1][0], slots)
            for f in range(members):
                for group in range(cells_x):
                    chunk = tile * per_tile + group // ranks_y
                    z_send[chunk, f, group % ranks_y, rows] = both[f][group]
        if tile == 0:
            pl.semaphore_wait(barrier, ranks_y + slots - 2)
        for part in range(tile * per_tile * members, (tile + 1) * per_tile * members):
            z_start(part // members, part % members)
            if part == 0:
                for copy in copies[2:early]:
                    copy.wait()
                for copy in copies[early:]:
                    copy.start()
                own_spectrum()
                send_spectrum()

    for copy in copies[early:]:
        copy.wait()
    sides = cells_x // ranks_y
    rows_side = LANES // sides
    for target, source, count in ((back_hi, side_hi, 2), (back_lo, side_lo, 1)):
        blank = jnp.zeros((rows_side, length_z), BF16)
        for chunk in range(chunks):
            for block in range(count * sides):
                rows = pl.ds(block * rows_side, rows_side)
                for side in range(sides):
                    value = source[chunk] if block % sides == side else blank
                    target[chunk, rows, pl.ds(side * length_z, length_z)] = value

    spot = s_recv.at[pl.ds(0, half_y - 1)]
    pltpu.make_async_remote_copy(
        src_ref=spot, dst_ref=spot, send_sem=send_sem.at[4], recv_sem=s_sem.at[0],
        device_id={"py": others[0]}, device_id_type=MESH,
    ).wait_recv()
    edge_copy(others[0]).wait_recv()
    s_recv[my_place] = s_send[me_y]
    pair = [s_recv[:, 1, tile].reshape(rows_m, LANES) for tile in range(tiles)]
    pair = jnp.concatenate(halves(jnp.concatenate(pair, 1)), 0)
    held[1, pl.ds(0, rows_m)] = mm(mirror_y[...], pair)
    sublane = lax.broadcasted_iota(jnp.int32, (8, LANES), 0)
    for row in range(0, rows_m, 8):
        arrays = []
        for tile in range(tiles):
            arrays.append(s_recv[row // cells_y, 0, tile, pl.ds(row % cells_y, 8)])
            value = held[1, pl.ds(row, 8), pl.ds(tile * LANES, LANES)]
            if row == 0:
                value = jnp.where(sublane == 0, e_recv[tile], value)
            arrays.append(value)
        moved = exchange(arrays, 2)
        for rank in range(slots):
            t_send[rank, pl.ds(row, 8)] = moved[rank]
    t_route.start((), None)

    def strips_copy(source):
        return pltpu.make_async_remote_copy(
            src_ref=n_recv, dst_ref=m_recv.at[source], send_sem=send_sem.at[9],
            recv_sem=s_sem.at[3], device_id={"px": 0}, device_id_type=MESH,
        )

    def along_y(columns):
        high, low = halves(columns)
        both = mm(y_hi[...], jnp.concatenate([high, low], 1))
        return both[:, :LANES] + both[:, LANES:] + mm(y_lo[...], high)

    def combined(product, start, rows, ahead):
        by_cos = product[start : start + rows]
        by_sin = product[length_y + start : length_y + start + rows]
        return by_cos + turned(by_sin, slots, ahead)

    def y_ahead(chunk, f):
        part = chunk * members + f
        z_route.arrive((chunk, f), part)
        product = along_y(z_recv[chunk, f].reshape(length_y, LANES))
        for row in range(0, rows_part, 16):
            arrays = [combined(product, a * rows_part + row, 16, True) for a in range(slots)]
            moved = exchange(arrays, 1)
            for rank in range(slots):
                x_send[chunk, f, rank, pl.ds(row, 16)] = moved[rank]
        x_route.start((chunk, f), part)

    def gathered(ref, chunk, f):
        pieces = [[] for _ in range(slots)]
        for row in range(0, rows_part, 16):
            moved = exchange([ref[chunk, f, s, pl.ds(row, 16)] for s in range(slots)], 1)
            for index in range(slots):
                pieces[index].append(moved[index])
        return jnp.concatenate([piece for some in pieces for piece in some], 0)

    def along_x(values, table):
        product = mm(jnp.concatenate(halves(values), 1), table[...])
        return product[:, :LANES] + product[:, LANES:]

    def x_both(chunk, f):
        part = chunk * members + f
        x_route.arrive((chunk, f), part)
        table = other if part == 1 else tables.at[chunk]
        values = along_x(gathered(x_recv, chunk, f), x_ahead)
        values = along_x(values * table[...].reshape(length_y, LANES), x_back)
        for row in range(0, rows_part, 16):
            arrays = [values[a * rows_part + row : a * rows_part + row + 16] for a in range(slots)]
            moved = exchange(arrays, 1)
            for s in range(slots):
                w_send[chunk, f, s, pl.ds(row, 16)] = moved[s]
        w_route.start((chunk, f), part)

    def y_back(chunk, f):
        part = chunk * members + f
        w_route.arrive((chunk, f), part)
        product = along_y(gathered(w_recv, chunk, f))
        for p in range(ranks_y):
            b_send[chunk, f, p] = combined(product, p * cells_y, cells_y, False)
        b_route.start((chunk, f), part)

    def table_rows(tile, block, rows, part):
        even = lane % 2 == 0
        first = jnp.where(even, part, pltpu.roll(part, 1, 1))
        second = jnp.where(even, pltpu.roll(part, LANES - 1, 1), part)
        tables[tile * per_tile, block, rows] = first
        tables[tile * per_tile + 1, block, rows] = second
        if tile == 0:
            other[block, rows] = first

    def spectrum_tables():
        t_route.arrive((), None)
        images = [[] for _ in range(tiles)]
        for row in range(0, rows_m, 8):
            rows = pl.ds(row, 8)
            moved = exchange([t_recv[s, rows] for s in range(slots)], 2)
            for tile in range(tiles):
                table_rows(tile, my_half, rows, moved[2 * tile])
                images[tile].append(moved[2 * tile + 1])
        images = jnp.concatenate([piece for pieces in images for piece in pieces], 0)
        images = mm(jnp.concatenate(halves(images), 1), mirror_x[...])
        for tile in range(tiles):
            for row in range(0, rows_m, 8):
                at = tile * rows_m + row
                table_rows(tile, 1 - my_half, pl.ds(row, 8), images[at : at + 8])

        @pl.when((me_y == 0) & (me_x == 0))
        def _():
            spot = m_recv.at[pl.ds(1, slots - 1)]
            pltpu.make_async_remote_copy(
                src_ref=spot, dst_ref=spot, send_sem=send_sem.at[9], recv_sem=s_sem.at[3],
                device_id={"px": 1}, device_id_type=MESH,
            ).wait_recv()
            for p in range(ranks_y):
                strips = [n_recv[p] if s == 0 else m_recv[s, p] for s in range(slots)]
                for part in range(cells_y // 8):
                    value = strips[part]
                    for s in range(slots):
                        shift = (s - part) * 2 % LANES
                        moved = pltpu.roll(strips[s], shift, 1) if shift else strips[s]
                        value = jnp.where(quarter == s, moved, value)
                    at = p * cells_y + part * 8
                    other[at // rows_m, pl.ds(at % rows_m, 8)] = value

    @pl.when(me_y == 0)
    def _():
        spot = n_recv.at[pl.ds(0, ranks_y - 1)]
        pltpu.make_async_remote_copy(
            src_ref=spot, dst_ref=spot, send_sem=send_sem.at[8], recv_sem=s_sem.at[2],
            device_id={"py": 1}, device_id_type=MESH,
        ).wait_recv()
        n_recv[0] = n_send[...]
        pl.when(me_x != 0)(lambda: strips_copy(me_x).start())

    steps = {"y": y_ahead, "x": x_both, "b": y_back}

    def run(order):
        for step in order:
            if step == "T":
                spectrum_tables()
            else:
                steps[step[0]](int(step[1:]) // members, int(step[1:]) % members)

    run(ORDER)

    tall = cells // 4 // ranks_y
    def z_back(chunk, f):
        pieces = [[] for _ in range(ranks_y)]
        for row in range(0, cells_y, 8):
            rows = pl.ds(row, 8)
            arrays = [b_recv[chunk, f, group, rows] for group in range(ranks_y)]
            if chunk == 0:
                pair = [b_recv[0, 0, 0, rows], b_recv[0, 1, 0, rows]]
                arrays[0] = swap_slot(*pair, slots)[f]
            moved = exchange(arrays, width)
            for x in range(ranks_y):
                pieces[x].append(moved[x])
        high, low = halves(jnp.concatenate([piece for some in pieces for piece in some], 0))
        fields = mm(jnp.concatenate([high, low], 1), back_hi[chunk]) + mm(high, back_lo[chunk])
        if chunk > 0:
            fields = fields + partial[f]
        if chunk + 1 < chunks:
            partial[f] = fields
            return
        values = jnp.exp(0.5 * fields)
        for side in range(sides):
            lanes = slice(side * length_z, (side + 1) * length_z)
            cut = values[:, lanes].reshape(ranks_y, cells_y, length_z)
            modulus[f, pl.ds(side * ranks_y, ranks_y)] = cut
        high, low = halves(values)
        pooled = mm(pool_rows[...], high) + mm(pool_rows[...], low)
        pooled = [pooled[:, side * length_z : (side + 1) * length_z] for side in range(sides)]
        high, low = halves(jnp.concatenate(pooled, 0))
        coarse = mm(high, pool_columns[...]) + mm(low, pool_columns[...])
        per_side = ranks_y // sides
        height = coarse.shape[0] // sides
        for d in range(ranks_y):
            base = d // per_side * height
            at = base + d % per_side * tall
            c_send[f][d, pl.ds(0, tall)] = coarse[at : at + tall, :LANES]
            at = base + per_side * tall + d % per_side * 8
            value = coarse[at : at + 8, LANES:]
            value = jnp.where(lane < LANES // 2, value, pltpu.roll(value, 4, 0))
            if f == 0:
                lower[d] = value
            else:
                c_send[f][d, pl.ds(tall, 8)] = jnp.where(
                    sublane < 4, lower[d], pltpu.roll(value, 4, 0)
                )
        c_routes[f].start((), None)

    def pick(f):
        c_routes[f].arrive((), None)
        for g in range(ranks_y):
            d_send[f][g, pl.ds(0, tall)] = c_recv[f][group_table[0, g], pl.ds(0, tall)]
            if f == 1:
                second = c_recv[f][group_table[1, g], pl.ds(tall, 8)]
                third = c_recv[f][group_table[2, g], pl.ds(tall, 8)]
                d_send[f][g, pl.ds(tall, 8)] = jnp.where(lane < LANES // 2, second, third)
        d_routes[f].start((), None)

    for chunk in range(chunks):
        for f in range(members):
            b_route.arrive((chunk, f), chunk * members + f)
            if chunk > 0:
                z_back(chunk, f)
        if chunk == 0:
            for f in range(members):
                z_back(chunk, f)
    for f in range(members):
        pick(f)
    for f in range(members):
        d_routes[f].arrive((), None)

    every = pl.ds(0, chunks)
    z_route.drain((every, pl.ds(0, members)))

    @pl.when(taker)
    def _():
        pltpu.make_async_remote_copy(
            src_ref=h_recv, dst_ref=h_recv, send_sem=send_sem.at[11], recv_sem=h_sem.at[0],
            device_id={"py": others[0]}, device_id_type=MESH,
        ).wait_send()

    x_route.drain((every, pl.ds(0, members)))
    w_route.drain((every, pl.ds(0, members)))
    b_route.drain((every, pl.ds(0, members)))
    spot = s_send.at[pl.ds(0, half_y - 1)]
    pltpu.make_async_remote_copy(
        src_ref=spot, dst_ref=spot, send_sem=send_sem.at[4], recv_sem=s_sem.at[0],
        device_id={"py": others[0]}, device_id_type=MESH,
    ).wait_send()

    @pl.when(my_place == 0)
    def _():
        spot = s_send.at[pl.ds(0, half_y), 1, :, pl.ds(0, 8)]
        pltpu.make_async_remote_copy(
            src_ref=spot, dst_ref=spot, send_sem=send_sem.at[10], recv_sem=s_sem.at[4],
            device_id={"py": others[0]}, device_id_type=MESH,
        ).wait_send()

    t_route.drain(())
    for some in c_routes + d_routes:
        some.drain(())
    pl.when(me_y != 0)(lambda: strip_copy().wait_send())
    pl.when((me_y == 0) & (me_x != 0))(lambda: strips_copy(me_x).wait_send())


def leaving_kernel(modulus, first, second, modulus_out, one_out, level_two, level_three, sems):
    members, cells_x, cells_y, length_z = modulus.shape
    ranks_y, tall = first.shape[:2]
    copies = []
    for f, coarse in enumerate((first, second)):
        for x in range(0, cells_x, 2):
            rows = pl.ds(x, 2)
            copies.append((modulus.at[f, rows], modulus_out.at[f, rows]))
        copies.append((coarse.at[:, pl.ds(0, tall)], one_out.at[f]))
    copies = [
        pltpu.make_async_copy(source, target, sems.at[index])
        for index, (source, target) in enumerate(copies)
    ]
    for copy in copies:
        copy.start()
    row = lax.broadcasted_iota(jnp.int32, (8, LANES), 0)
    short = cells_y // 4
    lows = [second[d, pl.ds(tall, 8)] for d in range(ranks_y)]
    for f in range(members):
        shifts = [4 * f, 4 - 4 * f]
        for x in range(ranks_y // 2):
            pair = [
                pltpu.roll(low, shift, 0) if shift else low
                for low, shift in zip(lows[2 * x : 2 * x + 2], shifts)
            ]
            value = jnp.where(row < 4, *pair)
            level_two[f, x] = value[:short, : length_z // 4]
        for x in range(ranks_y // 4):
            value = jnp.zeros((8, LANES), F32)
            for y in range(4):
                low = lows[4 * x + y]
                shift = (y - 4 * f) % 8
                low = pltpu.roll(low, shift, 0) if shift else low
                value = jnp.where(row == y, low, value)
            value = pltpu.roll(value, LANES // 2, 1)
            level_three[f, x] = value[: short // 2, : length_z // 8]
    for copy in copies:
        copy.wait()


def lanes_path(white_noise, spectrum, group_table):
    members, cells_x, cells_y, length_z = white_noise.shape
    size_px, size_py = lax.axis_size("px"), lax.axis_size("py")
    length_x, length_y = cells_x * size_px, cells_y * size_py
    slots, width = size_px, 2 * size_px
    tiles = length_z // LANES
    per_tile = cells_x // size_py
    chunks = tiles * per_tile
    blocks = slots // members
    rows_m = length_y // blocks

    column = np.arange(length_z)
    tile, lane = column // LANES, column % LANES
    part = (lane // slots) % 2
    group = lane // width
    rank_q, rank_p, inner = lane % slots, group % size_py, group // size_py
    k = ((tile * size_py + rank_p) * slots + rank_q) * per_tile + inner
    angles = angles_of(length_z)
    sign = np.where(np.arange(length_z) % 2 == 0, 1.0, -1.0)
    z_ahead = np.where(part == 0, np.cos(angles[:, k]), -np.sin(angles[:, k]))
    z_back = 2.0 * z_ahead
    first = (k == 0) & (part == 0)
    second = (k == 0) & (part == 1)
    z_ahead[:, second] = sign[:, None]
    z_back[:, first] = 1.0
    z_back[:, second] = sign[:, None]
    z_back = z_back.T / (length_x * length_y * length_z)

    sides = cells_x // size_py
    half_cells = cells_x * cells_y // sides
    back_hi, back_lo = host_halves(z_back.reshape(chunks, LANES // sides, length_z))

    angles = angles_of(length_y)
    y_table = np.concatenate([np.cos(angles), np.sin(angles)], 0)

    lane = np.arange(LANES)
    cell = (lane // slots % 2, lane % slots * cells_x + lane // width)
    mode = (lane % 2, lane // 2 % slots * cells_x + lane // width)

    def x_table(direction, rows, columns):
        table = complex_array(length_x, direction)[rows][:, columns[0], columns[1]]
        high, low = host_halves(table)
        return jnp.concatenate(
            [
                jnp.concatenate([high, low], 1),
                jnp.concatenate([high, jnp.zeros_like(low)], 1),
            ],
            0,
        )

    at = np.arange(1, LANES)
    mirror_z = np.zeros((LANES, LANES))
    mirror_z[LANES - at, at] = 1.0
    at = np.arange(1, rows_m)
    mirror_y = np.zeros((rows_m, rows_m))
    mirror_y[at, rows_m - at] = 1.0
    same = (mode[1][:, None] + mode[1][None]) % length_x == 0
    mirror_x = np.where(same & (mode[0][:, None] == mode[0][None]), 1.0, 0.0)

    def pool(extent_x, extent_y, factor):
        short_x, short_y = extent_x // factor, extent_y // factor
        row, cell = np.arange(short_x * short_y), np.arange(extent_x * extent_y)
        same_x = cell[None] // extent_y // factor == row[:, None] // short_y
        same_y = cell[None] % extent_y // factor == row[:, None] % short_y
        return np.where(same_x & same_y, 1.0 / factor**3, 0.0)

    per_side = size_py // sides
    some = size_py, cells_y
    lower = np.zeros((per_side, 8, half_cells))
    lower[:, :4] = pool(*some, 4).reshape(per_side, 4, -1)
    lower[:, 4:5] = pool(*some, 8).reshape(per_side, 1, -1)
    pool_rows = np.concatenate([pool(*some, 2), lower.reshape(8 * per_side, -1)], 0)
    pool_columns = np.zeros((length_z, 2 * LANES))
    z = np.arange(length_z)
    pool_columns[z, z // 2] = 1.0
    pool_columns[z, LANES + z // 4] = 1.0
    pool_columns[z, LANES + length_z // 4 + z // 8] = 1.0

    ahead = [
        jnp.concatenate(host_halves(z_ahead[:, at : at + LANES]), 1)
        for at in range(0, length_z, LANES)
    ]
    held_in = [
        white_noise,
        jnp.stack(ahead),
        spectrum,
        jnp.asarray(np.tile(mirror_z, (2, 1)), BF16),
        jnp.asarray(np.tile(mirror_x, (2, 1)), BF16),
        jnp.asarray(np.tile(mirror_y, (1, 2)), BF16),
        *host_halves(y_table),
        x_table(-1.0, cell, mode),
        x_table(1.0, mode, cell),
        back_hi,
        back_lo,
        jnp.asarray(pool_rows, BF16),
        jnp.asarray(pool_columns, BF16),
        group_table,
    ]
    sizes = (cells_x, cells_y, length_z, slots, size_py)

    def body(*refs):
        whole_kernel(sizes, len(held_in), *refs)

    def vmem(*shape):
        return pltpu.VMEM(shape, F32)

    x_shape = (chunks, members, slots, length_y // slots, LANES)
    b_shape = (chunks, members, size_py, cells_y, LANES)
    s_shape = (2, tiles, cells_y, LANES)
    t_shape = (slots, rows_m, LANES)
    tall = cells_x * cells_y // 4 // size_py
    c_shapes = [(size_py, tall, LANES), (size_py, tall + 8, LANES)]
    sem = pltpu.SemaphoreType.DMA
    scratch = [pltpu.VMEM(value.shape, value.dtype) for value in held_in[:-1]]
    scratch.append(pltpu.SMEM(group_table.shape, group_table.dtype))
    for shape in (b_shape, x_shape, x_shape, b_shape):
        scratch += [vmem(*shape), vmem(*shape)]
    scratch += [vmem(size_py, *s_shape), vmem(size_py // 2, *s_shape), vmem(tiles, 8, LANES)]
    scratch += [vmem(*t_shape), vmem(*t_shape)]
    scratch += [vmem(8, LANES), vmem(size_py, 8, LANES), vmem(slots, size_py, 8, LANES)]
    scratch += [
        vmem(chunks, blocks, rows_m, LANES),
        vmem(blocks, rows_m, LANES),
        vmem(members, cells_x * cells_y, length_z),
        vmem(cells_x * cells_y, LANES),
        vmem(members, half_cells, sides * length_z),
        pltpu.VMEM((chunks, 2 * LANES, sides * length_z), BF16),
        pltpu.VMEM((chunks, LANES, sides * length_z), BF16),
        vmem(size_py, 8, LANES),
        vmem(chunks, members, size_py // 2, cells_y, LANES),
        *[vmem(*shape) for shape in c_shapes * 3],
    ]
    scratch += [
        sem((len(held_in),)), sem((16,)), sem((chunks * members,)), sem((chunks * members,)),
        sem((chunks * members,)), sem((chunks * members,)), sem((members,)), sem((members,)), sem((5,)), sem((chunks * members,)),
    ]
    hbm = pl.BlockSpec(memory_space=pltpu.HBM)
    local = pl.BlockSpec(memory_space=pltpu.VMEM)
    leaving = pl.pallas_call(
        body,
        out_shape=[jax.ShapeDtypeStruct(shape, F32) for shape in [white_noise.shape] + c_shapes],
        in_specs=[hbm] * len(held_in),
        out_specs=[local] * 3,
        scratch_shapes=scratch,
        compiler_params=pltpu.CompilerParams(
            collective_id=0, has_side_effects=True, vmem_limit_bytes=40 * 1024 * 1024
        ),
    )(*[pltpu.with_memory_space_constraint(v, pltpu.HBM) for v in held_in])
    outs = [white_noise.shape]
    for level in range(1, 4):
        outs.append((members,) + tuple(extent >> level for extent in white_noise.shape[1:]))
    return tuple(
        pl.pallas_call(
            leaving_kernel,
            out_shape=[jax.ShapeDtypeStruct(shape, F32) for shape in outs],
            in_specs=[local] * 3,
            out_specs=[hbm, hbm, local, local],
            scratch_shapes=[sem((members * (cells_x // 2 + 1),))],
            compiler_params=pltpu.CompilerParams(vmem_limit_bytes=4 * 1024 * 1024),
        )(*leaving)
    )


def on_device(white_noise, spectrum, group_table):
    members, cells_x, cells_y, length_z = white_noise.shape
    size_px, size_py = lax.axis_size("px"), lax.axis_size("py")
    fits = members == 2 and length_z == 2 * LANES and size_px == 4 and size_py == 8
    fits = fits and 2 * cells_x * size_px == LANES and cells_x == 2 * size_py
    fits = fits and cells_y == 2 * cells_x
    chosen = lanes_path if fits else general_path
    return chosen(white_noise, spectrum, group_table)


def solution(mesh):
    in_specs = (P(None, "px", "py", None), P("px", "py", None), P())
    out_specs = (P(None, "px", "py", None),) * 4
    return jax.shard_map(
        on_device, mesh=mesh, in_specs=in_specs, out_specs=out_specs, check_vma=False
    )
```

```python
import numpy as np

import jax
import jax.numpy as jnp
from jax import lax
from jax.experimental import pallas as pl
from jax.experimental.pallas import tpu as pltpu
from jax.sharding import PartitionSpec as P


def angles_of(length):
    positions = np.arange(length, dtype=np.int64)
    return (positions[:, None] * positions[None, :] % length) * (2.0 * np.pi / length)


def complex_array(length, direction):
    angles = angles_of(length)
    cos, sin = np.cos(angles), direction * np.sin(angles)
    return np.stack([np.stack([cos, sin], 1), np.stack([-sin, cos], 1)], 0)


def complex_table(length, direction):
    return jnp.asarray(complex_array(length, direction), jnp.float32)


def half_tables(length):
    angles = angles_of(length)[:, : length // 2]
    ahead = np.stack([np.cos(angles), -np.sin(angles)], 1)
    back = 2.0 * ahead
    nyquist = np.where(np.arange(length) % 2 == 0, 1.0, -1.0)
    ahead[:, 1, 0] = nyquist
    back[:, 0, 0] = 1.0
    back[:, 1, 0] = nyquist
    return jnp.asarray(ahead, jnp.float32), jnp.asarray(back, jnp.float32)


def einsum(pattern, left, right):
    return jnp.einsum(pattern, left, right, precision=lax.Precision.HIGH)


def swap_first(values):
    first = values[:, :, :1]
    turned = jnp.swapaxes(first, 0, 1)
    return jnp.concatenate([turned, values[:, :, 1:]], 2)


def coarsen(values):
    members, size_x, size_y, size_z = values.shape
    blocks = values.reshape(members, size_x // 2, 2, size_y // 2, 2, size_z // 2, 2)
    return blocks.mean(axis=(2, 4, 6))


def general_path(white_noise, spectrum, group_table):
    members, cells_x, cells_y, length_z = white_noise.shape
    size_px, size_py = lax.axis_size("px"), lax.axis_size("py")
    length_x, length_y = cells_x * size_px, cells_y * size_py
    half_z = length_z // 2
    block_py, block = half_z // size_py, half_z // size_py // size_px
    z_ahead, z_back = half_tables(length_z)
    scale = 1.0 / (length_x * length_y * length_z)

    table = jnp.transpose(spectrum, (2, 0, 1))
    last = jnp.broadcast_to(table[half_z : half_z + 1], (size_py, 1, cells_x, cells_y))
    table = jnp.concatenate([table[:half_z].reshape(size_py, block_py, cells_x, cells_y), last], 1)
    table = lax.all_to_all(table, "py", split_axis=0, concat_axis=3, tiled=True)[0]
    last = jnp.broadcast_to(table[block_py:], (size_px, 1, cells_x, length_y))
    table = jnp.concatenate([table[:block_py].reshape(size_px, block, cells_x, length_y), last], 1)
    table = lax.all_to_all(table, "px", split_axis=0, concat_axis=2, tiled=True)[0] * scale
    is_first = (lax.axis_index("px") == 0) & (lax.axis_index("py") == 0)
    other = jnp.where(is_first, table[block:], table[:1])
    tables = jnp.stack([table[:block], jnp.concatenate([other, table[1:block]], 0)], 0)

    values = einsum("fxyz,zck->fckxy", white_noise, z_ahead)
    values = swap_first(values)
    values = lax.all_to_all(values, "py", split_axis=2, concat_axis=4, tiled=True)
    values = einsum("fckxy,cydm->fdkxm", values, complex_table(length_y, -1.0))
    values = lax.all_to_all(values, "px", split_axis=2, concat_axis=3, tiled=True)
    values = einsum("fckxm,cxdj->fdkjm", values, complex_table(length_x, -1.0))
    values = values * tables[:, None]
    values = einsum("fckjm,cjdx->fdkxm", values, complex_table(length_x, 1.0))
    values = lax.all_to_all(values, "px", split_axis=3, concat_axis=2, tiled=True)
    values = einsum("fckxm,cmdy->fdkxy", values, complex_table(length_y, 1.0))
    values = lax.all_to_all(values, "py", split_axis=4, concat_axis=2, tiled=True)
    values = swap_first(values)
    fields = einsum("fckxy,zck->fxyz", values, z_back)
    modulus = jnp.exp(0.5 * fields)

    levels = []
    level = modulus
    for _ in range(3):
        level = coarsen(level)
        levels.append(level)
    pieces = [jnp.reshape(level, (size_py, -1)) for level in levels]
    widths = [piece.shape[1] for piece in pieces]
    joined = jnp.concatenate(pieces, 1)
    spread = lax.all_to_all(joined, "py", split_axis=0, concat_axis=0, tiled=True)
    picked, start = [], 0
    for index, width in enumerate(widths):
        part = spread[:, start : start + width]
        picked.append(jnp.take(part, group_table[index], axis=0))
        start += width
    joined = lax.all_to_all(
        jnp.concatenate(picked, 1), "py", split_axis=0, concat_axis=0, tiled=True
    )
    routed, start = [], 0
    for level, width in zip(levels, widths):
        routed.append(joined[:, start : start + width].reshape(level.shape))
        start += width
    return (modulus, routed[0], routed[1], routed[2])


LANES = 128
ORDER = (
    "y0", "y1", "T", "y2", "x0", "y3", "x1", "y4", "x2", "b0", "x3", "y5", "b1",
    "y6", "x4", "b2", "y7", "b3", "x5", "x6", "b4", "x7", "b5", "b6", "b7",
)
MESH = pl.DeviceIdType.MESH
BF16 = jnp.bfloat16
F32 = jnp.float32


def halves(values):
    high = values.astype(BF16)
    low = (values - high.astype(F32)).astype(BF16)
    return high, low


def host_halves(values):
    values = np.asarray(values, np.float64)
    high = values.astype(np.float32).astype(BF16)
    low = (values - high.astype(np.float64)).astype(np.float32).astype(BF16)
    return jnp.asarray(high), jnp.asarray(low)


def mm(left, right):
    return jnp.dot(left, right, preferred_element_type=F32)


def lane_of(shape):
    return lax.broadcasted_iota(jnp.int32, shape, len(shape) - 1)


def exchange(arrays, width):
    count = len(arrays)
    field = (lane_of(arrays[0].shape) // width) % count
    skewed = [pltpu.roll(a, i * width, 1) if i else a for i, a in enumerate(arrays)]
    moved = [skewed[-index % count] for index in range(count)]
    distance = 1
    while distance < count:
        take = (field // distance) % 2 == 1
        moved = [
            jnp.where(take, moved[(index - distance) % count], moved[index])
            for index in range(count)
        ]
        distance *= 2
    return [pltpu.roll(m, LANES - i * width, 1) if i else m for i, m in enumerate(moved)]


def turned(values, slots, ahead):
    real = (lane_of(values.shape) // slots) % 2 == 0
    from_imag = pltpu.roll(values, LANES - slots, 1)
    from_real = pltpu.roll(values, slots, 1)
    if ahead:
        return jnp.where(real, from_imag, -from_real)
    return jnp.where(real, -from_imag, from_real)


def swap_slot(first, second, slots):
    place = lane_of(first.shape) % (2 * slots)
    return (
        jnp.where(place == slots, pltpu.roll(second, slots, 1), first),
        jnp.where(place == 0, pltpu.roll(first, LANES - slots, 1), second),
    )


class Route:
    def __init__(self, axis, count, away, source, target, send, recv):
        self.axis, self.count, self.away = axis, count, away
        self.source, self.target = source, target
        self.send, self.recv = send, recv
        self.me = lax.axis_index(axis)

    def copy(self, source, target, peer, part):
        return pltpu.make_async_remote_copy(
            src_ref=source,
            dst_ref=target,
            send_sem=self.send,
            recv_sem=self.recv.at[part] if part is not None else self.recv,
            device_id={self.axis: peer},
            device_id_type=MESH,
        )

    def at(self, ref, where, index):
        return ref.at[where + (index,)]

    def start(self, where, part):
        for peer in self.away:
            source = self.at(self.source, where, peer)
            target = self.at(self.target, where, self.me)
            self.copy(source, target, peer, part).start()

    def arrive(self, where, part):
        spot = self.at(self.target, where, pl.ds(0, self.count - 1))
        self.copy(spot, spot, self.away[0], part).wait_recv()
        self.target[where + (self.me,)] = self.source[where + (self.me,)]

    def drain(self, where):
        spot = self.source.at[where + (pl.ds(0, self.count - 1),)]
        self.copy(spot, spot, self.away[0], 0 if len(self.recv.shape) else None).wait_send()


def whole_kernel(sizes, loads, *refs):
    cells_x, cells_y, length_z, slots, ranks_y = sizes
    members = 2
    width = 2 * slots
    per_tile = cells_x // ranks_y
    tiles = length_z // LANES
    chunks = tiles * per_tile
    length_y = cells_y * ranks_y
    blocks = slots // members
    rows_m = length_y // blocks
    rows_part = length_y // slots
    sources, held_in = refs[:loads], refs[3 + loads : 3 + 2 * loads]
    modulus, d_recv_0, d_recv_1 = refs[loads : 3 + loads]
    (
        z_send, z_recv, x_send, x_recv, w_send, w_recv, b_send, b_recv,
        s_send, s_recv, e_recv, t_send, t_recv, n_send, n_recv, m_recv,
        tables, other, held, image, partial, back_hi, back_lo, h_recv, g_recv, c_send_0, c_send_1, c_recv_0, c_recv_1,
        d_send_0, d_send_1,
        load_sem, send_sem, z_sem, x_sem, w_sem, b_sem, c_sem, d_sem, s_sem, h_sem, g_sem,
    ) = refs[3 + 2 * loads :]
    (
        noise, ahead, spectrum, mirror_z, mirror_x, mirror_y, y_hi, y_lo, x_ahead, x_back,
        side_hi, side_lo, pool_rows, pool_columns, group_table,
    ) = held_in

    me_x, me_y = lax.axis_index("px"), lax.axis_index("py")
    pairs = [(sources[0].at[f], noise.at[f]) for f in range(members)]
    pairs = [pairs[0], (sources[1], ahead), *pairs[1:], *list(zip(sources, held_in))[2:]]
    copies = [
        pltpu.make_async_copy(source, target, load_sem.at[index])
        for index, (source, target) in enumerate(pairs)
    ]
    place, core = me_y // 2, me_y % 2
    chips = ranks_y // 2
    near = chips - 1 - (chips - 2) * (place % 2)
    steps = [chips // 2, near, chips - near]
    away_y = []
    for step in steps:
        for side in (0, 1):
            away_y.append((place + step) % chips * 2 + (core + side) % 2)
    away_y.append(place * 2 + 1 - core)
    away_x = [slots - 1 - me_x, (me_x + 2) % slots, me_x + 1 - 2 * (me_x % 2)]

    barrier = pltpu.get_barrier_semaphore()
    for peer in away_y:
        pl.semaphore_signal(barrier, inc=1, device_id={"py": peer}, device_id_type=MESH)
    for peer in away_x:
        pl.semaphore_signal(barrier, inc=1, device_id={"px": peer}, device_id_type=MESH)

    early = 5
    for copy in copies[:early]:
        copy.start()

    def route(axis, source, target, send, recv):
        away, count = (away_y, ranks_y) if axis == "py" else (away_x, slots)
        return Route(axis, count, away, source, target, send_sem.at[send], recv)

    z_route = route("py", z_send, z_recv, 0, z_sem)
    x_route = route("px", x_send, x_recv, 1, x_sem)
    w_route = route("px", w_send, w_recv, 2, w_sem)
    b_route = route("py", b_send, b_recv, 3, b_sem)
    t_route = route("px", t_send, t_recv, 5, s_sem.at[1])
    c_send, c_recv = (c_send_0, c_send_1), (c_recv_0, c_recv_1)
    d_send, d_recv = (d_send_0, d_send_1), (d_recv_0, d_recv_1)
    c_routes = [route("py", c_send[f], c_recv[f], 12 + f, c_sem.at[f]) for f in range(members)]
    d_routes = [route("py", d_send[f], d_recv[f], 14 + f, d_sem.at[f]) for f in range(members)]

    lane = lane_of((8, LANES))
    quarter = (lane // 2) % slots
    half_y = ranks_y // 2
    my_half, my_place = me_y // half_y, me_y % half_y

    def strip_copy():
        return pltpu.make_async_remote_copy(
            src_ref=n_send, dst_ref=n_recv.at[me_y], send_sem=send_sem.at[8],
            recv_sem=s_sem.at[2], device_id={"py": 0}, device_id_type=MESH,
        )

    def half_copy(peer):
        return pltpu.make_async_remote_copy(
            src_ref=s_send.at[peer], dst_ref=s_recv.at[my_place], send_sem=send_sem.at[4],
            recv_sem=s_sem.at[0], device_id={"py": peer}, device_id_type=MESH,
        )

    def edge_copy(peer):
        return pltpu.make_async_remote_copy(
            src_ref=s_send.at[peer, 1, :, pl.ds(0, 8)], dst_ref=e_recv, send_sem=send_sem.at[10],
            recv_sem=s_sem.at[4], device_id={"py": peer}, device_id_type=MESH,
        )

    others = [my_half * half_y + (my_place + step) % half_y for step in range(1, half_y)]
    across = [(1 - my_half) * half_y + step for step in range(half_y)]

    def send_spectrum():
        pl.when(me_y != 0)(lambda: strip_copy().start())
        for peer in others[1:] + others[:1]:
            half_copy(peer).start()

        @pl.when(my_place == 0)
        def _():
            for peer in across:
                edge_copy(peer).start()

    middle = (place == chips // 2) | (place == chips // 2 - 1)
    giver, taker = middle & (core == 0), middle & (core == 1)

    def shared_start(route, where, part, hand, hand_sem, extra):
        source, target = route.source, route.target
        blocks_away = source.at[where + (pl.ds((1 - my_half) * half_y, half_y),)]

        def hand_copy():
            return pltpu.make_async_remote_copy(
                src_ref=blocks_away, dst_ref=hand, send_sem=route.send, recv_sem=hand_sem,
                device_id={"py": place * 2 + 1 - core}, device_id_type=MESH,
            )

        @pl.when(giver)
        def _():
            hand_copy().start()
            for peer in others:
                spot = source.at[where + (peer,)]
                route.copy(spot, target.at[where + (me_y,)], peer, part).start()

        @pl.when(jnp.logical_not(giver))
        def _():
            route.start(where, part)

        @pl.when(taker)
        def _():
            hand_copy().wait_recv()
            for step, peer in enumerate(across):
                pltpu.make_async_remote_copy(
                    src_ref=hand.at[step], dst_ref=target.at[where + (me_y - 1,)],
                    send_sem=send_sem.at[extra], recv_sem=route.recv.at[part],
                    device_id={"py": peer}, device_id_type=MESH,
                ).start()

    def z_start(chunk, f):
        part = chunk * members + f
        shared_start(z_route, (chunk, f), part, h_recv.at[chunk, f], h_sem.at[part], 11)

    def own_spectrum():
        mirrored = jnp.concatenate(
            halves(spectrum[:, :, LANES : 2 * LANES].reshape(cells_x * cells_y, LANES)), 1
        )
        image[...] = mm(mirrored, mirror_z[...])
        for row in range(0, cells_y, 8):
            rows = pl.ds(row, 8)
            plain = [spectrum[x, rows, pl.ds(0, LANES)] for x in range(cells_x)]
            turned_z = []
            for x in range(cells_x):
                value = image[pl.ds(x * cells_y + row, 8)]
                turned_z.append(jnp.where(lane == 0, plain[x], value))
            for kind, arrays in enumerate((plain, turned_z)):
                moved = exchange(arrays, width)
                for group in range(cells_x):
                    s_send[group % ranks_y, kind, group // ranks_y, rows] = moved[group]
        strip = jnp.zeros((8, LANES), F32)
        for x in range(cells_x):
            for part in range(cells_y // 8):
                value = spectrum[x, pl.ds(part * 8, 8), pl.ds(LANES, 1)]
                strip = jnp.where((lane // width == x) & (quarter == part), value, strip)
        n_send[...] = strip

    cells = cells_x * cells_y
    lined = []
    for tile in range(tiles):
        for f in range(members):
            if tile == 0:
                for copy in copies[2 * f : 2 + f]:
                    copy.wait()
                lined.append(halves(noise[f].reshape(cells, length_z)))
            high, low = lined[f]
            both = mm(high, ahead[tile])
            both = both[:, :LANES] + both[:, LANES:] + mm(low, ahead[tile, :, pl.ds(0, LANES)])
            held[f, :, pl.ds(tile * LANES, LANES)] = both
        lanes = pl.ds(tile * LANES, LANES)
        for row in range(0, cells_y, 8):
            rows = pl.ds(row, 8)
            both = []
            for f in range(members):
                both.append(
                    exchange(
                        [held[f, pl.ds(x * cells_y + row, 8), lanes] for x in range(cells_x)],
                        width,
                    )
                )
            if tile == 0:
                both[0][0], both[1][0] = swap_slot(both[0][0], both[1][0], slots)
            for f in range(members):
                for group in range(cells_x):
                    chunk = tile * per_tile + group // ranks_y
                    z_send[chunk, f, group % ranks_y, rows] = both[f][group]
        if tile == 0:
            pl.semaphore_wait(barrier, ranks_y + slots - 2)
        for part in range(tile * per_tile * members, (tile + 1) * per_tile * members):
            z_start(part // members, part % members)
            if part == 0:
                for copy in copies[3:early]:
                    copy.wait()
                for copy in copies[early:]:
                    copy.start()
                own_spectrum()
                send_spectrum()

    for copy in copies[early:]:
        copy.wait()
    sides = cells_x // ranks_y
    rows_side = LANES // sides
    for target, source, count in ((back_hi, side_hi, 2), (back_lo, side_lo, 1)):
        blank = jnp.zeros((rows_side, length_z), BF16)
        for chunk in range(chunks):
            for block in range(count * sides):
                rows = pl.ds(block * rows_side, rows_side)
                for side in range(sides):
                    value = source[chunk] if block % sides == side else blank
                    target[chunk, rows, pl.ds(side * length_z, length_z)] = value

    spot = s_recv.at[pl.ds(0, half_y - 1)]
    pltpu.make_async_remote_copy(
        src_ref=spot, dst_ref=spot, send_sem=send_sem.at[4], recv_sem=s_sem.at[0],
        device_id={"py": others[0]}, device_id_type=MESH,
    ).wait_recv()
    edge_copy(others[0]).wait_recv()
    s_recv[my_place] = s_send[me_y]
    pair = [s_recv[:, 1, tile].reshape(rows_m, LANES) for tile in range(tiles)]
    pair = jnp.concatenate(halves(jnp.concatenate(pair, 1)), 0)
    held[1, pl.ds(0, rows_m)] = mm(mirror_y[...], pair)
    sublane = lax.broadcasted_iota(jnp.int32, (8, LANES), 0)
    for row in range(0, rows_m, 8):
        arrays = []
        for tile in range(tiles):
            arrays.append(s_recv[row // cells_y, 0, tile, pl.ds(row % cells_y, 8)])
            value = held[1, pl.ds(row, 8), pl.ds(tile * LANES, LANES)]
            if row == 0:
                value = jnp.where(sublane == 0, e_recv[tile], value)
            arrays.append(value)
        moved = exchange(arrays, 2)
        for rank in range(slots):
            t_send[rank, pl.ds(row, 8)] = moved[rank]
    t_route.start((), None)

    def strips_copy(source):
        return pltpu.make_async_remote_copy(
            src_ref=n_recv, dst_ref=m_recv.at[source], send_sem=send_sem.at[9],
            recv_sem=s_sem.at[3], device_id={"px": 0}, device_id_type=MESH,
        )

    def along_y(columns):
        high, low = halves(columns)
        both = mm(y_hi[...], jnp.concatenate([high, low], 1))
        return both[:, :LANES] + both[:, LANES:] + mm(y_lo[...], high)

    def combined(product, start, rows, ahead):
        by_cos = product[start : start + rows]
        by_sin = product[length_y + start : length_y + start + rows]
        return by_cos + turned(by_sin, slots, ahead)

    def y_ahead(chunk, f):
        part = chunk * members + f
        z_route.arrive((chunk, f), part)
        product = along_y(z_recv[chunk, f].reshape(length_y, LANES))
        for row in range(0, rows_part, 16):
            arrays = [combined(product, a * rows_part + row, 16, True) for a in range(slots)]
            moved = exchange(arrays, 1)
            for rank in range(slots):
                x_send[chunk, f, rank, pl.ds(row, 16)] = moved[rank]
        x_route.start((chunk, f), part)

    def gathered(ref, chunk, f):
        pieces = [[] for _ in range(slots)]
        for row in range(0, rows_part, 16):
            moved = exchange([ref[chunk, f, s, pl.ds(row, 16)] for s in range(slots)], 1)
            for index in range(slots):
                pieces[index].append(moved[index])
        return jnp.concatenate([piece for some in pieces for piece in some], 0)

    def along_x(values, table):
        product = mm(jnp.concatenate(halves(values), 1), table[...])
        return product[:, :LANES] + product[:, LANES:]

    def x_both(chunk, f):
        part = chunk * members + f
        x_route.arrive((chunk, f), part)
        table = other if part == 1 else tables.at[chunk]
        values = along_x(gathered(x_recv, chunk, f), x_ahead)
        values = along_x(values * table[...].reshape(length_y, LANES), x_back)
        for row in range(0, rows_part, 16):
            arrays = [values[a * rows_part + row : a * rows_part + row + 16] for a in range(slots)]
            moved = exchange(arrays, 1)
            for s in range(slots):
                w_send[chunk, f, s, pl.ds(row, 16)] = moved[s]
        w_route.start((chunk, f), part)

    def y_back(chunk, f):
        part = chunk * members + f
        w_route.arrive((chunk, f), part)
        product = along_y(gathered(w_recv, chunk, f))
        for p in range(ranks_y):
            b_send[chunk, f, p] = combined(product, p * cells_y, cells_y, False)
        late = part - (chunks * members - g_recv.shape[0])
        if late >= 0:
            shared_start(b_route, (chunk, f), part, g_recv.at[late], g_sem.at[late], 7)
        else:
            b_route.start((chunk, f), part)

    def table_rows(tile, block, rows, part):
        even = lane % 2 == 0
        first = jnp.where(even, part, pltpu.roll(part, 1, 1))
        second = jnp.where(even, pltpu.roll(part, LANES - 1, 1), part)
        tables[tile * per_tile, block, rows] = first
        tables[tile * per_tile + 1, block, rows] = second
        if tile == 0:
            other[block, rows] = first

    def spectrum_tables():
        t_route.arrive((), None)
        images = [[] for _ in range(tiles)]
        for row in range(0, rows_m, 8):
            rows = pl.ds(row, 8)
            moved = exchange([t_recv[s, rows] for s in range(slots)], 2)
            for tile in range(tiles):
                table_rows(tile, my_half, rows, moved[2 * tile])
                images[tile].append(moved[2 * tile + 1])
        images = jnp.concatenate([piece for pieces in images for piece in pieces], 0)
        images = mm(jnp.concatenate(halves(images), 1), mirror_x[...])
        for tile in range(tiles):
            for row in range(0, rows_m, 8):
                at = tile * rows_m + row
                table_rows(tile, 1 - my_half, pl.ds(row, 8), images[at : at + 8])

        @pl.when((me_y == 0) & (me_x == 0))
        def _():
            spot = m_recv.at[pl.ds(1, slots - 1)]
            pltpu.make_async_remote_copy(
                src_ref=spot, dst_ref=spot, send_sem=send_sem.at[9], recv_sem=s_sem.at[3],
                device_id={"px": 1}, device_id_type=MESH,
            ).wait_recv()
            for p in range(ranks_y):
                strips = [n_recv[p] if s == 0 else m_recv[s, p] for s in range(slots)]
                for part in range(cells_y // 8):
                    value = strips[part]
                    for s in range(slots):
                        shift = (s - part) * 2 % LANES
                        moved = pltpu.roll(strips[s], shift, 1) if shift else strips[s]
                        value = jnp.where(quarter == s, moved, value)
                    at = p * cells_y + part * 8
                    other[at // rows_m, pl.ds(at % rows_m, 8)] = value

    @pl.when(me_y == 0)
    def _():
        spot = n_recv.at[pl.ds(0, ranks_y - 1)]
        pltpu.make_async_remote_copy(
            src_ref=spot, dst_ref=spot, send_sem=send_sem.at[8], recv_sem=s_sem.at[2],
            device_id={"py": 1}, device_id_type=MESH,
        ).wait_recv()
        n_recv[0] = n_send[...]
        pl.when(me_x != 0)(lambda: strips_copy(me_x).start())

    steps = {"y": y_ahead, "x": x_both, "b": y_back}

    def run(order):
        for step in order:
            if step == "T":
                spectrum_tables()
            else:
                steps[step[0]](int(step[1:]) // members, int(step[1:]) % members)

    run(ORDER)

    tall = cells // 4 // ranks_y
    def z_back(chunk, f):
        pieces = [[] for _ in range(ranks_y)]
        for row in range(0, cells_y, 8):
            rows = pl.ds(row, 8)
            arrays = [b_recv[chunk, f, group, rows] for group in range(ranks_y)]
            if chunk == 0:
                pair = [b_recv[0, 0, 0, rows], b_recv[0, 1, 0, rows]]
                arrays[0] = swap_slot(*pair, slots)[f]
            moved = exchange(arrays, width)
            for x in range(ranks_y):
                pieces[x].append(moved[x])
        high, low = halves(jnp.concatenate([piece for some in pieces for piece in some], 0))
        fields = mm(jnp.concatenate([high, low], 1), back_hi[chunk]) + mm(high, back_lo[chunk])
        if chunk > 0:
            fields = fields + partial[f]
        if chunk + 1 < chunks:
            partial[f] = fields
            return
        values = jnp.exp(0.5 * fields)
        for side in range(sides):
            lanes = slice(side * length_z, (side + 1) * length_z)
            cut = values[:, lanes].reshape(ranks_y, cells_y, length_z)
            modulus[f, pl.ds(side * ranks_y, ranks_y)] = cut
        paired = values.reshape(ranks_y // 2, 2, cells_y, sides * length_z)
        paired = (paired[:, 0] + paired[:, 1]).reshape(-1, sides * length_z)
        high, low = halves(paired)
        pooled = mm(pool_rows[...], high) + mm(pool_rows[...], low)
        pooled = [pooled[:, side * length_z : (side + 1) * length_z] for side in range(sides)]
        high, low = halves(jnp.concatenate(pooled, 0))
        coarse = mm(high, pool_columns[...]) + mm(low, pool_columns[...])
        per_side = ranks_y // sides
        height = coarse.shape[0] // sides
        for d in range(ranks_y):
            base = d // per_side * height
            at = base + d % per_side * tall
            c_send[f][d, pl.ds(0, tall)] = coarse[at : at + tall, :LANES]
            at = base + per_side * tall + d % per_side * 8
            value = coarse[at : at + 8, LANES:]
            value = jnp.where(lane < LANES // 2, value, pltpu.roll(value, 4, 0))
            c_send[f][d, pl.ds(tall, 4)] = value[:4]
        c_routes[f].start((), None)

    def pick(f):
        c_routes[f].arrive((), None)
        for g in range(ranks_y):
            d_send[f][g, pl.ds(0, tall)] = c_recv[f][group_table[0, g], pl.ds(0, tall)]
            second = c_recv[f][group_table[1, g], pl.ds(tall, 4)]
            third = c_recv[f][group_table[2, g], pl.ds(tall, 4)]
            d_send[f][g, pl.ds(tall, 4)] = jnp.where(lane[:4] < LANES // 2, second, third)
        d_routes[f].start((), None)

    for chunk in range(chunks):
        for f in range(members):
            b_route.arrive((chunk, f), chunk * members + f)
            if chunk > 0:
                z_back(chunk, f)
        if chunk == 0:
            for f in range(members):
                z_back(chunk, f)
    for f in range(members):
        pick(f)
    for f in range(members):
        d_routes[f].arrive((), None)

    every = pl.ds(0, chunks)
    z_route.drain((every, pl.ds(0, members)))

    @pl.when(taker)
    def _():
        pltpu.make_async_remote_copy(
            src_ref=h_recv, dst_ref=h_recv, send_sem=send_sem.at[11], recv_sem=h_sem.at[0],
            device_id={"py": others[0]}, device_id_type=MESH,
        ).wait_send()
        pltpu.make_async_remote_copy(
            src_ref=g_recv, dst_ref=g_recv, send_sem=send_sem.at[7], recv_sem=g_sem.at[0],
            device_id={"py": others[0]}, device_id_type=MESH,
        ).wait_send()

    x_route.drain((every, pl.ds(0, members)))
    w_route.drain((every, pl.ds(0, members)))
    b_route.drain((every, pl.ds(0, members)))
    spot = s_send.at[pl.ds(0, half_y - 1)]
    pltpu.make_async_remote_copy(
        src_ref=spot, dst_ref=spot, send_sem=send_sem.at[4], recv_sem=s_sem.at[0],
        device_id={"py": others[0]}, device_id_type=MESH,
    ).wait_send()

    @pl.when(my_place == 0)
    def _():
        spot = s_send.at[pl.ds(0, half_y), 1, :, pl.ds(0, 8)]
        pltpu.make_async_remote_copy(
            src_ref=spot, dst_ref=spot, send_sem=send_sem.at[10], recv_sem=s_sem.at[4],
            device_id={"py": others[0]}, device_id_type=MESH,
        ).wait_send()

    t_route.drain(())
    for some in c_routes + d_routes:
        some.drain(())
    pl.when(me_y != 0)(lambda: strip_copy().wait_send())
    pl.when((me_y == 0) & (me_x != 0))(lambda: strips_copy(me_x).wait_send())


def leaving_kernel(modulus, first, second, *refs):
    modulus_out, one_out, two_out, three_out, level_two, level_three, sems = refs
    members, cells_x, cells_y, length_z = modulus.shape
    ranks_y, tall = first.shape[0], first.shape[1] - 4
    copies = []
    for f, coarse in enumerate((first, second)):
        copies.append((modulus.at[f], modulus_out.at[f]))
        copies.append((coarse.at[:, pl.ds(0, tall)], one_out.at[f]))
    copies = [
        pltpu.make_async_copy(source, target, sems.at[index])
        for index, (source, target) in enumerate(copies)
    ]
    for copy in copies:
        copy.start()
    wide, narrow = level_two.shape[3], level_three.shape[3]
    for f, coarse in enumerate((first, second)):
        for d in range(ranks_y):
            low = coarse[d, pl.ds(tall, 4)]
            level_two[f, d // 2, pl.ds(d % 2 * 4, 4)] = low[:, :wide]
            low = pltpu.roll(low, LANES // 2, 1)
            level_three[f, d // 4, pl.ds(d % 4, 1)] = low[:1, :narrow]
    for level, out in ((level_two, two_out), (level_three, three_out)):
        copies.append(pltpu.make_async_copy(level, out, sems.at[len(copies)]))
        copies[-1].start()
    for copy in copies:
        copy.wait()


def lanes_path(white_noise, spectrum, group_table):
    members, cells_x, cells_y, length_z = white_noise.shape
    size_px, size_py = lax.axis_size("px"), lax.axis_size("py")
    length_x, length_y = cells_x * size_px, cells_y * size_py
    slots, width = size_px, 2 * size_px
    tiles = length_z // LANES
    per_tile = cells_x // size_py
    chunks = tiles * per_tile
    blocks = slots // members
    rows_m = length_y // blocks

    column = np.arange(length_z)
    tile, lane = column // LANES, column % LANES
    part = (lane // slots) % 2
    group = lane // width
    rank_q, rank_p, inner = lane % slots, group % size_py, group // size_py
    k = ((tile * size_py + rank_p) * slots + rank_q) * per_tile + inner
    angles = angles_of(length_z)
    sign = np.where(np.arange(length_z) % 2 == 0, 1.0, -1.0)
    z_ahead = np.where(part == 0, np.cos(angles[:, k]), -np.sin(angles[:, k]))
    z_back = 2.0 * z_ahead
    first = (k == 0) & (part == 0)
    second = (k == 0) & (part == 1)
    z_ahead[:, second] = sign[:, None]
    z_back[:, first] = 1.0
    z_back[:, second] = sign[:, None]
    z_back = z_back.T / (length_x * length_y * length_z)

    sides = cells_x // size_py
    half_cells = cells_x * cells_y // sides
    back_hi, back_lo = host_halves(z_back.reshape(chunks, LANES // sides, length_z))

    angles = angles_of(length_y)
    y_table = np.concatenate([np.cos(angles), np.sin(angles)], 0)

    lane = np.arange(LANES)
    cell = (lane // slots % 2, lane % slots * cells_x + lane // width)
    mode = (lane % 2, lane // 2 % slots * cells_x + lane // width)

    def x_table(direction, rows, columns):
        table = complex_array(length_x, direction)[rows][:, columns[0], columns[1]]
        high, low = host_halves(table)
        return jnp.concatenate(
            [
                jnp.concatenate([high, low], 1),
                jnp.concatenate([high, jnp.zeros_like(low)], 1),
            ],
            0,
        )

    at = np.arange(1, LANES)
    mirror_z = np.zeros((LANES, LANES))
    mirror_z[LANES - at, at] = 1.0
    at = np.arange(1, rows_m)
    mirror_y = np.zeros((rows_m, rows_m))
    mirror_y[at, rows_m - at] = 1.0
    same = (mode[1][:, None] + mode[1][None]) % length_x == 0
    mirror_x = np.where(same & (mode[0][:, None] == mode[0][None]), 1.0, 0.0)

    def pool(extent_x, extent_y, factor):
        short_x, short_y = 2 * extent_x // factor, extent_y // factor
        row, cell = np.arange(short_x * short_y), np.arange(extent_x * extent_y)
        same_x = cell[None] // extent_y // (factor // 2) == row[:, None] // short_y
        same_y = cell[None] % extent_y // factor == row[:, None] % short_y
        return np.where(same_x & same_y, 1.0 / factor**3, 0.0)

    per_side = size_py // sides
    some = size_py // 2, cells_y
    lower = np.zeros((per_side, 8, half_cells // 2))
    lower[:, :4] = pool(*some, 4).reshape(per_side, 4, -1)
    lower[:, 4:5] = pool(*some, 8).reshape(per_side, 1, -1)
    pool_rows = np.concatenate([pool(*some, 2), lower.reshape(8 * per_side, -1)], 0)
    pool_columns = np.zeros((length_z, 2 * LANES))
    z = np.arange(length_z)
    pool_columns[z, z // 2] = 1.0
    pool_columns[z, LANES + z // 4] = 1.0
    pool_columns[z, LANES + length_z // 4 + z // 8] = 1.0

    ahead = [
        jnp.concatenate(host_halves(z_ahead[:, at : at + LANES]), 1)
        for at in range(0, length_z, LANES)
    ]
    held_in = [
        white_noise,
        jnp.stack(ahead),
        spectrum,
        jnp.asarray(np.tile(mirror_z, (2, 1)), BF16),
        jnp.asarray(np.tile(mirror_x, (2, 1)), BF16),
        jnp.asarray(np.tile(mirror_y, (1, 2)), BF16),
        *host_halves(y_table),
        x_table(-1.0, cell, mode),
        x_table(1.0, mode, cell),
        back_hi,
        back_lo,
        jnp.asarray(pool_rows, BF16),
        jnp.asarray(pool_columns, BF16),
        group_table,
    ]
    sizes = (cells_x, cells_y, length_z, slots, size_py)

    def body(*refs):
        whole_kernel(sizes, len(held_in), *refs)

    def vmem(*shape):
        return pltpu.VMEM(shape, F32)

    x_shape = (chunks, members, slots, length_y // slots, LANES)
    b_shape = (chunks, members, size_py, cells_y, LANES)
    s_shape = (2, tiles, cells_y, LANES)
    t_shape = (slots, rows_m, LANES)
    tall = cells_x * cells_y // 4 // size_py
    c_shapes = [(size_py, tall + 4, LANES)] * members
    sem = pltpu.SemaphoreType.DMA
    scratch = [pltpu.VMEM(value.shape, value.dtype) for value in held_in[:-1]]
    scratch.append(pltpu.SMEM(group_table.shape, group_table.dtype))
    for shape in (b_shape, x_shape, x_shape, b_shape):
        scratch += [vmem(*shape), vmem(*shape)]
    scratch += [vmem(size_py, *s_shape), vmem(size_py // 2, *s_shape), vmem(tiles, 8, LANES)]
    scratch += [vmem(*t_shape), vmem(*t_shape)]
    scratch += [vmem(8, LANES), vmem(size_py, 8, LANES), vmem(slots, size_py, 8, LANES)]
    scratch += [
        vmem(chunks, blocks, rows_m, LANES),
        vmem(blocks, rows_m, LANES),
        vmem(members, cells_x * cells_y, length_z),
        vmem(cells_x * cells_y, LANES),
        vmem(members, half_cells, sides * length_z),
        pltpu.VMEM((chunks, 2 * LANES, sides * length_z), BF16),
        pltpu.VMEM((chunks, LANES, sides * length_z), BF16),
        vmem(chunks, members, size_py // 2, cells_y, LANES),
        vmem(members, size_py // 2, cells_y, LANES),
        *[vmem(*shape) for shape in c_shapes * 3],
    ]
    scratch += [
        sem((len(held_in) + 1,)), sem((16,)), sem((chunks * members,)), sem((chunks * members,)),
        sem((chunks * members,)), sem((chunks * members,)), sem((members,)), sem((members,)), sem((5,)), sem((chunks * members,)), sem((members,)),
    ]
    hbm = pl.BlockSpec(memory_space=pltpu.HBM)
    local = pl.BlockSpec(memory_space=pltpu.VMEM)
    leaving = pl.pallas_call(
        body,
        out_shape=[jax.ShapeDtypeStruct(shape, F32) for shape in [white_noise.shape] + c_shapes],
        in_specs=[hbm] * len(held_in),
        out_specs=[local] * 3,
        scratch_shapes=scratch,
        compiler_params=pltpu.CompilerParams(
            collective_id=0, has_side_effects=True, vmem_limit_bytes=40 * 1024 * 1024
        ),
    )(*[pltpu.with_memory_space_constraint(v, pltpu.HBM) for v in held_in])
    outs = [white_noise.shape]
    for level in range(1, 4):
        outs.append((members,) + tuple(extent >> level for extent in white_noise.shape[1:]))
    return tuple(
        pl.pallas_call(
            leaving_kernel,
            out_shape=[jax.ShapeDtypeStruct(shape, F32) for shape in outs],
            in_specs=[local] * 3,
            out_specs=[hbm] * 4,
            scratch_shapes=[vmem(*outs[2]), vmem(*outs[3]), sem((2 * members + 2,))],
            compiler_params=pltpu.CompilerParams(vmem_limit_bytes=4 * 1024 * 1024),
        )(*leaving)
    )


def on_device(white_noise, spectrum, group_table):
    members, cells_x, cells_y, length_z = white_noise.shape
    size_px, size_py = lax.axis_size("px"), lax.axis_size("py")
    fits = members == 2 and length_z == 2 * LANES and size_px == 4 and size_py == 8
    fits = fits and 2 * cells_x * size_px == LANES and cells_x == 2 * size_py
    fits = fits and cells_y == 2 * cells_x
    chosen = lanes_path if fits else general_path
    return chosen(white_noise, spectrum, group_table)


def solution(mesh):
    in_specs = (P(None, "px", "py", None), P("px", "py", None), P())
    out_specs = (P(None, "px", "py", None),) * 4
    return jax.shard_map(
        on_device, mesh=mesh, in_specs=in_specs, out_specs=out_specs, check_vma=False
    )
```

```python
import numpy as np

import jax
import jax.numpy as jnp
from jax import lax
from jax.experimental import pallas as pl
from jax.experimental.pallas import tpu as pltpu
from jax.sharding import PartitionSpec as P


def angles_of(length):
    positions = np.arange(length, dtype=np.int64)
    return (positions[:, None] * positions[None, :] % length) * (2.0 * np.pi / length)


def complex_array(length, direction):
    angles = angles_of(length)
    cos, sin = np.cos(angles), direction * np.sin(angles)
    return np.stack([np.stack([cos, sin], 1), np.stack([-sin, cos], 1)], 0)


def complex_table(length, direction):
    return jnp.asarray(complex_array(length, direction), jnp.float32)


def half_tables(length):
    angles = angles_of(length)[:, : length // 2]
    ahead = np.stack([np.cos(angles), -np.sin(angles)], 1)
    back = 2.0 * ahead
    nyquist = np.where(np.arange(length) % 2 == 0, 1.0, -1.0)
    ahead[:, 1, 0] = nyquist
    back[:, 0, 0] = 1.0
    back[:, 1, 0] = nyquist
    return jnp.asarray(ahead, jnp.float32), jnp.asarray(back, jnp.float32)


def einsum(pattern, left, right):
    return jnp.einsum(pattern, left, right, precision=lax.Precision.HIGH)


def swap_first(values):
    first = values[:, :, :1]
    turned = jnp.swapaxes(first, 0, 1)
    return jnp.concatenate([turned, values[:, :, 1:]], 2)


def coarsen(values):
    members, size_x, size_y, size_z = values.shape
    blocks = values.reshape(members, size_x // 2, 2, size_y // 2, 2, size_z // 2, 2)
    return blocks.mean(axis=(2, 4, 6))


def general_path(white_noise, spectrum, group_table):
    members, cells_x, cells_y, length_z = white_noise.shape
    size_px, size_py = lax.axis_size("px"), lax.axis_size("py")
    length_x, length_y = cells_x * size_px, cells_y * size_py
    half_z = length_z // 2
    block_py, block = half_z // size_py, half_z // size_py // size_px
    z_ahead, z_back = half_tables(length_z)
    scale = 1.0 / (length_x * length_y * length_z)

    table = jnp.transpose(spectrum, (2, 0, 1))
    last = jnp.broadcast_to(table[half_z : half_z + 1], (size_py, 1, cells_x, cells_y))
    table = jnp.concatenate([table[:half_z].reshape(size_py, block_py, cells_x, cells_y), last], 1)
    table = lax.all_to_all(table, "py", split_axis=0, concat_axis=3, tiled=True)[0]
    last = jnp.broadcast_to(table[block_py:], (size_px, 1, cells_x, length_y))
    table = jnp.concatenate([table[:block_py].reshape(size_px, block, cells_x, length_y), last], 1)
    table = lax.all_to_all(table, "px", split_axis=0, concat_axis=2, tiled=True)[0] * scale
    is_first = (lax.axis_index("px") == 0) & (lax.axis_index("py") == 0)
    other = jnp.where(is_first, table[block:], table[:1])
    tables = jnp.stack([table[:block], jnp.concatenate([other, table[1:block]], 0)], 0)

    values = einsum("fxyz,zck->fckxy", white_noise, z_ahead)
    values = swap_first(values)
    values = lax.all_to_all(values, "py", split_axis=2, concat_axis=4, tiled=True)
    values = einsum("fckxy,cydm->fdkxm", values, complex_table(length_y, -1.0))
    values = lax.all_to_all(values, "px", split_axis=2, concat_axis=3, tiled=True)
    values = einsum("fckxm,cxdj->fdkjm", values, complex_table(length_x, -1.0))
    values = values * tables[:, None]
    values = einsum("fckjm,cjdx->fdkxm", values, complex_table(length_x, 1.0))
    values = lax.all_to_all(values, "px", split_axis=3, concat_axis=2, tiled=True)
    values = einsum("fckxm,cmdy->fdkxy", values, complex_table(length_y, 1.0))
    values = lax.all_to_all(values, "py", split_axis=4, concat_axis=2, tiled=True)
    values = swap_first(values)
    fields = einsum("fckxy,zck->fxyz", values, z_back)
    modulus = jnp.exp(0.5 * fields)

    levels = []
    level = modulus
    for _ in range(3):
        level = coarsen(level)
        levels.append(level)
    pieces = [jnp.reshape(level, (size_py, -1)) for level in levels]
    widths = [piece.shape[1] for piece in pieces]
    joined = jnp.concatenate(pieces, 1)
    spread = lax.all_to_all(joined, "py", split_axis=0, concat_axis=0, tiled=True)
    picked, start = [], 0
    for index, width in enumerate(widths):
        part = spread[:, start : start + width]
        picked.append(jnp.take(part, group_table[index], axis=0))
        start += width
    joined = lax.all_to_all(
        jnp.concatenate(picked, 1), "py", split_axis=0, concat_axis=0, tiled=True
    )
    routed, start = [], 0
    for level, width in zip(levels, widths):
        routed.append(joined[:, start : start + width].reshape(level.shape))
        start += width
    return (modulus, routed[0], routed[1], routed[2])


LANES = 128
ORDER = (
    "y0", "y1", "T", "y2", "x0", "y3", "x1", "y4", "x2", "b0", "x3", "y5", "b1",
    "y6", "x4", "b2", "y7", "b3", "x5", "x6", "b4", "x7", "b5", "b6", "b7",
)
MESH = pl.DeviceIdType.MESH
BF16 = jnp.bfloat16
F32 = jnp.float32


def halves(values):
    high = values.astype(BF16)
    low = (values - high.astype(F32)).astype(BF16)
    return high, low


def host_halves(values):
    values = np.asarray(values, np.float64)
    high = values.astype(np.float32).astype(BF16)
    low = (values - high.astype(np.float64)).astype(np.float32).astype(BF16)
    return jnp.asarray(high), jnp.asarray(low)


def mm(left, right):
    return jnp.dot(left, right, preferred_element_type=F32)


def lane_of(shape):
    return lax.broadcasted_iota(jnp.int32, shape, len(shape) - 1)


def exchange(arrays, width):
    count = len(arrays)
    field = (lane_of(arrays[0].shape) // width) % count
    skewed = [pltpu.roll(a, i * width, 1) if i else a for i, a in enumerate(arrays)]
    moved = [skewed[-index % count] for index in range(count)]
    distance = 1
    while distance < count:
        take = (field // distance) % 2 == 1
        moved = [
            jnp.where(take, moved[(index - distance) % count], moved[index])
            for index in range(count)
        ]
        distance *= 2
    return [pltpu.roll(m, LANES - i * width, 1) if i else m for i, m in enumerate(moved)]


def turned(values, slots, ahead):
    real = (lane_of(values.shape) // slots) % 2 == 0
    from_imag = pltpu.roll(values, LANES - slots, 1)
    from_real = pltpu.roll(values, slots, 1)
    if ahead:
        return jnp.where(real, from_imag, -from_real)
    return jnp.where(real, -from_imag, from_real)


def swap_slot(first, second, slots):
    place = lane_of(first.shape) % (2 * slots)
    return (
        jnp.where(place == slots, pltpu.roll(second, slots, 1), first),
        jnp.where(place == 0, pltpu.roll(first, LANES - slots, 1), second),
    )


class Route:
    def __init__(self, axis, count, away, source, target, send, recv):
        self.axis, self.count, self.away = axis, count, away
        self.source, self.target = source, target
        self.send, self.recv = send, recv
        self.me = lax.axis_index(axis)

    def copy(self, source, target, peer, part):
        return pltpu.make_async_remote_copy(
            src_ref=source,
            dst_ref=target,
            send_sem=self.send,
            recv_sem=self.recv.at[part] if part is not None else self.recv,
            device_id={self.axis: peer},
            device_id_type=MESH,
        )

    def at(self, ref, where, index):
        return ref.at[where + (index,)]

    def start(self, where, part):
        for peer in self.away:
            source = self.at(self.source, where, peer)
            target = self.at(self.target, where, self.me)
            self.copy(source, target, peer, part).start()

    def arrive(self, where, part):
        spot = self.at(self.target, where, pl.ds(0, self.count - 1))
        self.copy(spot, spot, self.away[0], part).wait_recv()
        self.target[where + (self.me,)] = self.source[where + (self.me,)]

    def drain(self, where):
        spot = self.source.at[where + (pl.ds(0, self.count - 1),)]
        self.copy(spot, spot, self.away[0], 0 if len(self.recv.shape) else None).wait_send()


def whole_kernel(sizes, loads, *refs):
    cells_x, cells_y, length_z, slots, ranks_y = sizes
    members = 2
    width = 2 * slots
    per_tile = cells_x // ranks_y
    tiles = length_z // LANES
    chunks = tiles * per_tile
    length_y = cells_y * ranks_y
    blocks = slots // members
    rows_m = length_y // blocks
    rows_part = length_y // slots
    sources, held_in = refs[:loads], refs[3 + loads : 3 + 2 * loads]
    modulus, d_recv_0, d_recv_1 = refs[loads : 3 + loads]
    (
        z_send, z_recv, x_send, x_recv, w_send, w_recv, b_send, b_recv,
        s_send, s_recv, e_recv, t_send, t_recv, n_send, n_recv, m_recv,
        tables, other, held, image, partial, h_recv, g_recv, c_send_0, c_send_1, c_recv_0, c_recv_1,
        d_send_0, d_send_1,
        load_sem, send_sem, z_sem, x_sem, w_sem, b_sem, c_sem, d_sem, s_sem, h_sem, g_sem,
    ) = refs[3 + 2 * loads :]
    (
        noise, ahead, spectrum, mirror_z, mirror_x, mirror_y, y_hi, y_lo, x_ahead, x_back,
        back, pool_rows, pool_columns, group_table,
    ) = held_in

    me_x, me_y = lax.axis_index("px"), lax.axis_index("py")
    pairs = [(sources[0].at[f], noise.at[f]) for f in range(members)]
    pairs = [pairs[0], (sources[1], ahead), *pairs[1:], *list(zip(sources, held_in))[2:]]
    copies = [
        pltpu.make_async_copy(source, target, load_sem.at[index])
        for index, (source, target) in enumerate(pairs)
    ]
    place, core = me_y // 2, me_y % 2
    chips = ranks_y // 2
    near = chips - 1 - (chips - 2) * (place % 2)
    inner = (place + 1) // 2 % 2
    far = near - (near - chips // 2) * inner
    steps = [far, near + chips // 2 - far, chips - near]
    away_y = []
    for step in steps:
        for side in (0, 1):
            away_y.append((place + step) % chips * 2 + (core + side) % 2)
    away_y.append(place * 2 + 1 - core)
    away_x = [slots - 1 - me_x, (me_x + 2) % slots, me_x + 1 - 2 * (me_x % 2)]

    barrier = pltpu.get_barrier_semaphore()
    for peer in away_y:
        pl.semaphore_signal(barrier, inc=1, device_id={"py": peer}, device_id_type=MESH)
    for peer in away_x:
        pl.semaphore_signal(barrier, inc=1, device_id={"px": peer}, device_id_type=MESH)

    early = 5
    for copy in copies[:early]:
        copy.start()

    def route(axis, source, target, send, recv):
        away, count = (away_y, ranks_y) if axis == "py" else (away_x, slots)
        return Route(axis, count, away, source, target, send_sem.at[send], recv)

    z_route = route("py", z_send, z_recv, 0, z_sem)
    x_route = route("px", x_send, x_recv, 1, x_sem)
    w_route = route("px", w_send, w_recv, 2, w_sem)
    b_route = route("py", b_send, b_recv, 3, b_sem)
    t_route = route("px", t_send, t_recv, 5, s_sem.at[1])
    c_send, c_recv = (c_send_0, c_send_1), (c_recv_0, c_recv_1)
    d_send, d_recv = (d_send_0, d_send_1), (d_recv_0, d_recv_1)
    c_routes = [route("py", c_send[f], c_recv[f], 12 + f, c_sem.at[f]) for f in range(members)]
    d_routes = [route("py", d_send[f], d_recv[f], 14 + f, d_sem.at[f]) for f in range(members)]

    lane = lane_of((8, LANES))
    quarter = (lane // 2) % slots
    half_y = ranks_y // 2
    my_half, my_place = me_y // half_y, me_y % half_y

    def strip_copy():
        return pltpu.make_async_remote_copy(
            src_ref=n_send, dst_ref=n_recv.at[me_y], send_sem=send_sem.at[8],
            recv_sem=s_sem.at[2], device_id={"py": 0}, device_id_type=MESH,
        )

    def half_copy(peer):
        return pltpu.make_async_remote_copy(
            src_ref=s_send.at[peer], dst_ref=s_recv.at[my_place], send_sem=send_sem.at[4],
            recv_sem=s_sem.at[0], device_id={"py": peer}, device_id_type=MESH,
        )

    def edge_copy(peer):
        return pltpu.make_async_remote_copy(
            src_ref=s_send.at[peer, 1, :, pl.ds(0, 1)], dst_ref=e_recv, send_sem=send_sem.at[10],
            recv_sem=s_sem.at[4], device_id={"py": peer}, device_id_type=MESH,
        )

    others = [my_half * half_y + (my_place + step) % half_y for step in range(1, half_y)]
    places = [(step + half_y // 2 * (1 - my_half)) % half_y for step in range(half_y)]
    across = [(1 - my_half) * half_y + spot for spot in places]

    def send_spectrum():
        pl.when(me_y != 0)(lambda: strip_copy().start())
        for peer in others[1:] + others[:1]:
            half_copy(peer).start()

        @pl.when(my_place == 0)
        def _():
            for peer in across:
                edge_copy(peer).start()

    middle = (place == chips // 2) | (place == chips // 2 - 1)
    giver, taker = middle & (core == 0), middle & (core == 1)

    def shared_start(route, where, part, hand, hand_sem, extra):
        source, target = route.source, route.target
        blocks_away = source.at[where + (pl.ds((1 - my_half) * half_y, half_y),)]

        def hand_copy():
            return pltpu.make_async_remote_copy(
                src_ref=blocks_away, dst_ref=hand, send_sem=route.send, recv_sem=hand_sem,
                device_id={"py": place * 2 + 1 - core}, device_id_type=MESH,
            )

        @pl.when(giver)
        def _():
            hand_copy().start()
            for peer in others:
                spot = source.at[where + (peer,)]
                route.copy(spot, target.at[where + (me_y,)], peer, part).start()

        @pl.when(jnp.logical_not(giver))
        def _():
            route.start(where, part)

        @pl.when(taker)
        def _():
            hand_copy().wait_recv()
            for spot, peer in zip(places, across):
                pltpu.make_async_remote_copy(
                    src_ref=hand.at[spot], dst_ref=target.at[where + (me_y - 1,)],
                    send_sem=send_sem.at[extra], recv_sem=route.recv.at[part],
                    device_id={"py": peer}, device_id_type=MESH,
                ).start()

    def z_start(chunk, f):
        part = chunk * members + f
        shared_start(z_route, (chunk, f), part, h_recv.at[chunk, f], h_sem.at[part], 11)

    def own_spectrum():
        mirrored = jnp.concatenate(
            halves(spectrum[:, :, LANES : 2 * LANES].reshape(cells_x * cells_y, LANES)), 1
        )
        image[...] = mm(mirrored, mirror_z[...])
        for row in range(0, cells_y, 8):
            rows = pl.ds(row, 8)
            plain = [spectrum[x, rows, pl.ds(0, LANES)] for x in range(cells_x)]
            turned_z = []
            for x in range(cells_x):
                value = image[pl.ds(x * cells_y + row, 8)]
                turned_z.append(jnp.where(lane == 0, plain[x], value))
            for kind, arrays in enumerate((plain, turned_z)):
                moved = exchange(arrays, width)
                for group in range(cells_x):
                    s_send[group % ranks_y, kind, group // ranks_y, rows] = moved[group]
        strip = jnp.zeros((8, LANES), F32)
        for x in range(cells_x):
            for part in range(cells_y // 8):
                value = spectrum[x, pl.ds(part * 8, 8), pl.ds(LANES, 1)]
                strip = jnp.where((lane // width == x) & (quarter == part), value, strip)
        n_send[...] = strip

    cells = cells_x * cells_y
    lined = []
    for tile in range(tiles):
        for f in range(members):
            if tile == 0:
                for copy in copies[2 * f : 2 + f]:
                    copy.wait()
                lined.append(halves(noise[f].reshape(cells, length_z)))
            high, low = lined[f]
            both = mm(high, ahead[tile])
            both = both[:, :LANES] + both[:, LANES:] + mm(low, ahead[tile, :, pl.ds(0, LANES)])
            held[f, :, pl.ds(tile * LANES, LANES)] = both
        lanes = pl.ds(tile * LANES, LANES)
        for row in range(0, cells_y, 8):
            rows = pl.ds(row, 8)
            both = []
            for f in range(members):
                both.append(
                    exchange(
                        [held[f, pl.ds(x * cells_y + row, 8), lanes] for x in range(cells_x)],
                        width,
                    )
                )
            if tile == 0:
                both[0][0], both[1][0] = swap_slot(both[0][0], both[1][0], slots)
            for f in range(members):
                for group in range(cells_x):
                    chunk = tile * per_tile + group // ranks_y
                    z_send[chunk, f, group % ranks_y, rows] = both[f][group]
        if tile == 0:
            pl.semaphore_wait(barrier, ranks_y + slots - 2)
        for part in range(tile * per_tile * members, (tile + 1) * per_tile * members):
            z_start(part // members, part % members)
            if part == 0:
                for copy in copies[3:early]:
                    copy.wait()
                for copy in copies[early:]:
                    copy.start()
                own_spectrum()
                send_spectrum()

    for copy in copies[early:]:
        copy.wait()
    sides = cells_x // ranks_y

    spot = s_recv.at[pl.ds(0, half_y - 1)]
    pltpu.make_async_remote_copy(
        src_ref=spot, dst_ref=spot, send_sem=send_sem.at[4], recv_sem=s_sem.at[0],
        device_id={"py": others[0]}, device_id_type=MESH,
    ).wait_recv()
    edge_copy(others[0]).wait_recv()
    s_recv[my_place] = s_send[me_y]
    pair = [s_recv[:, 1, tile].reshape(rows_m, LANES) for tile in range(tiles)]
    pair = jnp.concatenate(halves(jnp.concatenate(pair, 1)), 0)
    held[1, pl.ds(0, rows_m)] = mm(mirror_y[...], pair)
    sublane = lax.broadcasted_iota(jnp.int32, (8, LANES), 0)
    for row in range(0, rows_m, 8):
        arrays = []
        for tile in range(tiles):
            arrays.append(s_recv[row // cells_y, 0, tile, pl.ds(row % cells_y, 8)])
            value = held[1, pl.ds(row, 8), pl.ds(tile * LANES, LANES)]
            if row == 0:
                value = jnp.where(sublane == 0, e_recv[tile], value)
            arrays.append(value)
        moved = exchange(arrays, 2)
        for rank in range(slots):
            t_send[rank, pl.ds(row, 8)] = moved[rank]
    t_route.start((), None)

    def strips_copy(source):
        return pltpu.make_async_remote_copy(
            src_ref=n_recv, dst_ref=m_recv.at[source], send_sem=send_sem.at[9],
            recv_sem=s_sem.at[3], device_id={"px": 0}, device_id_type=MESH,
        )

    def along_y(columns):
        high, low = halves(columns)
        both = mm(y_hi[...], jnp.concatenate([high, low], 1))
        return both[:, :LANES] + both[:, LANES:] + mm(y_lo[...], high)

    def combined(product, start, rows, ahead):
        by_cos = product[start : start + rows]
        by_sin = product[length_y + start : length_y + start + rows]
        return by_cos + turned(by_sin, slots, ahead)

    def y_ahead(chunk, f):
        part = chunk * members + f
        z_route.arrive((chunk, f), part)
        product = along_y(z_recv[chunk, f].reshape(length_y, LANES))
        for row in range(0, rows_part, 16):
            arrays = [combined(product, a * rows_part + row, 16, True) for a in range(slots)]
            moved = exchange(arrays, 1)
            for rank in range(slots):
                x_send[chunk, f, rank, pl.ds(row, 16)] = moved[rank]
        x_route.start((chunk, f), part)

    def gathered(ref, chunk, f):
        pieces = [[] for _ in range(slots)]
        for row in range(0, rows_part, 16):
            moved = exchange([ref[chunk, f, s, pl.ds(row, 16)] for s in range(slots)], 1)
            for index in range(slots):
                pieces[index].append(moved[index])
        return jnp.concatenate([piece for some in pieces for piece in some], 0)

    def along_x(values, table):
        product = mm(jnp.concatenate(halves(values), 1), table[...])
        return product[:, :LANES] + product[:, LANES:]

    def x_both(chunk, f):
        part = chunk * members + f
        x_route.arrive((chunk, f), part)
        table = other if part == 1 else tables.at[chunk]
        values = along_x(gathered(x_recv, chunk, f), x_ahead)
        values = along_x(values * table[...].reshape(length_y, LANES), x_back)
        for row in range(0, rows_part, 16):
            arrays = [values[a * rows_part + row : a * rows_part + row + 16] for a in range(slots)]
            moved = exchange(arrays, 1)
            for s in range(slots):
                w_send[chunk, f, s, pl.ds(row, 16)] = moved[s]
        w_route.start((chunk, f), part)

    def y_back(chunk, f):
        part = chunk * members + f
        w_route.arrive((chunk, f), part)
        product = along_y(gathered(w_recv, chunk, f))
        for p in range(ranks_y):
            b_send[chunk, f, p] = combined(product, p * cells_y, cells_y, False)
        late = part - (chunks * members - g_recv.shape[0])
        if late >= 0:
            shared_start(b_route, (chunk, f), part, g_recv.at[late], g_sem.at[late], 7)
        else:
            b_route.start((chunk, f), part)

    def table_rows(tile, block, rows, part):
        even = lane % 2 == 0
        first = jnp.where(even, part, pltpu.roll(part, 1, 1))
        second = jnp.where(even, pltpu.roll(part, LANES - 1, 1), part)
        tables[tile * per_tile, block, rows] = first
        tables[tile * per_tile + 1, block, rows] = second
        if tile == 0:
            other[block, rows] = first

    def spectrum_tables():
        t_route.arrive((), None)
        images = [[] for _ in range(tiles)]
        for row in range(0, rows_m, 8):
            rows = pl.ds(row, 8)
            moved = exchange([t_recv[s, rows] for s in range(slots)], 2)
            for tile in range(tiles):
                table_rows(tile, my_half, rows, moved[2 * tile])
                images[tile].append(moved[2 * tile + 1])
        images = jnp.concatenate([piece for pieces in images for piece in pieces], 0)
        images = mm(jnp.concatenate(halves(images), 1), mirror_x[...])
        for tile in range(tiles):
            for row in range(0, rows_m, 8):
                at = tile * rows_m + row
                table_rows(tile, 1 - my_half, pl.ds(row, 8), images[at : at + 8])

        @pl.when((me_y == 0) & (me_x == 0))
        def _():
            spot = m_recv.at[pl.ds(1, slots - 1)]
            pltpu.make_async_remote_copy(
                src_ref=spot, dst_ref=spot, send_sem=send_sem.at[9], recv_sem=s_sem.at[3],
                device_id={"px": 1}, device_id_type=MESH,
            ).wait_recv()
            for p in range(ranks_y):
                strips = [n_recv[p] if s == 0 else m_recv[s, p] for s in range(slots)]
                for part in range(cells_y // 8):
                    value = strips[part]
                    for s in range(slots):
                        shift = (s - part) * 2 % LANES
                        moved = pltpu.roll(strips[s], shift, 1) if shift else strips[s]
                        value = jnp.where(quarter == s, moved, value)
                    at = p * cells_y + part * 8
                    other[at // rows_m, pl.ds(at % rows_m, 8)] = value

    @pl.when(me_y == 0)
    def _():
        spot = n_recv.at[pl.ds(0, ranks_y - 1)]
        pltpu.make_async_remote_copy(
            src_ref=spot, dst_ref=spot, send_sem=send_sem.at[8], recv_sem=s_sem.at[2],
            device_id={"py": 1}, device_id_type=MESH,
        ).wait_recv()
        n_recv[0] = n_send[...]
        pl.when(me_x != 0)(lambda: strips_copy(me_x).start())

    steps = {"y": y_ahead, "x": x_both, "b": y_back}

    def run(order):
        for step in order:
            if step == "T":
                spectrum_tables()
            else:
                steps[step[0]](int(step[1:]) // members, int(step[1:]) % members)

    run(ORDER)

    tall = cells // 4 // ranks_y
    def z_back(chunk, f):
        pieces = [[] for _ in range(ranks_y)]
        for row in range(0, cells_y, 8):
            rows = pl.ds(row, 8)
            arrays = [b_recv[chunk, f, group, rows] for group in range(ranks_y)]
            if chunk == 0:
                pair = [b_recv[0, 0, 0, rows], b_recv[0, 1, 0, rows]]
                arrays[0] = swap_slot(*pair, slots)[f]
            moved = exchange(arrays, width)
            for x in range(ranks_y):
                pieces[x].append(moved[x])
        cells_by = jnp.concatenate([piece for some in pieces for piece in some], 0)
        swapped = pltpu.roll(cells_by, LANES // 2, 1)
        near_side = lane_of(cells_by.shape) < LANES // 2
        first_side = 0 if chunk + 1 < chunks else 1 - my_half
        if chunk + 1 == chunks:
            flip = first_side == 1
            cells_by, swapped = (
                jnp.where(flip, swapped, cells_by), jnp.where(flip, cells_by, swapped)
            )

        def fields(value, beside, side):
            high = value.astype(BF16)
            low = beside - beside.astype(BF16).astype(F32)
            mixed = jnp.where(near_side, high.astype(F32), low).astype(BF16)
            result = mm(jnp.concatenate([mixed, high], 1), back[chunk])
            return result + partial[f, side] if chunk > 0 else result

        if chunk + 1 < chunks:
            partial[f, 0] = fields(cells_by, swapped, 0)
            partial[f, 1] = fields(swapped, cells_by, 1)
            return
        for side, peers, value, beside in (
            (1 - my_half, across, cells_by, swapped), (my_half, others, swapped, cells_by)
        ):
            values = jnp.exp2(fields(value, beside, side))
            cut = values.reshape(ranks_y, cells_y, length_z)
            modulus[f, pl.ds(side * ranks_y, ranks_y)] = cut
            paired = values.reshape(ranks_y // 2, 2, cells_y, length_z)
            paired = (paired[:, 0] + paired[:, 1]).reshape(-1, length_z)
            high_part, low_part = halves(paired)
            pooled = mm(pool_rows[...], jnp.concatenate([high_part, low_part], 0))
            high_part, low_part = halves(pooled)
            coarse = mm(high_part, pool_columns[...]) + mm(low_part, pool_columns[...])
            for e in range(half_y):
                piece = side * half_y + e
                c_send[f][piece, pl.ds(0, tall)] = coarse[e * tall : (e + 1) * tall, :LANES]
                at = half_y * tall + e * 8
                value = coarse[at : at + 8, LANES:]
                value = jnp.where(lane < LANES // 2, value, pltpu.roll(value, 4, 0))
                c_send[f][piece, pl.ds(tall, 4)] = value[:4]
            for peer in peers:
                spot = c_recv[f].at[me_y]
                c_routes[f].copy(c_send[f].at[peer], spot, peer, None).start()

    def pick(f):
        c_routes[f].arrive((), None)
        for g in range(ranks_y):
            d_send[f][g, pl.ds(0, tall)] = c_recv[f][group_table[0, g], pl.ds(0, tall)]
            second = c_recv[f][group_table[1, g], pl.ds(tall, 4)]
            third = c_recv[f][group_table[2, g], pl.ds(tall, 4)]
            d_send[f][g, pl.ds(tall, 4)] = jnp.where(lane[:4] < LANES // 2, second, third)
        d_routes[f].start((), None)

    for chunk in range(chunks):
        for f in range(members):
            b_route.arrive((chunk, f), chunk * members + f)
            if chunk > 0:
                z_back(chunk, f)
        if chunk == 0:
            for f in range(members):
                z_back(chunk, f)
    for f in range(members):
        pick(f)
    for f in range(members):
        d_routes[f].arrive((), None)

    every = pl.ds(0, chunks)
    z_route.drain((every, pl.ds(0, members)))

    @pl.when(taker)
    def _():
        pltpu.make_async_remote_copy(
            src_ref=h_recv, dst_ref=h_recv, send_sem=send_sem.at[11], recv_sem=h_sem.at[0],
            device_id={"py": others[0]}, device_id_type=MESH,
        ).wait_send()
        pltpu.make_async_remote_copy(
            src_ref=g_recv, dst_ref=g_recv, send_sem=send_sem.at[7], recv_sem=g_sem.at[0],
            device_id={"py": others[0]}, device_id_type=MESH,
        ).wait_send()

    x_route.drain((every, pl.ds(0, members)))
    w_route.drain((every, pl.ds(0, members)))
    b_route.drain((every, pl.ds(0, members)))
    spot = s_send.at[pl.ds(0, half_y - 1)]
    pltpu.make_async_remote_copy(
        src_ref=spot, dst_ref=spot, send_sem=send_sem.at[4], recv_sem=s_sem.at[0],
        device_id={"py": others[0]}, device_id_type=MESH,
    ).wait_send()

    @pl.when(my_place == 0)
    def _():
        spot = s_send.at[pl.ds(0, half_y), 1, :, pl.ds(0, 1)]
        pltpu.make_async_remote_copy(
            src_ref=spot, dst_ref=spot, send_sem=send_sem.at[10], recv_sem=s_sem.at[4],
            device_id={"py": others[0]}, device_id_type=MESH,
        ).wait_send()

    t_route.drain(())
    for some in c_routes + d_routes:
        some.drain(())
    pl.when(me_y != 0)(lambda: strip_copy().wait_send())
    pl.when((me_y == 0) & (me_x != 0))(lambda: strips_copy(me_x).wait_send())


def leaving_kernel(modulus, first, second, *refs):
    modulus_out, one_out, two_out, three_out, level_two, level_three, sems = refs
    members, cells_x, cells_y, length_z = modulus.shape
    ranks_y, tall = first.shape[0], first.shape[1] - 4
    copies = []
    for f, coarse in enumerate((first, second)):
        copies.append((modulus.at[f], modulus_out.at[f]))
        copies.append((coarse.at[:, pl.ds(0, tall)], one_out.at[f]))
    copies = [
        pltpu.make_async_copy(source, target, sems.at[index])
        for index, (source, target) in enumerate(copies)
    ]
    for copy in copies:
        copy.start()
    wide, narrow = level_two.shape[3], level_three.shape[3]
    for f, coarse in enumerate((first, second)):
        for d in range(ranks_y):
            low = coarse[d, pl.ds(tall, 4)]
            level_two[f, d // 2, pl.ds(d % 2 * 4, 4)] = low[:, :wide]
            low = pltpu.roll(low, LANES // 2, 1)
            level_three[f, d // 4, pl.ds(d % 4, 1)] = low[:1, :narrow]
    for level, out in ((level_two, two_out), (level_three, three_out)):
        copies.append(pltpu.make_async_copy(level, out, sems.at[len(copies)]))
        copies[-1].start()
    for copy in copies:
        copy.wait()


def lanes_path(white_noise, spectrum, group_table):
    members, cells_x, cells_y, length_z = white_noise.shape
    size_px, size_py = lax.axis_size("px"), lax.axis_size("py")
    length_x, length_y = cells_x * size_px, cells_y * size_py
    slots, width = size_px, 2 * size_px
    tiles = length_z // LANES
    per_tile = cells_x // size_py
    chunks = tiles * per_tile
    blocks = slots // members
    rows_m = length_y // blocks

    column = np.arange(length_z)
    tile, lane = column // LANES, column % LANES
    part = (lane // slots) % 2
    group = lane // width
    rank_q, rank_p, inner = lane % slots, group % size_py, group // size_py
    k = ((tile * size_py + rank_p) * slots + rank_q) * per_tile + inner
    angles = angles_of(length_z)
    sign = np.where(np.arange(length_z) % 2 == 0, 1.0, -1.0)
    z_ahead = np.where(part == 0, np.cos(angles[:, k]), -np.sin(angles[:, k]))
    z_back = 2.0 * z_ahead
    first = (k == 0) & (part == 0)
    second = (k == 0) & (part == 1)
    z_ahead[:, second] = sign[:, None]
    z_back[:, first] = 1.0
    z_back[:, second] = sign[:, None]
    z_back = z_back.T * (0.5 / np.log(2.0) / (length_x * length_y * length_z))

    sides = cells_x // size_py
    half_cells = cells_x * cells_y // sides
    back_hi, back_lo = host_halves(z_back.reshape(chunks, LANES // sides, length_z))
    back = jnp.concatenate([back_hi, back_hi, back_lo, jnp.zeros_like(back_lo)], 1)

    angles = angles_of(length_y)
    y_table = np.concatenate([np.cos(angles), np.sin(angles)], 0)

    lane = np.arange(LANES)
    cell = (lane // slots % 2, lane % slots * cells_x + lane // width)
    mode = (lane % 2, lane // 2 % slots * cells_x + lane // width)

    def x_table(direction, rows, columns):
        table = complex_array(length_x, direction)[rows][:, columns[0], columns[1]]
        high, low = host_halves(table)
        return jnp.concatenate(
            [
                jnp.concatenate([high, low], 1),
                jnp.concatenate([high, jnp.zeros_like(low)], 1),
            ],
            0,
        )

    at = np.arange(1, LANES)
    mirror_z = np.zeros((LANES, LANES))
    mirror_z[LANES - at, at] = 1.0
    at = np.arange(1, rows_m)
    mirror_y = np.zeros((rows_m, rows_m))
    mirror_y[at, rows_m - at] = 1.0
    same = (mode[1][:, None] + mode[1][None]) % length_x == 0
    mirror_x = np.where(same & (mode[0][:, None] == mode[0][None]), 1.0, 0.0)

    def pool(extent_x, extent_y, factor):
        short_x, short_y = 2 * extent_x // factor, extent_y // factor
        row, cell = np.arange(short_x * short_y), np.arange(extent_x * extent_y)
        same_x = cell[None] // extent_y // (factor // 2) == row[:, None] // short_y
        same_y = cell[None] % extent_y // factor == row[:, None] % short_y
        return np.where(same_x & same_y, 1.0 / factor**3, 0.0)

    per_side = size_py // sides
    some = size_py // 2, cells_y
    lower = np.zeros((per_side, 8, half_cells // 2))
    lower[:, :4] = pool(*some, 4).reshape(per_side, 4, -1)
    lower[:, 4:5] = pool(*some, 8).reshape(per_side, 1, -1)
    pool_rows = np.concatenate([pool(*some, 2), lower.reshape(8 * per_side, -1)], 0)
    pool_columns = np.zeros((length_z, 2 * LANES))
    z = np.arange(length_z)
    pool_columns[z, z // 2] = 1.0
    pool_columns[z, LANES + z // 4] = 1.0
    pool_columns[z, LANES + length_z // 4 + z // 8] = 1.0

    ahead = [
        jnp.concatenate(host_halves(z_ahead[:, at : at + LANES]), 1)
        for at in range(0, length_z, LANES)
    ]
    held_in = [
        white_noise,
        jnp.stack(ahead),
        spectrum,
        jnp.asarray(np.tile(mirror_z, (2, 1)), BF16),
        jnp.asarray(np.tile(mirror_x, (2, 1)), BF16),
        jnp.asarray(np.tile(mirror_y, (1, 2)), BF16),
        *host_halves(y_table),
        x_table(-1.0, cell, mode),
        x_table(1.0, mode, cell),
        back,
        jnp.asarray(np.tile(pool_rows, (1, 2)), BF16),
        jnp.asarray(pool_columns, BF16),
        group_table,
    ]
    sizes = (cells_x, cells_y, length_z, slots, size_py)

    def body(*refs):
        whole_kernel(sizes, len(held_in), *refs)

    def vmem(*shape):
        return pltpu.VMEM(shape, F32)

    x_shape = (chunks, members, slots, length_y // slots, LANES)
    b_shape = (chunks, members, size_py, cells_y, LANES)
    s_shape = (2, tiles, cells_y, LANES)
    t_shape = (slots, rows_m, LANES)
    tall = cells_x * cells_y // 4 // size_py
    c_shapes = [(size_py, tall + 4, LANES)] * members
    sem = pltpu.SemaphoreType.DMA
    scratch = [pltpu.VMEM(value.shape, value.dtype) for value in held_in[:-1]]
    scratch.append(pltpu.SMEM(group_table.shape, group_table.dtype))
    for shape in (b_shape, x_shape, x_shape, b_shape):
        scratch += [vmem(*shape), vmem(*shape)]
    scratch += [vmem(size_py, *s_shape), vmem(size_py // 2, *s_shape), vmem(tiles, 1, LANES)]
    scratch += [vmem(*t_shape), vmem(*t_shape)]
    scratch += [vmem(8, LANES), vmem(size_py, 8, LANES), vmem(slots, size_py, 8, LANES)]
    scratch += [
        vmem(chunks, blocks, rows_m, LANES),
        vmem(blocks, rows_m, LANES),
        vmem(members, cells_x * cells_y, length_z),
        vmem(cells_x * cells_y, LANES),
        vmem(members, sides, half_cells, length_z),
        vmem(chunks, members, size_py // 2, cells_y, LANES),
        vmem(members, size_py // 2, cells_y, LANES),
        *[vmem(*shape) for shape in c_shapes * 3],
    ]
    scratch += [
        sem((len(held_in) + 1,)), sem((16,)), sem((chunks * members,)), sem((chunks * members,)),
        sem((chunks * members,)), sem((chunks * members,)), sem((members,)), sem((members,)), sem((5,)), sem((chunks * members,)), sem((members,)),
    ]
    hbm = pl.BlockSpec(memory_space=pltpu.HBM)
    local = pl.BlockSpec(memory_space=pltpu.VMEM)
    leaving = pl.pallas_call(
        body,
        out_shape=[jax.ShapeDtypeStruct(shape, F32) for shape in [white_noise.shape] + c_shapes],
        in_specs=[hbm] * len(held_in),
        out_specs=[local] * 3,
        scratch_shapes=scratch,
        compiler_params=pltpu.CompilerParams(
            collective_id=0, has_side_effects=True, vmem_limit_bytes=40 * 1024 * 1024
        ),
    )(*[pltpu.with_memory_space_constraint(v, pltpu.HBM) for v in held_in])
    outs = [white_noise.shape]
    for level in range(1, 4):
        outs.append((members,) + tuple(extent >> level for extent in white_noise.shape[1:]))
    return tuple(
        pl.pallas_call(
            leaving_kernel,
            out_shape=[jax.ShapeDtypeStruct(shape, F32) for shape in outs],
            in_specs=[local] * 3,
            out_specs=[hbm] * 4,
            scratch_shapes=[vmem(*outs[2]), vmem(*outs[3]), sem((2 * members + 2,))],
            compiler_params=pltpu.CompilerParams(vmem_limit_bytes=4 * 1024 * 1024),
        )(*leaving)
    )


def on_device(white_noise, spectrum, group_table):
    members, cells_x, cells_y, length_z = white_noise.shape
    size_px, size_py = lax.axis_size("px"), lax.axis_size("py")
    fits = members == 2 and length_z == 2 * LANES and size_px == 4 and size_py == 8
    fits = fits and 2 * cells_x * size_px == LANES and cells_x == 2 * size_py
    fits = fits and cells_y == 2 * cells_x
    chosen = lanes_path if fits else general_path
    return chosen(white_noise, spectrum, group_table)


def solution(mesh):
    in_specs = (P(None, "px", "py", None), P("px", "py", None), P())
    out_specs = (P(None, "px", "py", None),) * 4
    return jax.shard_map(
        on_device, mesh=mesh, in_specs=in_specs, out_specs=out_specs, check_vma=False
    )
```

```python
import numpy as np

import jax
import jax.numpy as jnp
from jax import lax
from jax.experimental import pallas as pl
from jax.experimental.pallas import tpu as pltpu
from jax.sharding import PartitionSpec as P


def angles_of(length):
    positions = np.arange(length, dtype=np.int64)
    return (positions[:, None] * positions[None, :] % length) * (2.0 * np.pi / length)


def complex_array(length, direction):
    angles = angles_of(length)
    cos, sin = np.cos(angles), direction * np.sin(angles)
    return np.stack([np.stack([cos, sin], 1), np.stack([-sin, cos], 1)], 0)


def complex_table(length, direction):
    return jnp.asarray(complex_array(length, direction), jnp.float32)


def half_tables(length):
    angles = angles_of(length)[:, : length // 2]
    ahead = np.stack([np.cos(angles), -np.sin(angles)], 1)
    back = 2.0 * ahead
    nyquist = np.where(np.arange(length) % 2 == 0, 1.0, -1.0)
    ahead[:, 1, 0] = nyquist
    back[:, 0, 0] = 1.0
    back[:, 1, 0] = nyquist
    return jnp.asarray(ahead, jnp.float32), jnp.asarray(back, jnp.float32)


def einsum(pattern, left, right):
    return jnp.einsum(pattern, left, right, precision=lax.Precision.HIGH)


def swap_first(values):
    first = values[:, :, :1]
    turned = jnp.swapaxes(first, 0, 1)
    return jnp.concatenate([turned, values[:, :, 1:]], 2)


def coarsen(values):
    members, size_x, size_y, size_z = values.shape
    blocks = values.reshape(members, size_x // 2, 2, size_y // 2, 2, size_z // 2, 2)
    return blocks.mean(axis=(2, 4, 6))


def general_path(white_noise, spectrum, group_table):
    members, cells_x, cells_y, length_z = white_noise.shape
    size_px, size_py = lax.axis_size("px"), lax.axis_size("py")
    length_x, length_y = cells_x * size_px, cells_y * size_py
    half_z = length_z // 2
    block_py, block = half_z // size_py, half_z // size_py // size_px
    z_ahead, z_back = half_tables(length_z)
    scale = 1.0 / (length_x * length_y * length_z)

    table = jnp.transpose(spectrum, (2, 0, 1))
    last = jnp.broadcast_to(table[half_z : half_z + 1], (size_py, 1, cells_x, cells_y))
    table = jnp.concatenate([table[:half_z].reshape(size_py, block_py, cells_x, cells_y), last], 1)
    table = lax.all_to_all(table, "py", split_axis=0, concat_axis=3, tiled=True)[0]
    last = jnp.broadcast_to(table[block_py:], (size_px, 1, cells_x, length_y))
    table = jnp.concatenate([table[:block_py].reshape(size_px, block, cells_x, length_y), last], 1)
    table = lax.all_to_all(table, "px", split_axis=0, concat_axis=2, tiled=True)[0] * scale
    is_first = (lax.axis_index("px") == 0) & (lax.axis_index("py") == 0)
    other = jnp.where(is_first, table[block:], table[:1])
    tables = jnp.stack([table[:block], jnp.concatenate([other, table[1:block]], 0)], 0)

    values = einsum("fxyz,zck->fckxy", white_noise, z_ahead)
    values = swap_first(values)
    values = lax.all_to_all(values, "py", split_axis=2, concat_axis=4, tiled=True)
    values = einsum("fckxy,cydm->fdkxm", values, complex_table(length_y, -1.0))
    values = lax.all_to_all(values, "px", split_axis=2, concat_axis=3, tiled=True)
    values = einsum("fckxm,cxdj->fdkjm", values, complex_table(length_x, -1.0))
    values = values * tables[:, None]
    values = einsum("fckjm,cjdx->fdkxm", values, complex_table(length_x, 1.0))
    values = lax.all_to_all(values, "px", split_axis=3, concat_axis=2, tiled=True)
    values = einsum("fckxm,cmdy->fdkxy", values, complex_table(length_y, 1.0))
    values = lax.all_to_all(values, "py", split_axis=4, concat_axis=2, tiled=True)
    values = swap_first(values)
    fields = einsum("fckxy,zck->fxyz", values, z_back)
    modulus = jnp.exp(0.5 * fields)

    levels = []
    level = modulus
    for _ in range(3):
        level = coarsen(level)
        levels.append(level)
    pieces = [jnp.reshape(level, (size_py, -1)) for level in levels]
    widths = [piece.shape[1] for piece in pieces]
    joined = jnp.concatenate(pieces, 1)
    spread = lax.all_to_all(joined, "py", split_axis=0, concat_axis=0, tiled=True)
    picked, start = [], 0
    for index, width in enumerate(widths):
        part = spread[:, start : start + width]
        picked.append(jnp.take(part, group_table[index], axis=0))
        start += width
    joined = lax.all_to_all(
        jnp.concatenate(picked, 1), "py", split_axis=0, concat_axis=0, tiled=True
    )
    routed, start = [], 0
    for level, width in zip(levels, widths):
        routed.append(joined[:, start : start + width].reshape(level.shape))
        start += width
    return (modulus, routed[0], routed[1], routed[2])


LANES = 128
ORDER = (
    "y0", "y1", "T", "y2", "x0", "y3", "x1", "y4", "x2", "b0", "x3", "y5", "b1",
    "y6", "x4", "b2", "y7", "b3", "x5", "x6", "b4", "x7", "b5", "b6", "b7",
)
MESH = pl.DeviceIdType.MESH
BF16 = jnp.bfloat16
F32 = jnp.float32


def halves(values):
    high = values.astype(BF16)
    low = (values - high.astype(F32)).astype(BF16)
    return high, low


def host_halves(values):
    values = np.asarray(values, np.float64)
    high = values.astype(np.float32).astype(BF16)
    low = (values - high.astype(np.float64)).astype(np.float32).astype(BF16)
    return jnp.asarray(high), jnp.asarray(low)


def mm(left, right):
    return jnp.dot(left, right, preferred_element_type=F32)


def lane_of(shape):
    return lax.broadcasted_iota(jnp.int32, shape, len(shape) - 1)


def exchange(arrays, width):
    count = len(arrays)
    field = (lane_of(arrays[0].shape) // width) % count
    skewed = [pltpu.roll(a, i * width, 1) if i else a for i, a in enumerate(arrays)]
    moved = [skewed[-index % count] for index in range(count)]
    distance = 1
    while distance < count:
        take = (field // distance) % 2 == 1
        moved = [
            jnp.where(take, moved[(index - distance) % count], moved[index])
            for index in range(count)
        ]
        distance *= 2
    return [pltpu.roll(m, LANES - i * width, 1) if i else m for i, m in enumerate(moved)]


def turned(values, slots, ahead):
    real = (lane_of(values.shape) // slots) % 2 == 0
    from_imag = pltpu.roll(values, LANES - slots, 1)
    from_real = pltpu.roll(values, slots, 1)
    if ahead:
        return jnp.where(real, from_imag, -from_real)
    return jnp.where(real, -from_imag, from_real)


def swap_slot(first, second, slots):
    place = lane_of(first.shape) % (2 * slots)
    return (
        jnp.where(place == slots, pltpu.roll(second, slots, 1), first),
        jnp.where(place == 0, pltpu.roll(first, LANES - slots, 1), second),
    )


class Route:
    def __init__(self, axis, count, away, source, target, send, recv):
        self.axis, self.count, self.away = axis, count, away
        self.source, self.target = source, target
        self.send, self.recv = send, recv
        self.me = lax.axis_index(axis)

    def copy(self, source, target, peer, part):
        return pltpu.make_async_remote_copy(
            src_ref=source,
            dst_ref=target,
            send_sem=self.send,
            recv_sem=self.recv.at[part] if part is not None else self.recv,
            device_id={self.axis: peer},
            device_id_type=MESH,
        )

    def at(self, ref, where, index):
        return ref.at[where + (index,)]

    def start(self, where, part):
        for peer in self.away:
            source = self.at(self.source, where, peer)
            target = self.at(self.target, where, self.me)
            self.copy(source, target, peer, part).start()

    def arrive(self, where, part):
        spot = self.at(self.target, where, pl.ds(0, self.count - 1))
        self.copy(spot, spot, self.away[0], part).wait_recv()
        self.target[where + (self.me,)] = self.source[where + (self.me,)]

    def drain(self, where):
        spot = self.source.at[where + (pl.ds(0, self.count - 1),)]
        self.copy(spot, spot, self.away[0], 0 if len(self.recv.shape) else None).wait_send()


def whole_kernel(sizes, loads, *refs):
    cells_x, cells_y, length_z, slots, ranks_y = sizes
    members = 2
    width = 2 * slots
    per_tile = cells_x // ranks_y
    tiles = length_z // LANES
    chunks = tiles * per_tile
    length_y = cells_y * ranks_y
    blocks = slots // members
    rows_m = length_y // blocks
    rows_part = length_y // slots
    sources, held_in = refs[:loads], refs[3 + loads : 3 + 2 * loads]
    modulus, d_recv_0, d_recv_1 = refs[loads : 3 + loads]
    (
        z_send, z_recv, x_send, x_recv, w_send, w_recv, b_send, b_recv,
        s_send, s_recv, e_recv, t_send, t_recv, n_send, n_recv, m_recv,
        tables, other, held, image, partial, h_recv, g_recv, c_send_0, c_send_1, c_recv_0, c_recv_1,
        d_send_0, d_send_1,
        load_sem, send_sem, z_sem, x_sem, w_sem, b_sem, c_sem, d_sem, s_sem, h_sem, g_sem,
    ) = refs[3 + 2 * loads :]
    (
        noise, ahead, spectrum, mirror_z, mirror_x, mirror_y, y_hi, y_lo, x_ahead, x_back,
        back, pool_rows, pool_columns, group_table,
    ) = held_in

    me_x, me_y = lax.axis_index("px"), lax.axis_index("py")
    pairs = [(sources[0].at[f], noise.at[f]) for f in range(members)]
    pairs = [pairs[0], (sources[1], ahead), *pairs[1:], *list(zip(sources, held_in))[2:]]
    copies = [
        pltpu.make_async_copy(source, target, load_sem.at[index])
        for index, (source, target) in enumerate(pairs)
    ]
    place, core = me_y // 2, me_y % 2
    chips = ranks_y // 2
    near = chips - 1 - (chips - 2) * (place % 2)
    inner = (place + 1) // 2 % 2
    far = near - (near - chips // 2) * inner
    steps = [far, near + chips // 2 - far, chips - near]
    away_y = []
    for step in steps:
        for side in (0, 1):
            away_y.append((place + step) % chips * 2 + (core + side) % 2)
    away_y.append(place * 2 + 1 - core)
    away_x = [slots - 1 - me_x, (me_x + 2) % slots, me_x + 1 - 2 * (me_x % 2)]

    barrier = pltpu.get_barrier_semaphore()
    for peer in away_y:
        pl.semaphore_signal(barrier, inc=1, device_id={"py": peer}, device_id_type=MESH)
    for peer in away_x:
        pl.semaphore_signal(barrier, inc=1, device_id={"px": peer}, device_id_type=MESH)

    early = 5
    for copy in copies[:early]:
        copy.start()

    def route(axis, source, target, send, recv):
        away, count = (away_y, ranks_y) if axis == "py" else (away_x, slots)
        return Route(axis, count, away, source, target, send_sem.at[send], recv)

    z_route = route("py", z_send, z_recv, 0, z_sem)
    x_route = route("px", x_send, x_recv, 1, x_sem)
    w_route = route("px", w_send, w_recv, 2, w_sem)
    b_route = route("py", b_send, b_recv, 3, b_sem)
    t_route = route("px", t_send, t_recv, 5, s_sem.at[1])
    c_send, c_recv = (c_send_0, c_send_1), (c_recv_0, c_recv_1)
    d_send, d_recv = (d_send_0, d_send_1), (d_recv_0, d_recv_1)
    c_routes = [route("py", c_send[f], c_recv[f], 12 + f, c_sem.at[f]) for f in range(members)]
    d_routes = [route("py", d_send[f], d_recv[f], 14 + f, d_sem.at[f]) for f in range(members)]

    lane = lane_of((8, LANES))
    quarter = (lane // 2) % slots
    half_y = ranks_y // 2
    my_half, my_place = me_y // half_y, me_y % half_y

    def strip_copy():
        return pltpu.make_async_remote_copy(
            src_ref=n_send, dst_ref=n_recv.at[me_y], send_sem=send_sem.at[8],
            recv_sem=s_sem.at[2], device_id={"py": 0}, device_id_type=MESH,
        )

    def half_copy(peer):
        return pltpu.make_async_remote_copy(
            src_ref=s_send.at[peer], dst_ref=s_recv.at[my_place], send_sem=send_sem.at[4],
            recv_sem=s_sem.at[0], device_id={"py": peer}, device_id_type=MESH,
        )

    def edge_copy(peer):
        return pltpu.make_async_remote_copy(
            src_ref=s_send.at[peer, 1, :, pl.ds(0, 1)], dst_ref=e_recv, send_sem=send_sem.at[10],
            recv_sem=s_sem.at[4], device_id={"py": peer}, device_id_type=MESH,
        )

    others = [my_half * half_y + (my_place + step) % half_y for step in range(1, half_y)]
    places = [(step + half_y // 2 * (1 - my_half)) % half_y for step in range(half_y)]
    across = [(1 - my_half) * half_y + spot for spot in places]

    def send_spectrum():
        pl.when(me_y != 0)(lambda: strip_copy().start())
        for peer in others[1:] + others[:1]:
            half_copy(peer).start()

        @pl.when(my_place == 0)
        def _():
            for peer in across:
                edge_copy(peer).start()

    middle = (place == chips // 2) | (place == chips // 2 - 1)
    giver, taker = middle & (core == 0), middle & (core == 1)

    def shared_start(route, where, part, hand, hand_sem, extra):
        source, target = route.source, route.target
        blocks_away = source.at[where + (pl.ds((1 - my_half) * half_y, half_y),)]

        def hand_copy():
            return pltpu.make_async_remote_copy(
                src_ref=blocks_away, dst_ref=hand, send_sem=route.send, recv_sem=hand_sem,
                device_id={"py": place * 2 + 1 - core}, device_id_type=MESH,
            )

        @pl.when(giver)
        def _():
            hand_copy().start()
            for peer in others:
                spot = source.at[where + (peer,)]
                route.copy(spot, target.at[where + (me_y,)], peer, part).start()

        @pl.when(jnp.logical_not(giver))
        def _():
            route.start(where, part)

        @pl.when(taker)
        def _():
            hand_copy().wait_recv()
            for spot, peer in zip(places, across):
                pltpu.make_async_remote_copy(
                    src_ref=hand.at[spot], dst_ref=target.at[where + (me_y - 1,)],
                    send_sem=send_sem.at[extra], recv_sem=route.recv.at[part],
                    device_id={"py": peer}, device_id_type=MESH,
                ).start()

    def z_start(chunk, f):
        part = chunk * members + f
        shared_start(z_route, (chunk, f), part, h_recv.at[chunk, f], h_sem.at[part], 11)

    def own_spectrum():
        mirrored = jnp.concatenate(
            halves(spectrum[:, :, LANES : 2 * LANES].reshape(cells_x * cells_y, LANES)), 1
        )
        image[...] = mm(mirrored, mirror_z[...])
        for row in range(0, cells_y, 8):
            rows = pl.ds(row, 8)
            plain = [spectrum[x, rows, pl.ds(0, LANES)] for x in range(cells_x)]
            turned_z = []
            for x in range(cells_x):
                value = image[pl.ds(x * cells_y + row, 8)]
                turned_z.append(jnp.where(lane == 0, plain[x], value))
            for kind, arrays in enumerate((plain, turned_z)):
                moved = exchange(arrays, width)
                for group in range(cells_x):
                    s_send[group % ranks_y, kind, group // ranks_y, rows] = moved[group]
        strip = jnp.zeros((8, LANES), F32)
        for x in range(cells_x):
            for part in range(cells_y // 8):
                value = spectrum[x, pl.ds(part * 8, 8), pl.ds(LANES, 1)]
                strip = jnp.where((lane // width == x) & (quarter == part), value, strip)
        n_send[...] = strip

    cells = cells_x * cells_y
    lined = []
    for tile in range(tiles):
        for f in range(members):
            if tile == 0:
                for copy in copies[2 * f : 2 + f]:
                    copy.wait()
                lined.append(halves(noise[f].reshape(cells, length_z)))
            high, low = lined[f]
            both = mm(high, ahead[tile])
            both = both[:, :LANES] + both[:, LANES:] + mm(low, ahead[tile, :, pl.ds(0, LANES)])
            held[f, :, pl.ds(tile * LANES, LANES)] = both
        lanes = pl.ds(tile * LANES, LANES)
        for row in range(0, cells_y, 8):
            rows = pl.ds(row, 8)
            both = []
            for f in range(members):
                both.append(
                    exchange(
                        [held[f, pl.ds(x * cells_y + row, 8), lanes] for x in range(cells_x)],
                        width,
                    )
                )
            if tile == 0:
                both[0][0], both[1][0] = swap_slot(both[0][0], both[1][0], slots)
            for f in range(members):
                for group in range(cells_x):
                    chunk = tile * per_tile + group // ranks_y
                    z_send[chunk, f, group % ranks_y, rows] = both[f][group]
        if tile == 0:
            pl.semaphore_wait(barrier, ranks_y + slots - 2)
        for part in range(tile * per_tile * members, (tile + 1) * per_tile * members):
            z_start(part // members, part % members)
            if part == 0:
                for copy in copies[3:early]:
                    copy.wait()
                for copy in copies[early:]:
                    copy.start()
                own_spectrum()
                send_spectrum()

    for copy in copies[early:]:
        copy.wait()
    sides = cells_x // ranks_y

    spot = s_recv.at[pl.ds(0, half_y - 1)]
    pltpu.make_async_remote_copy(
        src_ref=spot, dst_ref=spot, send_sem=send_sem.at[4], recv_sem=s_sem.at[0],
        device_id={"py": others[0]}, device_id_type=MESH,
    ).wait_recv()
    edge_copy(others[0]).wait_recv()
    s_recv[my_place] = s_send[me_y]
    pair = [s_recv[:, 1, tile].reshape(rows_m, LANES) for tile in range(tiles)]
    pair = jnp.concatenate(halves(jnp.concatenate(pair, 1)), 0)
    held[1, pl.ds(0, rows_m)] = mm(mirror_y[...], pair)
    sublane = lax.broadcasted_iota(jnp.int32, (8, LANES), 0)
    for row in range(0, rows_m, 8):
        arrays = []
        for tile in range(tiles):
            arrays.append(s_recv[row // cells_y, 0, tile, pl.ds(row % cells_y, 8)])
            value = held[1, pl.ds(row, 8), pl.ds(tile * LANES, LANES)]
            if row == 0:
                value = jnp.where(sublane == 0, e_recv[tile], value)
            arrays.append(value)
        moved = exchange(arrays, 2)
        for rank in range(slots):
            t_send[rank, pl.ds(row, 8)] = moved[rank]
    t_route.start((), None)

    def strips_copy(source):
        return pltpu.make_async_remote_copy(
            src_ref=n_recv, dst_ref=m_recv.at[source], send_sem=send_sem.at[9],
            recv_sem=s_sem.at[3], device_id={"px": 0}, device_id_type=MESH,
        )

    def along_y(columns):
        high, low = halves(columns)
        both = mm(y_hi[...], jnp.concatenate([high, low], 1))
        return both[:, :LANES] + both[:, LANES:] + mm(y_lo[...], high)

    def combined(product, start, rows, ahead):
        by_cos = product[start : start + rows]
        by_sin = product[length_y + start : length_y + start + rows]
        return by_cos + turned(by_sin, slots, ahead)

    def y_ahead(chunk, f):
        part = chunk * members + f
        z_route.arrive((chunk, f), part)
        product = along_y(z_recv[chunk, f].reshape(length_y, LANES))
        for row in range(0, rows_part, 16):
            arrays = [combined(product, a * rows_part + row, 16, True) for a in range(slots)]
            moved = exchange(arrays, 1)
            for rank in range(slots):
                x_send[chunk, f, rank, pl.ds(row, 16)] = moved[rank]
        x_route.start((chunk, f), part)

    def gathered(ref, chunk, f):
        pieces = [[] for _ in range(slots)]
        for row in range(0, rows_part, 16):
            moved = exchange([ref[chunk, f, s, pl.ds(row, 16)] for s in range(slots)], 1)
            for index in range(slots):
                pieces[index].append(moved[index])
        return jnp.concatenate([piece for some in pieces for piece in some], 0)

    def along_x(values, table):
        product = mm(jnp.concatenate(halves(values), 1), table[...])
        return product[:, :LANES] + product[:, LANES:]

    def x_both(chunk, f):
        part = chunk * members + f
        x_route.arrive((chunk, f), part)
        table = other if part == 1 else tables.at[chunk]
        values = along_x(gathered(x_recv, chunk, f), x_ahead)
        values = along_x(values * table[...].reshape(length_y, LANES), x_back)
        for row in range(0, rows_part, 16):
            arrays = [values[a * rows_part + row : a * rows_part + row + 16] for a in range(slots)]
            moved = exchange(arrays, 1)
            for s in range(slots):
                w_send[chunk, f, s, pl.ds(row, 16)] = moved[s]
        w_route.start((chunk, f), part)

    def y_back(chunk, f):
        part = chunk * members + f
        w_route.arrive((chunk, f), part)
        product = along_y(gathered(w_recv, chunk, f))
        for p in range(ranks_y):
            b_send[chunk, f, p] = combined(product, p * cells_y, cells_y, False)
        late = part - (chunks * members - g_recv.shape[0])
        if late >= 0:
            shared_start(b_route, (chunk, f), part, g_recv.at[late], g_sem.at[late], 7)
        else:
            b_route.start((chunk, f), part)

    def table_rows(tile, block, rows, part):
        even = lane % 2 == 0
        first = jnp.where(even, part, pltpu.roll(part, 1, 1))
        second = jnp.where(even, pltpu.roll(part, LANES - 1, 1), part)
        tables[tile * per_tile, block, rows] = first
        tables[tile * per_tile + 1, block, rows] = second
        if tile == 0:
            other[block, rows] = first

    def spectrum_tables():
        t_route.arrive((), None)
        images = [[] for _ in range(tiles)]
        for row in range(0, rows_m, 8):
            rows = pl.ds(row, 8)
            moved = exchange([t_recv[s, rows] for s in range(slots)], 2)
            for tile in range(tiles):
                table_rows(tile, my_half, rows, moved[2 * tile])
                images[tile].append(moved[2 * tile + 1])
        images = jnp.concatenate([piece for pieces in images for piece in pieces], 0)
        images = mm(jnp.concatenate(halves(images), 1), mirror_x[...])
        for tile in range(tiles):
            for row in range(0, rows_m, 8):
                at = tile * rows_m + row
                table_rows(tile, 1 - my_half, pl.ds(row, 8), images[at : at + 8])

        @pl.when((me_y == 0) & (me_x == 0))
        def _():
            spot = m_recv.at[pl.ds(1, slots - 1)]
            pltpu.make_async_remote_copy(
                src_ref=spot, dst_ref=spot, send_sem=send_sem.at[9], recv_sem=s_sem.at[3],
                device_id={"px": 1}, device_id_type=MESH,
            ).wait_recv()
            for p in range(ranks_y):
                strips = [n_recv[p] if s == 0 else m_recv[s, p] for s in range(slots)]
                for part in range(cells_y // 8):
                    value = strips[part]
                    for s in range(slots):
                        shift = (s - part) * 2 % LANES
                        moved = pltpu.roll(strips[s], shift, 1) if shift else strips[s]
                        value = jnp.where(quarter == s, moved, value)
                    at = p * cells_y + part * 8
                    other[at // rows_m, pl.ds(at % rows_m, 8)] = value

    @pl.when(me_y == 0)
    def _():
        spot = n_recv.at[pl.ds(0, ranks_y - 1)]
        pltpu.make_async_remote_copy(
            src_ref=spot, dst_ref=spot, send_sem=send_sem.at[8], recv_sem=s_sem.at[2],
            device_id={"py": 1}, device_id_type=MESH,
        ).wait_recv()
        n_recv[0] = n_send[...]
        pl.when(me_x != 0)(lambda: strips_copy(me_x).start())

    steps = {"y": y_ahead, "x": x_both, "b": y_back}

    def run(order):
        for step in order:
            if step == "T":
                spectrum_tables()
            else:
                steps[step[0]](int(step[1:]) // members, int(step[1:]) % members)

    run(ORDER)

    tall = cells // 4 // ranks_y
    def z_back(chunk, f):
        pieces = [[] for _ in range(ranks_y)]
        for row in range(0, cells_y, 8):
            rows = pl.ds(row, 8)
            arrays = [b_recv[chunk, f, group, rows] for group in range(ranks_y)]
            if chunk == 0:
                pair = [b_recv[0, 0, 0, rows], b_recv[0, 1, 0, rows]]
                arrays[0] = swap_slot(*pair, slots)[f]
            moved = exchange(arrays, width)
            for x in range(ranks_y):
                pieces[x].append(moved[x])
        cells_by = jnp.concatenate([piece for some in pieces for piece in some], 0)
        swapped = pltpu.roll(cells_by, LANES // 2, 1)
        near_side = lane_of(cells_by.shape) < LANES // 2
        first_side = 0 if chunk + 1 < chunks else 1 - my_half
        if chunk + 1 == chunks:
            flip = first_side == 1
            cells_by, swapped = (
                jnp.where(flip, swapped, cells_by), jnp.where(flip, cells_by, swapped)
            )

        def fields(value, beside, side):
            high = value.astype(BF16)
            low = beside - beside.astype(BF16).astype(F32)
            mixed = jnp.where(near_side, high.astype(F32), low).astype(BF16)
            result = mm(jnp.concatenate([mixed, high], 1), back[chunk])
            return result + partial[f, side] if chunk > 0 else result

        if chunk + 1 < chunks:
            partial[f, 0] = fields(cells_by, swapped, 0)
            partial[f, 1] = fields(swapped, cells_by, 1)
            return
        for side, peers, value, beside in (
            (1 - my_half, across, cells_by, swapped), (my_half, others, swapped, cells_by)
        ):
            values = jnp.exp2(fields(value, beside, side))
            cut = values.reshape(ranks_y, cells_y, length_z)
            modulus[f, pl.ds(side * ranks_y, ranks_y)] = cut
            paired = values.reshape(ranks_y // 2, 2, cells_y, length_z)
            paired = (paired[:, 0] + paired[:, 1]).reshape(-1, length_z)
            high_part, low_part = halves(paired)
            pooled = mm(pool_rows[...], jnp.concatenate([high_part, low_part], 0))
            high_part, low_part = halves(pooled)
            coarse = mm(high_part, pool_columns[...]) + mm(low_part, pool_columns[...])
            for e in range(half_y):
                piece = side * half_y + e
                c_send[f][piece, pl.ds(0, tall)] = coarse[e * tall : (e + 1) * tall, :LANES]
                at = half_y * tall + e * 8
                value = coarse[at : at + 8, LANES:]
                value = jnp.where(lane < LANES // 2, value, pltpu.roll(value, 4, 0))
                c_send[f][piece, pl.ds(tall, 4)] = value[:4]
            for peer in peers:
                spot = c_recv[f].at[me_y]
                c_routes[f].copy(c_send[f].at[peer], spot, peer, None).start()

    def pick(f):
        c_routes[f].arrive((), None)
        for g in range(ranks_y):
            d_send[f][g, pl.ds(0, tall)] = c_recv[f][group_table[0, g], pl.ds(0, tall)]
            second = c_recv[f][group_table[1, g], pl.ds(tall, 4)]
            third = c_recv[f][group_table[2, g], pl.ds(tall, 4)]
            d_send[f][g, pl.ds(tall, 4)] = jnp.where(lane[:4] < LANES // 2, second, third)
        d_routes[f].start((), None)

    for chunk in range(chunks):
        for f in range(members):
            b_route.arrive((chunk, f), chunk * members + f)
            if chunk > 0:
                z_back(chunk, f)
        if chunk == 0:
            for f in range(members):
                z_back(chunk, f)
    for f in range(members):
        pick(f)
    for f in range(members):
        d_routes[f].arrive((), None)

    every = pl.ds(0, chunks)
    z_route.drain((every, pl.ds(0, members)))

    @pl.when(taker)
    def _():
        pltpu.make_async_remote_copy(
            src_ref=h_recv, dst_ref=h_recv, send_sem=send_sem.at[11], recv_sem=h_sem.at[0],
            device_id={"py": others[0]}, device_id_type=MESH,
        ).wait_send()
        pltpu.make_async_remote_copy(
            src_ref=g_recv, dst_ref=g_recv, send_sem=send_sem.at[7], recv_sem=g_sem.at[0],
            device_id={"py": others[0]}, device_id_type=MESH,
        ).wait_send()

    x_route.drain((every, pl.ds(0, members)))
    w_route.drain((every, pl.ds(0, members)))
    b_route.drain((every, pl.ds(0, members)))
    spot = s_send.at[pl.ds(0, half_y - 1)]
    pltpu.make_async_remote_copy(
        src_ref=spot, dst_ref=spot, send_sem=send_sem.at[4], recv_sem=s_sem.at[0],
        device_id={"py": others[0]}, device_id_type=MESH,
    ).wait_send()

    @pl.when(my_place == 0)
    def _():
        spot = s_send.at[pl.ds(0, half_y), 1, :, pl.ds(0, 1)]
        pltpu.make_async_remote_copy(
            src_ref=spot, dst_ref=spot, send_sem=send_sem.at[10], recv_sem=s_sem.at[4],
            device_id={"py": others[0]}, device_id_type=MESH,
        ).wait_send()

    t_route.drain(())
    for some in c_routes + d_routes:
        some.drain(())
    pl.when(me_y != 0)(lambda: strip_copy().wait_send())
    pl.when((me_y == 0) & (me_x != 0))(lambda: strips_copy(me_x).wait_send())


def leaving_kernel(modulus, first, second, *refs):
    modulus_out, one_out, two_out, three_out, level_two, level_three, sems = refs
    members, cells_x, cells_y, length_z = modulus.shape
    ranks_y, tall = first.shape[0], first.shape[1] - 4
    copies = []
    for f, coarse in enumerate((first, second)):
        copies.append((modulus.at[f], modulus_out.at[f]))
        copies.append((coarse.at[:, pl.ds(0, tall)], one_out.at[f]))
    copies = [
        pltpu.make_async_copy(source, target, sems.at[index])
        for index, (source, target) in enumerate(copies)
    ]
    for copy in copies:
        copy.start()
    wide, narrow = level_two.shape[3], level_three.shape[3]
    for f, coarse in enumerate((first, second)):
        for d in range(ranks_y):
            low = coarse[d, pl.ds(tall, 4)]
            level_two[f, d // 2, pl.ds(d % 2 * 4, 4)] = low[:, :wide]
            low = pltpu.roll(low, LANES // 2, 1)
            level_three[f, d // 4, pl.ds(d % 4, 1)] = low[:1, :narrow]
    for level, out in ((level_two, two_out), (level_three, three_out)):
        copies.append(pltpu.make_async_copy(level, out, sems.at[len(copies)]))
        copies[-1].start()
    for copy in copies:
        copy.wait()


def lanes_path(white_noise, spectrum, group_table):
    members, cells_x, cells_y, length_z = white_noise.shape
    size_px, size_py = lax.axis_size("px"), lax.axis_size("py")
    length_x, length_y = cells_x * size_px, cells_y * size_py
    slots, width = size_px, 2 * size_px
    tiles = length_z // LANES
    per_tile = cells_x // size_py
    chunks = tiles * per_tile
    blocks = slots // members
    rows_m = length_y // blocks

    column = np.arange(length_z)
    tile, lane = column // LANES, column % LANES
    part = (lane // slots) % 2
    group = lane // width
    rank_q, rank_p, inner = lane % slots, group % size_py, group // size_py
    k = ((tile * size_py + rank_p) * slots + rank_q) * per_tile + inner
    angles = angles_of(length_z)
    sign = np.where(np.arange(length_z) % 2 == 0, 1.0, -1.0)
    z_ahead = np.where(part == 0, np.cos(angles[:, k]), -np.sin(angles[:, k]))
    z_back = 2.0 * z_ahead
    first = (k == 0) & (part == 0)
    second = (k == 0) & (part == 1)
    z_ahead[:, second] = sign[:, None]
    z_back[:, first] = 1.0
    z_back[:, second] = sign[:, None]
    z_back = z_back.T * (0.5 / np.log(2.0) / (length_x * length_y * length_z))

    sides = cells_x // size_py
    half_cells = cells_x * cells_y // sides
    back_hi, back_lo = host_halves(z_back.reshape(chunks, LANES // sides, length_z))
    back = jnp.concatenate([back_hi, back_hi, back_lo, jnp.zeros_like(back_lo)], 1)

    angles = angles_of(length_y)
    y_table = np.concatenate([np.cos(angles), np.sin(angles)], 0)

    lane = np.arange(LANES)
    cell = (lane // slots % 2, lane % slots * cells_x + lane // width)
    mode = (lane % 2, lane // 2 % slots * cells_x + lane // width)

    def x_table(direction, rows, columns):
        table = complex_array(length_x, direction)[rows][:, columns[0], columns[1]]
        high, low = host_halves(table)
        return jnp.concatenate(
            [
                jnp.concatenate([high, low], 1),
                jnp.concatenate([high, jnp.zeros_like(low)], 1),
            ],
            0,
        )

    at = np.arange(1, LANES)
    mirror_z = np.zeros((LANES, LANES))
    mirror_z[LANES - at, at] = 1.0
    at = np.arange(1, rows_m)
    mirror_y = np.zeros((rows_m, rows_m))
    mirror_y[at, rows_m - at] = 1.0
    same = (mode[1][:, None] + mode[1][None]) % length_x == 0
    mirror_x = np.where(same & (mode[0][:, None] == mode[0][None]), 1.0, 0.0)

    def pool(extent_x, extent_y, factor):
        short_x, short_y = 2 * extent_x // factor, extent_y // factor
        row, cell = np.arange(short_x * short_y), np.arange(extent_x * extent_y)
        same_x = cell[None] // extent_y // (factor // 2) == row[:, None] // short_y
        same_y = cell[None] % extent_y // factor == row[:, None] % short_y
        return np.where(same_x & same_y, 1.0 / factor**3, 0.0)

    per_side = size_py // sides
    some = size_py // 2, cells_y
    lower = np.zeros((per_side, 8, half_cells // 2))
    lower[:, :4] = pool(*some, 4).reshape(per_side, 4, -1)
    lower[:, 4:5] = pool(*some, 8).reshape(per_side, 1, -1)
    pool_rows = np.concatenate([pool(*some, 2), lower.reshape(8 * per_side, -1)], 0)
    pool_columns = np.zeros((length_z, 2 * LANES))
    z = np.arange(length_z)
    pool_columns[z, z // 2] = 1.0
    pool_columns[z, LANES + z // 4] = 1.0
    pool_columns[z, LANES + length_z // 4 + z // 8] = 1.0

    ahead = [
        jnp.concatenate(host_halves(z_ahead[:, at : at + LANES]), 1)
        for at in range(0, length_z, LANES)
    ]
    held_in = [
        white_noise,
        jnp.stack(ahead),
        spectrum,
        jnp.asarray(np.tile(mirror_z, (2, 1)), BF16),
        jnp.asarray(np.tile(mirror_x, (2, 1)), BF16),
        jnp.asarray(np.tile(mirror_y, (1, 2)), BF16),
        *host_halves(y_table),
        x_table(-1.0, cell, mode),
        x_table(1.0, mode, cell),
        back,
        jnp.asarray(np.tile(pool_rows, (1, 2)), BF16),
        jnp.asarray(pool_columns, BF16),
        group_table,
    ]
    sizes = (cells_x, cells_y, length_z, slots, size_py)

    def body(*refs):
        whole_kernel(sizes, len(held_in), *refs)

    def vmem(*shape):
        return pltpu.VMEM(shape, F32)

    x_shape = (chunks, members, slots, length_y // slots, LANES)
    b_shape = (chunks, members, size_py, cells_y, LANES)
    s_shape = (2, tiles, cells_y, LANES)
    t_shape = (slots, rows_m, LANES)
    tall = cells_x * cells_y // 4 // size_py
    c_shapes = [(size_py, tall + 4, LANES)] * members
    sem = pltpu.SemaphoreType.DMA
    scratch = [pltpu.VMEM(value.shape, value.dtype) for value in held_in[:-1]]
    scratch.append(pltpu.SMEM(group_table.shape, group_table.dtype))
    for shape in (b_shape, x_shape, x_shape, b_shape):
        scratch += [vmem(*shape), vmem(*shape)]
    scratch += [vmem(size_py, *s_shape), vmem(size_py // 2, *s_shape), vmem(tiles, 1, LANES)]
    scratch += [vmem(*t_shape), vmem(*t_shape)]
    scratch += [vmem(8, LANES), vmem(size_py, 8, LANES), vmem(slots, size_py, 8, LANES)]
    scratch += [
        vmem(chunks, blocks, rows_m, LANES),
        vmem(blocks, rows_m, LANES),
        vmem(members, cells_x * cells_y, length_z),
        vmem(cells_x * cells_y, LANES),
        vmem(members, sides, half_cells, length_z),
        vmem(chunks, members, size_py // 2, cells_y, LANES),
        vmem(2 * members, size_py // 2, cells_y, LANES),
        *[vmem(*shape) for shape in c_shapes * 3],
    ]
    scratch += [
        sem((len(held_in) + 1,)), sem((16,)), sem((chunks * members,)), sem((chunks * members,)),
        sem((chunks * members,)), sem((chunks * members,)), sem((members,)), sem((members,)), sem((5,)), sem((chunks * members,)), sem((2 * members,)),
    ]
    hbm = pl.BlockSpec(memory_space=pltpu.HBM)
    local = pl.BlockSpec(memory_space=pltpu.VMEM)
    leaving = pl.pallas_call(
        body,
        out_shape=[jax.ShapeDtypeStruct(shape, F32) for shape in [white_noise.shape] + c_shapes],
        in_specs=[hbm] * len(held_in),
        out_specs=[local] * 3,
        scratch_shapes=scratch,
        compiler_params=pltpu.CompilerParams(
            collective_id=0, has_side_effects=True, vmem_limit_bytes=40 * 1024 * 1024
        ),
    )(*[pltpu.with_memory_space_constraint(v, pltpu.HBM) for v in held_in])
    outs = [white_noise.shape]
    for level in range(1, 4):
        outs.append((members,) + tuple(extent >> level for extent in white_noise.shape[1:]))
    return tuple(
        pl.pallas_call(
            leaving_kernel,
            out_shape=[jax.ShapeDtypeStruct(shape, F32) for shape in outs],
            in_specs=[local] * 3,
            out_specs=[hbm] * 4,
            scratch_shapes=[vmem(*outs[2]), vmem(*outs[3]), sem((2 * members + 2,))],
            compiler_params=pltpu.CompilerParams(vmem_limit_bytes=4 * 1024 * 1024),
        )(*leaving)
    )


def on_device(white_noise, spectrum, group_table):
    members, cells_x, cells_y, length_z = white_noise.shape
    size_px, size_py = lax.axis_size("px"), lax.axis_size("py")
    fits = members == 2 and length_z == 2 * LANES and size_px == 4 and size_py == 8
    fits = fits and 2 * cells_x * size_px == LANES and cells_x == 2 * size_py
    fits = fits and cells_y == 2 * cells_x
    chosen = lanes_path if fits else general_path
    return chosen(white_noise, spectrum, group_table)


def solution(mesh):
    in_specs = (P(None, "px", "py", None), P("px", "py", None), P())
    out_specs = (P(None, "px", "py", None),) * 4
    return jax.shard_map(
        on_device, mesh=mesh, in_specs=in_specs, out_specs=out_specs, check_vma=False
    )
```
